8 devices in a mesh: dp: 1 (over z), tp: 2 (over y), sp: 4 (over x, core).
Axes of the slice: x: 2, y: 2, z: 1, core: 2. Of those that a mesh axis runs over, the one named last changes fastest.
Arguments:
- hidden: bfloat16 [64, 3072], P('dp')
- norm_scale: bfloat16 [3072], replicated
- w_qkv: bfloat16 [3072, 5120], P(None, 'tp')
- w_out: bfloat16 [3072, 3072], P('tp')
- k_cache: bfloat16 [64, 1024, 8, 128], P('dp', 'sp', 'tp')
- v_cache: bfloat16 [64, 1024, 8, 128], P('dp', 'sp', 'tp')
- positions: int32 [64], P('dp')
Outputs:
- output 1: bfloat16 [64, 3072], P('dp')
- output 2: bfloat16 [64, 1024, 8, 128], P('dp', 'sp', 'tp')
- output 3: bfloat16 [64, 1024, 8, 128], P('dp', 'sp', 'tp')
All inputs are finite; a program needn't handle non-finite values.
Results may differ from the reference program's by a relative error of at most 0.00645291.
Values sent between devices are 32-bit elements.
A program may use at most 1 GiB of HBM per device.

```python
import math
import jax
import jax.numpy as jnp
from jax import lax

BATCH = 64
SEQ = 1024
D = 3072
HEADS = 24
KV_HEADS = 8
HEAD = 128


def rope_apply(head_vals, positions):
    half_dim = head_vals.shape[-1] // 2
    inv_freq = jnp.exp(jnp.arange(half_dim, dtype=jnp.float32) * (-2.0 * math.log(500000.0) / head_vals.shape[-1]))
    angles = positions.astype(jnp.float32)[:, None] * inv_freq[None, :]
    cos_part = jnp.cos(angles)[:, None, None, :]
    sin_part = jnp.sin(angles)[:, None, None, :]
    first_half = head_vals[..., :half_dim]
    second_half = head_vals[..., half_dim:]
    return jnp.concatenate([first_half * cos_part - second_half * sin_part, second_half * cos_part + first_half * sin_part], axis=-1)


def setup_inputs(seed: int = 0, part: int = 0) -> dict:
    part_keys = jax.random.split(jax.random.fold_in(jax.random.key(seed), part), 5)
    shared_keys = jax.random.split(jax.random.key(seed + 1), 4)
    qkv_width = (HEADS + 2 * KV_HEADS) * HEAD
    hidden = jax.random.normal(part_keys[0], (BATCH, D), jnp.float32)
    norm_scale = 1.0 + 0.5 * jax.random.normal(shared_keys[0], (D,), jnp.float32)
    col_boost = jnp.where(jax.random.randint(shared_keys[1], (qkv_width,), 0, 16) == 0, 10.0, 1.0)
    w_qkv = jax.random.normal(shared_keys[2], (D, qkv_width), jnp.float32) * col_boost * (D ** -0.5)
    w_out = jax.random.normal(shared_keys[3], (HEADS * HEAD, D), jnp.float32) * (2.0 * (HEADS * HEAD) ** -0.5)
    k_cache = 0.5 * jax.random.normal(part_keys[1], (BATCH, SEQ, KV_HEADS, HEAD), jnp.float32)
    coarse = jax.random.normal(part_keys[2], (BATCH, 8, 1, KV_HEADS, HEAD), jnp.float32)
    fine_part = jax.random.normal(part_keys[3], (BATCH, 8, SEQ // 8, KV_HEADS, HEAD), jnp.float32)
    v_cache = (coarse + 0.5 * fine_part).reshape(BATCH, SEQ, KV_HEADS, HEAD)
    positions = jax.random.randint(part_keys[4], (BATCH,), SEQ // 8, SEQ)
    positions = positions.at[0].set(SEQ - 1).at[1].set(SEQ // 8)
    return {
        'hidden': hidden.astype(jnp.bfloat16),
        'norm_scale': norm_scale.astype(jnp.bfloat16),
        'w_qkv': w_qkv.astype(jnp.bfloat16),
        'w_out': w_out.astype(jnp.bfloat16),
        'k_cache': k_cache.astype(jnp.bfloat16),
        'v_cache': v_cache.astype(jnp.bfloat16),
        'positions': positions.astype(jnp.int32),
    }


def reference(hidden, norm_scale, w_qkv, w_out, k_cache, v_cache, positions):
    q_per_kv = HEADS // KV_HEADS
    hidden_f32 = hidden.astype(jnp.float32)
    row_mean = jnp.mean(hidden_f32, axis=-1, keepdims=True)
    centered = hidden_f32 - row_mean
    row_var = jnp.mean(centered * centered, axis=-1, keepdims=True)
    normed = (centered * lax.rsqrt(row_var + 1e-5) * norm_scale.astype(jnp.float32)).astype(jnp.bfloat16)
    qkv_proj = jnp.clip(jnp.dot(normed, w_qkv, preferred_element_type=jnp.float32).astype(jnp.bfloat16), -8.0, 8.0)
    grouped = qkv_proj.reshape(BATCH, KV_HEADS, q_per_kv + 2, HEAD)
    rotated = rope_apply(grouped[:, :, : q_per_kv + 1].astype(jnp.float32), positions).astype(jnp.bfloat16)
    queries = rotated[:, :, :q_per_kv]
    new_row = (jnp.arange(SEQ)[None, :] == positions[:, None])[:, :, None, None]
    k_upd = jnp.where(new_row, rotated[:, :, q_per_kv][:, None], k_cache)
    v_upd = jnp.where(new_row, grouped[:, :, q_per_kv + 1][:, None], v_cache)

    def one_sequence(seq_args):
        q_seq, k_seq, v_seq, p_seq = seq_args
        scores = jnp.einsum('gqd,sgd->gqs', q_seq.astype(jnp.float32), k_seq.astype(jnp.float32)) * (HEAD ** -0.5)
        valid_mask = jnp.arange(SEQ) <= p_seq
        scores = jnp.where(valid_mask[None, None, :], scores, -jnp.inf)
        weights_bf = jax.nn.softmax(scores, axis=-1).astype(jnp.bfloat16)
        return jnp.einsum('gqs,sgd->gqd', weights_bf.astype(jnp.float32), v_seq.astype(jnp.float32))

    attn_out = lax.map(one_sequence, (queries, k_upd, v_upd, positions))
    attn_flat = attn_out.reshape(BATCH, HEADS * HEAD).astype(jnp.bfloat16)
    h_out = (hidden_f32 + jnp.dot(attn_flat, w_out, preferred_element_type=jnp.float32)).astype(jnp.bfloat16)
    return (h_out, k_upd, v_upd)
```

```python
import math
import jax
import jax.numpy as jnp
import numpy as np
from jax import lax
from jax.experimental import pallas as pl
from jax.experimental.pallas import tpu as pltpu
from jax.sharding import PartitionSpec as P

MESH = pl.DeviceIdType.MESH
NEG = -1e30
MIB = 1024 * 1024
N_SP = 4
GROUP = 8
W_CHUNKS = 6
W_SLOTS = 3
HELD = 7
JOB = 2
SLOTS = 4
W_VMEM = 3


def attend_kernel(dims, pos, hidden, norm_scale, cos2, sin2, w_qkv, w_out, k_in, v_in,
                  h_out, k_vm, v_vm, new_k, new_v,
                  u, wq, acc, wo, k_rest, v_rest, q_rows, kn_rows, vn_rows, tok, part, recv, merged, proj, proj_in, sums,
                  w_sem, wo_sem, k_sem, v_sem, part_send, part_recv, proj_send, proj_recv, sum_send, sum_recv):
    n_seq, rows, kv, head, per_kv, d_model = dims
    n_heads = kv * per_kv
    n_groups = n_seq // GROUP
    pair_rows = 2 * n_heads
    own = n_seq // N_SP
    w_rows = d_model // W_CHUNKS
    sp = lax.axis_index('sp')
    tp = lax.axis_index('tp')
    seq_local = rows // kv
    scale2 = head ** -0.5 * math.log2(math.e)

    def w_copy(c):
        return pltpu.make_async_copy(w_qkv.at[pl.ds(c * w_rows, w_rows)], wq.at[c % W_SLOTS], w_sem.at[c])

    def held(ref, rest, n_held, g):
        return (ref, g) if g < n_held else (rest, g - n_held)

    def cache_copy(src, ref, rest, n_held, sem, g):
        dst, i = held(ref, rest, n_held, g)
        return pltpu.make_async_copy(src.at[pl.ds(g * GROUP, GROUP)], dst.at[pl.ds(i * GROUP, GROUP)], sem.at[g])

    def k_copy(g):
        return cache_copy(k_in, k_vm, k_rest, HELD, k_sem, g)

    def v_copy(g):
        return cache_copy(v_in, v_vm, v_rest, HELD, v_sem, g)

    wo_copy = pltpu.make_async_copy(w_out, wo, wo_sem)
    for c in range(W_SLOTS):
        w_copy(c).start()
    for g in range(n_groups - W_CHUNKS):
        k_copy(g).start()
        v_copy(g).start()

    barrier = pltpu.get_barrier_semaphore()
    for s in range(1, N_SP):
        pl.semaphore_signal(barrier, inc=1, device_id={'sp': lax.rem(sp + s, N_SP)}, device_id_type=MESH)
    pl.semaphore_signal(barrier, inc=1, device_id={'tp': 1 - tp}, device_id_type=MESH)

    hid = hidden[...].astype(jnp.float32)
    mean = jnp.mean(hid, axis=-1, keepdims=True)
    cen = hid - mean
    var = jnp.mean(cen * cen, axis=-1, keepdims=True)
    normed = (cen * lax.rsqrt(var + 1e-5) * norm_scale[...].astype(jnp.float32)).astype(jnp.bfloat16)
    for c in range(W_CHUNKS):
        u[c] = normed[:, c * w_rows:(c + 1) * w_rows]

    col = lax.broadcasted_iota(jnp.int32, (pair_rows, rows), 1)
    row = lax.broadcasted_iota(jnp.int32, (pair_rows, rows), 0)
    row_kv = lax.rem(row, n_heads) // per_kv
    tok[...] = jnp.where(lax.rem(col, kv) == row_kv, sp * seq_local + col // kv, 1 << 30)

    acc[...] = jnp.zeros_like(acc)

    for c in range(W_CHUNKS):
        w_copy(c).wait()
        g = c + (n_groups - W_CHUNKS)
        k_copy(g).start()
        v_copy(g).start()
        acc[...] += jnp.dot(u[c], wq[c % W_SLOTS], preferred_element_type=jnp.float32)
        if c + W_SLOTS < W_CHUNKS:
            w_copy(c + W_SLOTS).start()

    wo_copy.start()

    c2 = cos2[...]
    s2 = sin2[...]
    for g in range(kv):
        for j in range(per_kv + 2):
            lo = (g * (per_kv + 2) + j) * head
            x = jnp.clip(acc[:, lo:lo + head].astype(jnp.bfloat16).astype(jnp.float32), -8.0, 8.0)
            if j <= per_kv:
                x = (x * c2 + pltpu.roll(x, head // 2, 1) * s2).astype(jnp.bfloat16).astype(jnp.float32)
            if j < per_kv:
                q_rows[pl.ds(g * per_kv + j, n_seq, stride=n_heads), :] = x
            else:
                wide, rep = (kn_rows, new_k) if j == per_kv else (vn_rows, new_v)
                for i in range(per_kv):
                    wide[pl.ds(g * per_kv + i, n_seq, stride=n_heads), :] = x
                for i in range(16 // kv):
                    rep[pl.ds(i * kv + g, n_seq, stride=16), :] = x

    pl.semaphore_wait(barrier, N_SP)

    prow = lax.broadcasted_iota(jnp.int32, (pair_rows, 1), 0)
    first = prow < n_heads

    def part_copy(g, s):
        dst = lax.rem(sp + s, N_SP)
        return pltpu.make_async_remote_copy(
            src_ref=part.at[g, dst], dst_ref=recv.at[g, s - 1],
            send_sem=part_send.at[g, s - 1], recv_sem=part_recv.at[g, s - 1],
            device_id={'sp': dst}, device_id_type=MESH)

    def group_step(g, k_ref, v_ref, k_off, v_off):
        for d in range(N_SP):
            b = g * GROUP + 2 * d
            kb, vb = b - k_off, b - v_off
            q = q_rows[pl.ds(pl.multiple_of((g * N_SP + d) * pair_rows, 8), pair_rows), :]
            zero = jnp.zeros_like(q)
            q_blk = jnp.concatenate([jnp.where(first, q, zero), jnp.where(first, zero, q)], axis=1).astype(jnp.bfloat16)
            k_cat = jnp.concatenate([k_ref[kb], k_ref[kb + 1]], axis=1)
            s = lax.dot_general(q_blk, k_cat, (((1,), (1,)), ((), ())), preferred_element_type=jnp.float32)
            limit = jnp.where(first, pos[b], pos[b + 1])
            s = jnp.where(tok[...] < limit, s, NEG)
            m = jnp.max(s, axis=-1, keepdims=True)
            w = jnp.exp2((s - m) * scale2)
            l = jnp.sum(w, axis=-1, keepdims=True)
            v_cat = jnp.concatenate([v_ref[vb], v_ref[vb + 1]], axis=1)
            o = jnp.dot(w.astype(jnp.bfloat16), v_cat, preferred_element_type=jnp.float32)
            part[g, d, :, :head] = jnp.where(first, o[:, :head], o[:, head:])
            lane = lax.broadcasted_iota(jnp.int32, (pair_rows, head), 1)
            part[g, d, :, head:] = jnp.where(lane < head // 2, m, l)
        for s in range(1, N_SP):
            part_copy(g, s).start()

    def held_step(g, carry):
        s = pl.ds(g * GROUP, GROUP)
        pltpu.make_async_copy(k_in.at[s], k_vm.at[s], k_sem.at[g]).wait()
        pltpu.make_async_copy(v_in.at[s], v_vm.at[s], v_sem.at[g]).wait()
        group_step(g, k_vm, v_vm, 0, 0)
        return carry

    lax.fori_loop(0, HELD, held_step, 0)
    for g in range(HELD, n_groups):
        k_copy(g).wait()
        v_copy(g).wait()
        k_ref, ki = held(k_vm, k_rest, HELD, g)
        v_ref, vi = held(v_vm, v_rest, HELD, g)
        group_step(g, k_ref, v_ref, (g - ki) * GROUP, (g - vi) * GROUP)

    def merge_step(g, carry):
        for s in range(1, N_SP):
            part_copy(g, s).wait()
        r = pl.ds(pl.multiple_of((g * N_SP + sp) * pair_rows, 8), pair_rows)
        s_new = jnp.sum(q_rows[r, :] * kn_rows[r, :], axis=-1, keepdims=True)
        outs = [part[g, sp]] + [recv[g, s] for s in range(N_SP - 1)]
        ms = [x[:, head:head + 1] for x in outs]
        ls = [x[:, head + head // 2:head + head // 2 + 1] for x in outs]
        top = s_new
        for m in ms:
            top = jnp.maximum(top, m)
        f = jnp.exp2((s_new - top) * scale2)
        o = f * vn_rows[r, :]
        l = f
        for x, m, ll in zip(outs, ms, ls):
            f = jnp.exp2((m - top) * scale2)
            o = o + f * x[:, :head]
            l = l + f * ll
        merged[pl.ds(pl.multiple_of(g * pair_rows, 8), pair_rows), :] = o / l
        return carry

    lax.fori_loop(0, n_groups, merge_step, 0)
    attn = jnp.concatenate(
        [merged[pl.ds(n, own, stride=n_heads), :].astype(jnp.bfloat16) for n in range(n_heads)], axis=1)
    wo_copy.wait()
    for c in range(0, d_model, 512):
        proj[:, c:c + 512] = jnp.dot(attn, wo[:, c:c + 512], preferred_element_type=jnp.float32)

    swap = pltpu.make_async_remote_copy(proj, proj_in, proj_send, proj_recv,
                                        device_id={'tp': 1 - tp}, device_id_type=MESH)
    swap.start()
    swap.wait()
    sums[sp] = proj[...] + proj_in[...]

    def sum_copy(s):
        return pltpu.make_async_remote_copy(
            src_ref=sums.at[sp], dst_ref=sums.at[sp],
            send_sem=sum_send.at[s - 1], recv_sem=sum_recv.at[s - 1],
            device_id={'sp': lax.rem(sp + s, N_SP)}, device_id_type=MESH)

    for s in range(1, N_SP):
        sum_copy(s).start()
    for s in range(1, N_SP):
        sum_copy(s).wait()

    srow = lax.broadcasted_iota(jnp.int32, (GROUP, 1), 0)
    for g in range(n_groups):
        t = (2 * g) // GROUP * GROUP
        total = hidden[g * GROUP:(g + 1) * GROUP, :].astype(jnp.float32)
        gathered = jnp.zeros_like(total)
        for d in range(N_SP):
            x = sums[d, t:t + GROUP, :]
            shift = (2 * d - 2 * g) % GROUP
            if shift:
                x = pltpu.roll(x, shift, 0)
            gathered = jnp.where(srow // 2 == d, x, gathered)
        h_out[g * GROUP:(g + 1) * GROUP, :] = (total + gathered).astype(jnp.bfloat16)


def write_kernel(dims, pos, h_in, k_vm, v_vm, new_k, new_v, k_in, v_in, h_out, k_out, v_out,
                 slots, k_tile, v_tile, h_sem, rd_sem, wr_sem, k_sem, v_sem, k_row, v_row):
    n_seq, rows, kv, _, _, _ = dims
    sp = lax.axis_index('sp')
    seq_local = rows // kv
    n_held = HELD * GROUP
    per = 16 // kv
    sub = lax.broadcasted_iota(jnp.int32, (16, 1), 0) // kv
    held = ((k_vm, k_out, new_k, k_tile, k_sem, k_row), (v_vm, v_out, new_v, v_tile, v_sem, v_row))
    jobs = [(src, out, new, b) for src, out, new in ((k_in, k_out, new_k), (v_in, v_out, new_v))
            for b in range(n_held, n_seq, JOB)]

    def place(b):
        p = pos[b] - sp * seq_local
        blk = jnp.clip(p, 0, seq_local - 1) // per
        return pl.ds(pl.multiple_of(blk * 16, 16), 16), sub + blk * per == p

    def patched(ref, i, b, new):
        r, hit = place(b)
        fresh = new[pl.ds(pl.multiple_of(b * 16, 16), 16), :]
        return r, jnp.where(hit, fresh, ref[i, r, :].astype(jnp.float32)).astype(jnp.bfloat16)

    def read(j):
        src, _, _, b = jobs[j]
        return pltpu.make_async_copy(src.at[pl.ds(b, JOB)], slots.at[j % SLOTS], rd_sem.at[j])

    def write(j):
        _, out, _, b = jobs[j]
        return pltpu.make_async_copy(slots.at[j % SLOTS], out.at[pl.ds(b, JOB)], wr_sem.at[j])

    def block(vm, out, sem, g):
        s = pl.ds(g * GROUP, GROUP)
        return pltpu.make_async_copy(vm.at[s], out.at[s], sem.at[g])

    def run(j):
        _, _, new, b = jobs[j]
        slot = slots.at[j % SLOTS]
        read(j).wait()
        for i in range(JOB):
            r, x = patched(slot, i, b + i, new)
            slot[i, r, :] = x
        write(j).start()

    h_copy = pltpu.make_async_copy(h_in, h_out, h_sem)
    h_copy.start()
    for j in range(SLOTS):
        read(j).start()
    for vm, out, _, _, sem, _ in held:
        for g in range(HELD):
            block(vm, out, sem, g).start()
    for vm, _, new, tile, _, _ in held:
        def fill(b, carry):
            _, tile[b] = patched(vm, b, b, new)
            return carry

        lax.fori_loop(0, n_held, fill, 0)
    for j in range(len(jobs)):
        if j >= SLOTS:
            write(j - SLOTS).wait()
            read(j).start()
        if j < SLOTS:
            run(j)

    def row_copy(tile, out, row, b):
        r, _ = place(b)
        return pltpu.make_async_copy(tile.at[b], out.at[b, r], row.at[b])

    for n, (vm, out, _, tile, sem, row) in enumerate(held):
        def rows_out(g, carry):
            block(vm, out, sem, g).wait()
            for i in range(GROUP):
                row_copy(tile, out, row, g * GROUP + i).start()
            return carry

        lax.fori_loop(0, HELD, rows_out, 0)
        if n == 0:
            for j in range(SLOTS, len(jobs)):
                run(j)
    for _, out, _, tile, _, row in held:
        def drain(b, carry):
            row_copy(tile, out, row, b).wait()
            return carry

        lax.fori_loop(0, n_held, drain, 0)
    for j in range(SLOTS, len(jobs)):
        write(j).wait()
    h_copy.wait()


def solution(mesh):
    cache_spec = P('dp', 'sp', 'tp', None)

    def local_step(hidden, norm_scale, w_qkv, w_out, k_cache, v_cache, positions):
        n_seq, seq_local, kv, head = k_cache.shape
        d_model = hidden.shape[1]
        per_kv = w_qkv.shape[1] // (kv * head) - 2
        rows = seq_local * kv
        n_heads = kv * per_kv
        n_groups = n_seq // GROUP
        pair_rows = 2 * n_heads
        own = n_seq // N_SP
        n_jobs = 2 * (n_seq - HELD * GROUP) // JOB
        dims = (n_seq, rows, kv, head, per_kv, d_model)
        half = np.arange(head) % (head // 2)
        inv_freq = np.exp(half * (-2.0 * math.log(500000.0) / head)).astype(np.float32)
        sign = np.where(np.arange(head) < head // 2, -1.0, 1.0).astype(np.float32)
        angles = positions.astype(jnp.float32)[:, None] * inv_freq[None, :]
        cos2, sin2 = jnp.cos(angles), jnp.sin(angles) * sign
        f32, bf16 = jnp.float32, jnp.bfloat16
        vmem = pl.BlockSpec(memory_space=pltpu.VMEM)
        hbm = pl.BlockSpec(memory_space=pltpu.HBM)
        smem = pl.BlockSpec(memory_space=pltpu.SMEM)
        cache = (n_seq, rows, head)
        dma = pltpu.SemaphoreType.DMA
        keep = pltpu.with_memory_space_constraint
        w_qkv, w_out = keep(w_qkv, pltpu.HBM), keep(w_out, pltpu.HBM)
        k_flat = keep(k_cache.reshape(cache), pltpu.HBM)
        v_flat = keep(v_cache.reshape(cache), pltpu.HBM)
        h_vm, k_vm, v_vm, new_k, new_v = pl.pallas_call(
            lambda *refs: attend_kernel(dims, *refs),
            out_shape=(pltpu.VMEM(hidden.shape, bf16),
                       pltpu.VMEM((HELD * GROUP, rows, head), bf16),
                       pltpu.VMEM((HELD * GROUP, rows, head), bf16),
                       pltpu.VMEM((n_seq * 16, head), f32),
                       pltpu.VMEM((n_seq * 16, head), f32)),
            in_specs=[smem, vmem, vmem, vmem, vmem, hbm, hbm, hbm, hbm],
            out_specs=(vmem,) * 5,
            scratch_shapes=[
                pltpu.VMEM((W_CHUNKS, n_seq, d_model // W_CHUNKS), bf16),
                pltpu.VMEM((W_SLOTS, d_model // W_CHUNKS, w_qkv.shape[1]), bf16),
                pltpu.VMEM((n_seq, w_qkv.shape[1]), f32),
                pltpu.VMEM(w_out.shape, bf16),
                pltpu.VMEM((n_seq - HELD * GROUP, rows, head), bf16),
                pltpu.VMEM((n_seq - HELD * GROUP, rows, head), bf16),
                pltpu.VMEM((n_seq * n_heads, head), f32),
                pltpu.VMEM((n_seq * n_heads, head), f32),
                pltpu.VMEM((n_seq * n_heads, head), f32),
                pltpu.VMEM((pair_rows, rows), jnp.int32),
                pltpu.VMEM((n_groups, N_SP, pair_rows, 2 * head), f32),
                pltpu.VMEM((n_groups, N_SP - 1, pair_rows, 2 * head), f32),
                pltpu.VMEM((own * n_heads, head), f32),
                pltpu.VMEM((own, d_model), f32),
                pltpu.VMEM((own, d_model), f32),
                pltpu.VMEM((N_SP, own, d_model), f32),
                dma((W_CHUNKS,)), dma, dma((n_groups,)), dma((n_groups,)),
                dma((n_groups, N_SP - 1)), dma((n_groups, N_SP - 1)),
                dma, dma, dma((N_SP - 1,)), dma((N_SP - 1,)),
            ],
            compiler_params=pltpu.CompilerParams(
                collective_id=0, has_side_effects=True, vmem_limit_bytes=33 * MIB),
            name='attend',
        )(positions, hidden, norm_scale.reshape(1, d_model), cos2, sin2, w_qkv, w_out, k_flat, v_flat)
        h_out, k_out, v_out = pl.pallas_call(
            lambda *refs: write_kernel(dims, *refs),
            out_shape=(jax.ShapeDtypeStruct(hidden.shape, bf16),
                       jax.ShapeDtypeStruct(cache, bf16), jax.ShapeDtypeStruct(cache, bf16)),
            in_specs=[smem] + [vmem] * 5 + [hbm] * 2,
            out_specs=(hbm,) * 3,
            scratch_shapes=[
                pltpu.VMEM((SLOTS, JOB, rows, head), bf16),
                pltpu.VMEM((HELD * GROUP, 16, head), bf16),
                pltpu.VMEM((HELD * GROUP, 16, head), bf16),
                dma, dma((n_jobs,)), dma((n_jobs,)), dma((HELD,)), dma((HELD,)),
                dma((HELD * GROUP,)), dma((HELD * GROUP,)),
            ],
            compiler_params=pltpu.CompilerParams(vmem_limit_bytes=W_VMEM * MIB),
            name='write',
        )(positions, *[keep(x, pltpu.VMEM) for x in (h_vm, k_vm, v_vm, new_k, new_v)], k_flat, v_flat)
        return h_out, k_out.reshape(k_cache.shape), v_out.reshape(v_cache.shape)

    return jax.shard_map(
        local_step,
        mesh=mesh,
        in_specs=(P('dp', None), P(None), P(None, 'tp'), P('tp', None), cache_spec, cache_spec, P('dp')),
        out_specs=(P('dp', None), cache_spec, cache_spec),
        check_vma=False,
    )
```

```python
import math
import jax
import jax.numpy as jnp
import numpy as np
from jax import lax
from jax.experimental import pallas as pl
from jax.experimental.pallas import tpu as pltpu
from jax.sharding import PartitionSpec as P

MESH = pl.DeviceIdType.MESH
NEG = -1e30
MIB = 1024 * 1024
N_SP = 4
GROUP = 8
W_CHUNKS = 6
W_SLOTS = 3
AHEAD = 3
HELD = 7
JOB = 2
SLOTS = 4
WINDOW = 4
W_VMEM = 3


def attend_kernel(dims, pos, hidden, norm_scale, inv_freq, w_qkv, w_out, k_in, v_in,
                  h_out, k_vm, v_vm, new_k, new_v,
                  u, wq, acc, rope_c, rope_s, wo, k_rest, v_rest, q_rows, kn_rows, vn_rows, tok, part, recv, merged, proj, proj_in, sums,
                  w_sem, wo_sem, k_sem, v_sem, part_send, part_recv, proj_send, proj_recv, sum_send, sum_recv):
    n_seq, rows, kv, head, per_kv, d_model = dims
    n_heads = kv * per_kv
    n_groups = n_seq // GROUP
    pair_rows = 2 * n_heads
    own = n_seq // N_SP
    w_rows = d_model // W_CHUNKS
    sp = lax.axis_index('sp')
    tp = lax.axis_index('tp')
    seq_local = rows // kv
    scale2 = head ** -0.5 * math.log2(math.e)

    def w_copy(c):
        return pltpu.make_async_copy(w_qkv.at[pl.ds(c * w_rows, w_rows)], wq.at[c % W_SLOTS], w_sem.at[c])

    def held(ref, rest, n_held, g):
        return (ref, g) if g < n_held else (rest, g - n_held)

    def cache_copy(src, ref, rest, n_held, sem, g):
        dst, i = held(ref, rest, n_held, g)
        return pltpu.make_async_copy(src.at[pl.ds(g * GROUP, GROUP)], dst.at[pl.ds(i * GROUP, GROUP)], sem.at[g])

    def k_copy(g):
        return cache_copy(k_in, k_vm, k_rest, HELD, k_sem, g)

    def v_copy(g):
        return cache_copy(v_in, v_vm, v_rest, HELD, v_sem, g)

    def fetch(g):
        k_copy(g).start()
        v_copy(g).start()

    wo_copy = pltpu.make_async_copy(w_out, wo, wo_sem)
    for c in range(W_SLOTS):
        w_copy(c).start()

    barrier = pltpu.get_barrier_semaphore()
    for s in range(1, N_SP):
        pl.semaphore_signal(barrier, inc=1, device_id={'sp': lax.rem(sp + s, N_SP)}, device_id_type=MESH)
    pl.semaphore_signal(barrier, inc=1, device_id={'tp': 1 - tp}, device_id_type=MESH)

    hid = hidden[...].astype(jnp.float32)
    mean = jnp.mean(hid, axis=-1, keepdims=True)
    cen = hid - mean
    var = jnp.mean(cen * cen, axis=-1, keepdims=True)
    scale_rows = norm_scale[...].astype(jnp.float32)
    scale_row = jnp.concatenate([scale_rows[i:i + 1] for i in range(scale_rows.shape[0])], axis=1)
    normed = (cen * lax.rsqrt(var + 1e-5) * scale_row).astype(jnp.bfloat16)
    for c in range(W_CHUNKS):
        u[c] = normed[:, c * w_rows:(c + 1) * w_rows]

    col = lax.broadcasted_iota(jnp.int32, (pair_rows, rows), 1)
    row = lax.broadcasted_iota(jnp.int32, (pair_rows, rows), 0)
    row_kv = lax.rem(row, n_heads) // per_kv
    tok[...] = jnp.where(lax.rem(col, kv) == row_kv, sp * seq_local + col // kv, 1 << 30)

    acc[...] = jnp.zeros_like(acc)

    brow = lax.broadcasted_iota(jnp.int32, (n_seq, 1), 0)
    pos_col = jnp.zeros((n_seq, 1), jnp.int32)
    for b in range(n_seq):
        pos_col = jnp.where(brow == b, pos[b], pos_col)
    angles = pos_col.astype(jnp.float32) * inv_freq[...]
    c2 = jnp.cos(angles)
    s2 = jnp.sin(angles)
    s2 = jnp.where(lax.broadcasted_iota(jnp.int32, s2.shape, 1) < head // 2, -s2, s2)
    rope_c[...] = c2
    rope_s[...] = s2

    for c in range(W_CHUNKS):
        w_copy(c).wait()
        acc[...] += jnp.dot(u[c], wq[c % W_SLOTS], preferred_element_type=jnp.float32)
        if c + W_SLOTS < W_CHUNKS:
            w_copy(c + W_SLOTS).start()
        else:
            fetch(c + W_SLOTS - W_CHUNKS)

    c2 = rope_c[...]
    s2 = rope_s[...]
    for g in range(kv):
        for j in range(per_kv + 2):
            lo = (g * (per_kv + 2) + j) * head
            x = jnp.clip(acc[:, lo:lo + head].astype(jnp.bfloat16).astype(jnp.float32), -8.0, 8.0)
            if j <= per_kv:
                x = (x * c2 + pltpu.roll(x, head // 2, 1) * s2).astype(jnp.bfloat16).astype(jnp.float32)
            if j < per_kv:
                q_rows[pl.ds(g * per_kv + j, n_seq, stride=n_heads), :] = x
            else:
                wide, rep = (kn_rows, new_k) if j == per_kv else (vn_rows, new_v)
                for i in range(per_kv):
                    wide[pl.ds(g * per_kv + i, n_seq, stride=n_heads), :] = x
                for i in range(16 // kv):
                    rep[pl.ds(i * kv + g, n_seq, stride=16), :] = x

    pl.semaphore_wait(barrier, N_SP)

    prow = lax.broadcasted_iota(jnp.int32, (pair_rows, 1), 0)
    first = prow < n_heads

    def part_copy(g, s):
        dst = lax.rem(sp + s, N_SP)
        return pltpu.make_async_remote_copy(
            src_ref=part.at[g, dst], dst_ref=recv.at[g, s - 1],
            send_sem=part_send.at[g, s - 1], recv_sem=part_recv.at[g, s - 1],
            device_id={'sp': dst}, device_id_type=MESH)

    def group_step(g, k_ref, v_ref, k_off, v_off):
        for d in range(N_SP):
            b = g * GROUP + 2 * d
            kb, vb = b - k_off, b - v_off
            q = q_rows[pl.ds(pl.multiple_of((g * N_SP + d) * pair_rows, 8), pair_rows), :]
            zero = jnp.zeros_like(q)
            q_blk = jnp.concatenate([jnp.where(first, q, zero), jnp.where(first, zero, q)], axis=1).astype(jnp.bfloat16)
            k_cat = jnp.concatenate([k_ref[kb], k_ref[kb + 1]], axis=1)
            s = lax.dot_general(q_blk, k_cat, (((1,), (1,)), ((), ())), preferred_element_type=jnp.float32)
            limit = jnp.where(first, pos[b], pos[b + 1])
            s = jnp.where(tok[...] < limit, s, NEG)
            m = jnp.max(s, axis=-1, keepdims=True)
            w = jnp.exp2((s - m) * scale2)
            l = jnp.sum(w, axis=-1, keepdims=True)
            v_cat = jnp.concatenate([v_ref[vb], v_ref[vb + 1]], axis=1)
            o = jnp.dot(w.astype(jnp.bfloat16), v_cat, preferred_element_type=jnp.float32)
            part[g, d, :, :head] = jnp.where(first, o[:, :head], o[:, head:])
            lane = lax.broadcasted_iota(jnp.int32, (pair_rows, head), 1)
            part[g, d, :, head:] = jnp.where(lane < head // 2, m, l)
        for s in range(1, N_SP):
            part_copy(g, s).start()

    def held_step(g, carry):
        for src, dst, sem in ((k_in, k_vm, k_sem), (v_in, v_vm, v_sem)):
            now, later = pl.ds(g * GROUP, GROUP), pl.ds((g + AHEAD) * GROUP, GROUP)
            pltpu.make_async_copy(src.at[now], dst.at[now], sem.at[g]).wait()
            pltpu.make_async_copy(src.at[later], dst.at[later], sem.at[g + AHEAD]).start()
        group_step(g, k_vm, v_vm, 0, 0)
        return carry

    lax.fori_loop(0, HELD - AHEAD, held_step, 0)
    for g in range(HELD - AHEAD, n_groups):
        k_copy(g).wait()
        v_copy(g).wait()
        if g + AHEAD < n_groups:
            fetch(g + AHEAD)
        elif g + AHEAD == n_groups:
            wo_copy.start()
        k_ref, ki = held(k_vm, k_rest, HELD, g)
        v_ref, vi = held(v_vm, v_rest, HELD, g)
        group_step(g, k_ref, v_ref, (g - ki) * GROUP, (g - vi) * GROUP)

    def merge_step(g, carry):
        for s in range(1, N_SP):
            part_copy(g, s).wait()
        r = pl.ds(pl.multiple_of((g * N_SP + sp) * pair_rows, 8), pair_rows)
        s_new = jnp.sum(q_rows[r, :] * kn_rows[r, :], axis=-1, keepdims=True)
        outs = [part[g, sp]] + [recv[g, s] for s in range(N_SP - 1)]
        ms = [x[:, head:head + 1] for x in outs]
        ls = [x[:, head + head // 2:head + head // 2 + 1] for x in outs]
        top = s_new
        for m in ms:
            top = jnp.maximum(top, m)
        f = jnp.exp2((s_new - top) * scale2)
        o = f * vn_rows[r, :]
        l = f
        for x, m, ll in zip(outs, ms, ls):
            f = jnp.exp2((m - top) * scale2)
            o = o + f * x[:, :head]
            l = l + f * ll
        merged[pl.ds(pl.multiple_of(g * pair_rows, 8), pair_rows), :] = o / l
        return carry

    lax.fori_loop(0, n_groups, merge_step, 0)
    attn = jnp.concatenate(
        [merged[pl.ds(n, own, stride=n_heads), :].astype(jnp.bfloat16) for n in range(n_heads)], axis=1)
    wo_copy.wait()
    for c in range(0, d_model, 512):
        proj[:, c:c + 512] = jnp.dot(attn, wo[:, c:c + 512], preferred_element_type=jnp.float32)

    swap = pltpu.make_async_remote_copy(proj, proj_in, proj_send, proj_recv,
                                        device_id={'tp': 1 - tp}, device_id_type=MESH)
    swap.start()
    swap.wait()
    sums[sp] = proj[...] + proj_in[...]

    def sum_copy(s):
        return pltpu.make_async_remote_copy(
            src_ref=sums.at[sp], dst_ref=sums.at[sp],
            send_sem=sum_send.at[s - 1], recv_sem=sum_recv.at[s - 1],
            device_id={'sp': lax.rem(sp + s, N_SP)}, device_id_type=MESH)

    for s in range(1, N_SP):
        sum_copy(s).start()
    for s in range(1, N_SP):
        sum_copy(s).wait()

    srow = lax.broadcasted_iota(jnp.int32, (GROUP, 1), 0)
    for g in range(n_groups):
        t = (2 * g) // GROUP * GROUP
        total = hidden[g * GROUP:(g + 1) * GROUP, :].astype(jnp.float32)
        gathered = jnp.zeros_like(total)
        for d in range(N_SP):
            x = sums[d, t:t + GROUP, :]
            shift = (2 * d - 2 * g) % GROUP
            if shift:
                x = pltpu.roll(x, shift, 0)
            gathered = jnp.where(srow // 2 == d, x, gathered)
        h_out[g * GROUP:(g + 1) * GROUP, :] = (total + gathered).astype(jnp.bfloat16)


def write_kernel(dims, pos, h_in, k_vm, v_vm, new_k, new_v, k_in, v_in, h_out, k_out, v_out, k_same, v_same,
                 slots, h_sem, rd_sem, wr_sem, blk_sem):
    n_seq, rows, kv, _, _, _ = dims
    sp = lax.axis_index('sp')
    seq_local = rows // kv
    n_held = HELD * GROUP
    per = 16 // kv
    sub = lax.broadcasted_iota(jnp.int32, (16, 1), 0) // kv
    jobs = [(src, out, new, b) for src, out, new in ((k_in, k_out, new_k), (v_in, v_out, new_v))
            for b in range(n_held, n_seq, JOB)]

    def patch(ref, i, b, new):
        p = pos[b] - sp * seq_local
        blk = jnp.clip(p, 0, seq_local - 1) // per
        r = pl.ds(pl.multiple_of(blk * 16, 16), 16)
        fresh = new[pl.ds(pl.multiple_of(b * 16, 16), 16), :]
        ref[i, r, :] = jnp.where(sub + blk * per == p, fresh, ref[i, r, :].astype(jnp.float32)).astype(jnp.bfloat16)

    def read(j):
        src, _, _, b = jobs[j]
        return pltpu.make_async_copy(src.at[pl.ds(b, JOB)], slots.at[j % SLOTS], rd_sem.at[j])

    def write(j):
        _, out, _, b = jobs[j]
        return pltpu.make_async_copy(slots.at[j % SLOTS], out.at[pl.ds(b, JOB)], wr_sem.at[j])

    def run(j):
        _, _, new, b = jobs[j]
        read(j).wait()
        for i in range(JOB):
            patch(slots.at[j % SLOTS], i, b + i, new)
        write(j).start()

    def again(j):
        write(j - SLOTS).wait()
        read(j).start()

    def block(n):
        vm, out = ((k_vm, k_out), (v_vm, v_out))[n % 2]
        s = pl.ds(n // 2 * GROUP, GROUP)
        return pltpu.make_async_copy(vm.at[s], out.at[s], blk_sem.at[n])

    def send(n):
        vm, new = ((k_vm, new_k), (v_vm, new_v))[n % 2]
        for i in range(GROUP):
            b = n // 2 * GROUP + i
            patch(vm, b, b, new)
        block(n).start()

    n_blocks = 2 * HELD
    h_copy = pltpu.make_async_copy(h_in, h_out, h_sem)
    h_copy.start()
    for j in range(SLOTS):
        read(j).start()
    for n in range(n_blocks):
        if n >= WINDOW:
            block(n - WINDOW).wait()
        send(n)
        for j in range(len(jobs)):
            if j < SLOTS and n == WINDOW + j // 2 - 1:
                run(j)
            if j >= SLOTS and n == WINDOW + 2 + j // 2:
                again(j)
            if j >= SLOTS and n == WINDOW + 4 + j // 2:
                run(j)
    for n in range(n_blocks - WINDOW, n_blocks):
        block(n).wait()
    for j in range(len(jobs) - SLOTS, len(jobs)):
        write(j).wait()
    h_copy.wait()


def solution(mesh):
    cache_spec = P('dp', 'sp', 'tp', None)

    def local_step(hidden, norm_scale, w_qkv, w_out, k_cache, v_cache, positions):
        n_seq, seq_local, kv, head = k_cache.shape
        d_model = hidden.shape[1]
        per_kv = w_qkv.shape[1] // (kv * head) - 2
        rows = seq_local * kv
        n_heads = kv * per_kv
        n_groups = n_seq // GROUP
        pair_rows = 2 * n_heads
        own = n_seq // N_SP
        n_jobs = 2 * (n_seq - HELD * GROUP) // JOB
        dims = (n_seq, rows, kv, head, per_kv, d_model)
        half = np.arange(head) % (head // 2)
        inv_freq = np.exp(half * (-2.0 * math.log(500000.0) / head)).astype(np.float32)[None]
        f32, bf16 = jnp.float32, jnp.bfloat16
        vmem = pl.BlockSpec(memory_space=pltpu.VMEM)
        hbm = pl.BlockSpec(memory_space=pltpu.HBM)
        smem = pl.BlockSpec(memory_space=pltpu.SMEM)
        cache = (n_seq, rows, head)
        dma = pltpu.SemaphoreType.DMA
        keep = pltpu.with_memory_space_constraint
        w_qkv, w_out = keep(w_qkv, pltpu.HBM), keep(w_out, pltpu.HBM)
        k_flat = keep(k_cache.reshape(cache), pltpu.HBM)
        v_flat = keep(v_cache.reshape(cache), pltpu.HBM)
        h_vm, k_vm, v_vm, new_k, new_v = pl.pallas_call(
            lambda *refs: attend_kernel(dims, *refs),
            out_shape=(pltpu.VMEM(hidden.shape, bf16),
                       pltpu.VMEM((HELD * GROUP, rows, head), bf16),
                       pltpu.VMEM((HELD * GROUP, rows, head), bf16),
                       pltpu.VMEM((n_seq * 16, head), f32),
                       pltpu.VMEM((n_seq * 16, head), f32)),
            in_specs=[smem, vmem, vmem, vmem, hbm, hbm, hbm, hbm],
            out_specs=(vmem,) * 5,
            scratch_shapes=[
                pltpu.VMEM((W_CHUNKS, n_seq, d_model // W_CHUNKS), bf16),
                pltpu.VMEM((W_SLOTS, d_model // W_CHUNKS, w_qkv.shape[1]), bf16),
                pltpu.VMEM((n_seq, w_qkv.shape[1]), f32),
                pltpu.VMEM((n_seq, head), f32),
                pltpu.VMEM((n_seq, head), f32),
                pltpu.VMEM(w_out.shape, bf16),
                pltpu.VMEM((n_seq - HELD * GROUP, rows, head), bf16),
                pltpu.VMEM((n_seq - HELD * GROUP, rows, head), bf16),
                pltpu.VMEM((n_seq * n_heads, head), f32),
                pltpu.VMEM((n_seq * n_heads, head), f32),
                pltpu.VMEM((n_seq * n_heads, head), f32),
                pltpu.VMEM((pair_rows, rows), jnp.int32),
                pltpu.VMEM((n_groups, N_SP, pair_rows, 2 * head), f32),
                pltpu.VMEM((n_groups, N_SP - 1, pair_rows, 2 * head), f32),
                pltpu.VMEM((own * n_heads, head), f32),
                pltpu.VMEM((own, d_model), f32),
                pltpu.VMEM((own, d_model), f32),
                pltpu.VMEM((N_SP, own, d_model), f32),
                dma((W_CHUNKS,)), dma, dma((n_groups,)), dma((n_groups,)),
                dma((n_groups, N_SP - 1)), dma((n_groups, N_SP - 1)),
                dma, dma, dma((N_SP - 1,)), dma((N_SP - 1,)),
            ],
            compiler_params=pltpu.CompilerParams(
                collective_id=0, has_side_effects=True, vmem_limit_bytes=33 * MIB),
            name='attend',
        )(positions, hidden, norm_scale.reshape(d_model // 128, 128), inv_freq, w_qkv, w_out, k_flat, v_flat)
        h_out, k_out, v_out, _, _ = pl.pallas_call(
            lambda *refs: write_kernel(dims, *refs),
            out_shape=(jax.ShapeDtypeStruct(hidden.shape, bf16),
                       jax.ShapeDtypeStruct(cache, bf16), jax.ShapeDtypeStruct(cache, bf16),
                       pltpu.VMEM(k_vm.shape, bf16), pltpu.VMEM(v_vm.shape, bf16)),
            in_specs=[smem] + [vmem] * 5 + [hbm] * 2,
            out_specs=(hbm,) * 3 + (vmem,) * 2,
            input_output_aliases={2: 3, 3: 4},
            scratch_shapes=[
                pltpu.VMEM((SLOTS, JOB, rows, head), bf16),
                dma, dma((n_jobs,)), dma((n_jobs,)), dma((2 * HELD,)),
            ],
            compiler_params=pltpu.CompilerParams(vmem_limit_bytes=W_VMEM * MIB),
            name='write',
        )(positions, *[keep(x, pltpu.VMEM) for x in (h_vm, k_vm, v_vm, new_k, new_v)], k_flat, v_flat)
        return h_out, k_out.reshape(k_cache.shape), v_out.reshape(v_cache.shape)

    return jax.shard_map(
        local_step,
        mesh=mesh,
        in_specs=(P('dp', None), P(None), P(None, 'tp'), P('tp', None), cache_spec, cache_spec, P('dp')),
        out_specs=(P('dp', None), cache_spec, cache_spec),
        check_vma=False,
    )
```

```python
import math
import jax
import jax.numpy as jnp
import numpy as np
from jax import lax
from jax.experimental import pallas as pl
from jax.experimental.pallas import tpu as pltpu
from jax.sharding import PartitionSpec as P

MESH = pl.DeviceIdType.MESH
NEG = -1e30
MIB = 1024 * 1024
N_SP = 4
COLS = 4
WO_AT = 7
GROUP = 8
W_CHUNKS = 6
W_SLOTS = 3
AHEAD = 3
HELD = 7
JOB = 2
SLOTS = 4
WINDOW = 4
W_VMEM = 3


def attend_kernel(dims, pos, hidden, norm_scale, inv_freq, w_qkv, w_out, k_in, v_in,
                  h_out, k_vm, v_vm, new_k, new_v,
                  u, wq, acc, rope_c, rope_s, wo, k_rest, v_rest, q_rows, kn_rows, vn_rows, tok, score, part, recv, merged, proj, proj_in, sums,
                  w_sem, wo_sem, k_sem, v_sem, part_send, part_recv, tp_send, tp_recv, x_send, x_recv,
                  core_send, core_recv, fwd_send, fwd_recv):
    n_seq, rows, kv, head, per_kv, d_model = dims
    n_heads = kv * per_kv
    n_groups = n_seq // GROUP
    pair_rows = 2 * n_heads
    own = n_seq // N_SP
    w_rows = d_model // W_CHUNKS
    sp = lax.axis_index('sp')
    tp = lax.axis_index('tp')
    seq_local = rows // kv
    scale2 = head ** -0.5 * math.log2(math.e)

    def w_copy(c):
        return pltpu.make_async_copy(w_qkv.at[pl.ds(c * w_rows, w_rows)], wq.at[c % W_SLOTS], w_sem.at[c])

    def held(ref, rest, n_held, g):
        return (ref, g) if g < n_held else (rest, g - n_held)

    def cache_copy(src, ref, rest, n_held, sem, g):
        dst, i = held(ref, rest, n_held, g)
        return pltpu.make_async_copy(src.at[pl.ds(g * GROUP, GROUP)], dst.at[pl.ds(i * GROUP, GROUP)], sem.at[g])

    def k_copy(g):
        return cache_copy(k_in, k_vm, k_rest, HELD, k_sem, g)

    def v_copy(g):
        return cache_copy(v_in, v_vm, v_rest, HELD, v_sem, g)

    def fetch(g):
        k_copy(g).start()
        v_copy(g).start()

    wo_copy = pltpu.make_async_copy(w_out, wo, wo_sem)
    for c in range(W_SLOTS):
        w_copy(c).start()

    barrier = pltpu.get_barrier_semaphore()
    for s in range(1, N_SP):
        pl.semaphore_signal(barrier, inc=1, device_id={'sp': lax.rem(sp + s, N_SP)}, device_id_type=MESH)
    pl.semaphore_signal(barrier, inc=1, device_id={'tp': 1 - tp}, device_id_type=MESH)

    hid = hidden[...].astype(jnp.float32)
    mean = jnp.mean(hid, axis=-1, keepdims=True)
    cen = hid - mean
    var = jnp.mean(cen * cen, axis=-1, keepdims=True)
    scale_rows = norm_scale[...].astype(jnp.float32)
    scale_row = jnp.concatenate([scale_rows[i:i + 1] for i in range(scale_rows.shape[0])], axis=1)
    normed = (cen * lax.rsqrt(var + 1e-5) * scale_row).astype(jnp.bfloat16)
    for c in range(W_CHUNKS):
        u[c] = normed[:, c * w_rows:(c + 1) * w_rows]

    col = lax.broadcasted_iota(jnp.int32, (pair_rows, rows), 1)
    row = lax.broadcasted_iota(jnp.int32, (pair_rows, rows), 0)
    row_kv = lax.rem(row, n_heads) // per_kv
    tok[...] = jnp.where(lax.rem(col, kv) == row_kv, sp * seq_local + col // kv, 1 << 30)

    acc[...] = jnp.zeros_like(acc)

    brow = lax.broadcasted_iota(jnp.int32, (n_seq, 1), 0)
    pos_col = jnp.zeros((n_seq, 1), jnp.int32)
    for b in range(n_seq):
        pos_col = jnp.where(brow == b, pos[b], pos_col)
    angles = pos_col.astype(jnp.float32) * inv_freq[...]
    c2 = jnp.cos(angles)
    s2 = jnp.sin(angles)
    s2 = jnp.where(lax.broadcasted_iota(jnp.int32, s2.shape, 1) < head // 2, -s2, s2)
    rope_c[...] = c2
    rope_s[...] = s2

    for c in range(W_CHUNKS):
        w_copy(c).wait()
        acc[...] += jnp.dot(u[c], wq[c % W_SLOTS], preferred_element_type=jnp.float32)
        if c + W_SLOTS < W_CHUNKS:
            w_copy(c + W_SLOTS).start()
        else:
            fetch(c + W_SLOTS - W_CHUNKS)

    c2 = rope_c[...]
    s2 = rope_s[...]
    for g in range(kv):
        for j in range(per_kv + 2):
            lo = (g * (per_kv + 2) + j) * head
            x = jnp.clip(acc[:, lo:lo + head].astype(jnp.bfloat16).astype(jnp.float32), -8.0, 8.0)
            if j <= per_kv:
                x = (x * c2 + pltpu.roll(x, head // 2, 1) * s2).astype(jnp.bfloat16).astype(jnp.float32)
            if j < per_kv:
                q_rows[pl.ds(g * per_kv + j, n_seq, stride=n_heads), :] = x
            else:
                wide, rep = (kn_rows, new_k) if j == per_kv else (vn_rows, new_v)
                for i in range(per_kv):
                    wide[pl.ds(g * per_kv + i, n_seq, stride=n_heads), :] = x
                for i in range(16 // kv):
                    rep[pl.ds(i * kv + g, n_seq, stride=16), :] = x

    pl.semaphore_wait(barrier, N_SP)

    prow = lax.broadcasted_iota(jnp.int32, (pair_rows, 1), 0)
    first = prow < n_heads

    def part_copy(g, s):
        dst = lax.rem(sp + s, N_SP)
        return pltpu.make_async_remote_copy(
            src_ref=part.at[g, dst], dst_ref=recv.at[g, s - 1],
            send_sem=part_send.at[g, s - 1], recv_sem=part_recv.at[g, s - 1],
            device_id={'sp': dst}, device_id_type=MESH)

    lane = lax.broadcasted_iota(jnp.int32, (8, head), 1)
    n_stat = pair_rows // 8

    def scores(g, k_ref, k_off):
        for d in range(N_SP):
            kb = g * GROUP + 2 * d - k_off
            q = q_rows[pl.ds(pl.multiple_of((g * N_SP + d) * pair_rows, 8), pair_rows), :]
            zero = jnp.zeros_like(q)
            q_blk = jnp.concatenate([jnp.where(first, q, zero), jnp.where(first, zero, q)], axis=1).astype(jnp.bfloat16)
            k_cat = jnp.concatenate([k_ref[kb], k_ref[kb + 1]], axis=1)
            score[d] = lax.dot_general(q_blk, k_cat, (((1,), (1,)), ((), ())), preferred_element_type=jnp.float32)

    def values(g, v_ref, v_off):
        for d in range(N_SP):
            b = g * GROUP + 2 * d
            vb = b - v_off
            limit = jnp.where(first, pos[b], pos[b + 1])
            s = jnp.where(tok[...] < limit, score[d], NEG)
            m = jnp.max(s, axis=-1, keepdims=True)
            w = jnp.exp2((s - m) * scale2)
            l = jnp.sum(w, axis=-1, keepdims=True)
            v_cat = jnp.concatenate([v_ref[vb], v_ref[vb + 1]], axis=1)
            o = jnp.dot(w.astype(jnp.bfloat16), v_cat, preferred_element_type=jnp.float32)
            part[g, d, :pair_rows] = jnp.where(first, o[:, :head], o[:, head:])
            stat = jnp.zeros((8, head), jnp.float32)
            for i in range(n_stat):
                stat = jnp.where(lane == i, m[8 * i:8 * i + 8], stat)
                stat = jnp.where(lane == n_stat + i, l[8 * i:8 * i + 8], stat)
            part[g, d, pair_rows:] = stat
        for s in range(1, N_SP):
            part_copy(g, s).start()

    def held_step(g, carry):
        now, later = pl.ds(g * GROUP, GROUP), pl.ds((g + AHEAD) * GROUP, GROUP)
        pltpu.make_async_copy(k_in.at[now], k_vm.at[now], k_sem.at[g]).wait()
        pltpu.make_async_copy(k_in.at[later], k_vm.at[later], k_sem.at[g + AHEAD]).start()
        scores(g, k_vm, 0)
        pltpu.make_async_copy(v_in.at[now], v_vm.at[now], v_sem.at[g]).wait()
        pltpu.make_async_copy(v_in.at[later], v_vm.at[later], v_sem.at[g + AHEAD]).start()
        values(g, v_vm, 0)
        return carry

    lax.fori_loop(0, HELD - AHEAD, held_step, 0)
    for g in range(HELD - AHEAD, n_groups):
        k_ref, ki = held(k_vm, k_rest, HELD, g)
        v_ref, vi = held(v_vm, v_rest, HELD, g)
        k_copy(g).wait()
        if g + AHEAD < n_groups:
            k_copy(g + AHEAD).start()
        scores(g, k_ref, (g - ki) * GROUP)
        v_copy(g).wait()
        if g + AHEAD < n_groups:
            v_copy(g + AHEAD).start()
        if g == WO_AT:
            wo_copy.start()
        values(g, v_ref, (g - vi) * GROUP)

    def merge_step(g, carry):
        for s in range(1, N_SP):
            part_copy(g, s).wait()
        r = pl.ds(pl.multiple_of((g * N_SP + sp) * pair_rows, 8), pair_rows)
        s_new = jnp.sum(q_rows[r, :] * kn_rows[r, :], axis=-1, keepdims=True)
        outs = [part[g, sp]] + [recv[g, s] for s in range(N_SP - 1)]

        def column(x, first_lane):
            return jnp.concatenate(
                [x[pair_rows:, first_lane + i:first_lane + i + 1] for i in range(n_stat)], axis=0)

        ms = [column(x, 0) for x in outs]
        ls = [column(x, n_stat) for x in outs]
        top = s_new
        for m in ms:
            top = jnp.maximum(top, m)
        f = jnp.exp2((s_new - top) * scale2)
        o = f * vn_rows[r, :]
        l = f
        for x, m, ll in zip(outs, ms, ls):
            f = jnp.exp2((m - top) * scale2)
            o = o + f * x[:pair_rows]
            l = l + f * ll
        merged[pl.ds(pl.multiple_of(g * pair_rows, 8), pair_rows), :] = o / l
        return carry

    lax.fori_loop(0, n_groups, merge_step, 0)
    attn = jnp.concatenate(
        [merged[pl.ds(n, own, stride=n_heads), :].astype(jnp.bfloat16) for n in range(n_heads)], axis=1)
    wo_copy.wait()
    width = d_model // COLS
    partner = sp + 1 - 2 * lax.rem(sp, 2)
    across = lax.rem(sp + 2, N_SP)

    def tp_copy(c):
        return pltpu.make_async_remote_copy(proj.at[c], proj_in.at[c], tp_send.at[c], tp_recv.at[c],
                                            device_id={'tp': 1 - tp}, device_id_type=MESH)

    def x_copy(c):
        return pltpu.make_async_remote_copy(sums.at[c, sp], sums.at[c, sp], x_send.at[c], x_recv.at[c],
                                            device_id={'sp': across}, device_id_type=MESH)

    def core_copy(c):
        return pltpu.make_async_remote_copy(sums.at[c, sp], sums.at[c, sp], core_send.at[c], core_recv.at[c],
                                            device_id={'sp': partner}, device_id_type=MESH)

    def fwd_copy(c):
        return pltpu.make_async_remote_copy(sums.at[c, across], sums.at[c, across], fwd_send.at[c], fwd_recv.at[c],
                                            device_id={'sp': partner}, device_id_type=MESH)

    for c in range(COLS):
        proj[c] = jnp.dot(attn, wo[:, c * width:(c + 1) * width], preferred_element_type=jnp.float32)
        tp_copy(c).start()
    for c in range(COLS):
        tp_copy(c).wait()
        sums[c, sp] = proj[c] + proj_in[c]
        x_copy(c).start()
        core_copy(c).start()
    for c in range(COLS):
        x_copy(c).wait()
        fwd_copy(c).start()

    srow = lax.broadcasted_iota(jnp.int32, (GROUP, 1), 0)
    for c in range(COLS):
        core_copy(c).wait()
        fwd_copy(c).wait()
        lanes = slice(c * width, (c + 1) * width)
        for g in range(n_groups):
            t = (2 * g) // GROUP * GROUP
            gathered = None
            for d in range(N_SP):
                x = sums[c, d, t:t + GROUP, :]
                shift = (2 * d - 2 * g) % GROUP
                if shift:
                    x = pltpu.roll(x, shift, 0)
                gathered = x if gathered is None else jnp.where(srow // 2 == d, x, gathered)
            r = slice(g * GROUP, (g + 1) * GROUP)
            h_out[r, lanes] = (hidden[r, lanes].astype(jnp.float32) + gathered).astype(jnp.bfloat16)


def write_kernel(dims, pos, h_in, k_vm, v_vm, new_k, new_v, k_in, v_in, h_out, k_out, v_out, k_same, v_same,
                 slots, h_sem, rd_sem, wr_sem, blk_sem):
    n_seq, rows, kv, _, _, _ = dims
    sp = lax.axis_index('sp')
    seq_local = rows // kv
    n_held = HELD * GROUP
    per = 16 // kv
    sub = lax.broadcasted_iota(jnp.int32, (16, 1), 0) // kv
    jobs = [(src, out, new, b) for src, out, new in ((k_in, k_out, new_k), (v_in, v_out, new_v))
            for b in range(n_held, n_seq, JOB)]

    def patch(ref, i, b, new):
        p = pos[b] - sp * seq_local
        blk = jnp.clip(p, 0, seq_local - 1) // per
        r = pl.ds(pl.multiple_of(blk * 16, 16), 16)
        fresh = new[pl.ds(pl.multiple_of(b * 16, 16), 16), :]
        ref[i, r, :] = jnp.where(sub + blk * per == p, fresh, ref[i, r, :].astype(jnp.float32)).astype(jnp.bfloat16)

    def read(j):
        src, _, _, b = jobs[j]
        return pltpu.make_async_copy(src.at[pl.ds(b, JOB)], slots.at[j % SLOTS], rd_sem.at[j])

    def write(j):
        _, out, _, b = jobs[j]
        return pltpu.make_async_copy(slots.at[j % SLOTS], out.at[pl.ds(b, JOB)], wr_sem.at[j])

    def run(j):
        _, _, new, b = jobs[j]
        read(j).wait()
        for i in range(JOB):
            patch(slots.at[j % SLOTS], i, b + i, new)
        write(j).start()

    def again(j):
        write(j - SLOTS).wait()
        read(j).start()

    def block(n):
        vm, out = ((k_vm, k_out), (v_vm, v_out))[n % 2]
        s = pl.ds(n // 2 * GROUP, GROUP)
        return pltpu.make_async_copy(vm.at[s], out.at[s], blk_sem.at[n])

    def send(n):
        vm, new = ((k_vm, new_k), (v_vm, new_v))[n % 2]
        for i in range(GROUP):
            b = n // 2 * GROUP + i
            patch(vm, b, b, new)
        block(n).start()

    n_blocks = 2 * HELD
    h_copy = pltpu.make_async_copy(h_in, h_out, h_sem)
    h_copy.start()
    for j in range(SLOTS):
        read(j).start()
    for n in range(n_blocks):
        if n >= WINDOW:
            block(n - WINDOW).wait()
        send(n)
        for j in range(len(jobs)):
            if j < SLOTS and n == WINDOW + j // 2 - 1:
                run(j)
            if j >= SLOTS and n == WINDOW + 2 + j // 2:
                again(j)
            if j >= SLOTS and n == WINDOW + 4 + j // 2:
                run(j)
    for n in range(n_blocks - WINDOW, n_blocks):
        block(n).wait()
    for j in range(len(jobs) - SLOTS, len(jobs)):
        write(j).wait()
    h_copy.wait()


def solution(mesh):
    cache_spec = P('dp', 'sp', 'tp', None)

    def local_step(hidden, norm_scale, w_qkv, w_out, k_cache, v_cache, positions):
        n_seq, seq_local, kv, head = k_cache.shape
        d_model = hidden.shape[1]
        per_kv = w_qkv.shape[1] // (kv * head) - 2
        rows = seq_local * kv
        n_heads = kv * per_kv
        n_groups = n_seq // GROUP
        pair_rows = 2 * n_heads
        own = n_seq // N_SP
        n_jobs = 2 * (n_seq - HELD * GROUP) // JOB
        dims = (n_seq, rows, kv, head, per_kv, d_model)
        half = np.arange(head) % (head // 2)
        inv_freq = np.exp(half * (-2.0 * math.log(500000.0) / head)).astype(np.float32)[None]
        f32, bf16 = jnp.float32, jnp.bfloat16
        vmem = pl.BlockSpec(memory_space=pltpu.VMEM)
        hbm = pl.BlockSpec(memory_space=pltpu.HBM)
        smem = pl.BlockSpec(memory_space=pltpu.SMEM)
        cache = (n_seq, rows, head)
        dma = pltpu.SemaphoreType.DMA
        keep = pltpu.with_memory_space_constraint
        w_qkv, w_out = keep(w_qkv, pltpu.HBM), keep(w_out, pltpu.HBM)
        k_flat = keep(k_cache.reshape(cache), pltpu.HBM)
        v_flat = keep(v_cache.reshape(cache), pltpu.HBM)
        h_vm, k_vm, v_vm, new_k, new_v = pl.pallas_call(
            lambda *refs: attend_kernel(dims, *refs),
            out_shape=(pltpu.VMEM(hidden.shape, bf16),
                       pltpu.VMEM((HELD * GROUP, rows, head), bf16),
                       pltpu.VMEM((HELD * GROUP, rows, head), bf16),
                       pltpu.VMEM((n_seq * 16, head), f32),
                       pltpu.VMEM((n_seq * 16, head), f32)),
            in_specs=[smem, vmem, vmem, vmem, hbm, hbm, hbm, hbm],
            out_specs=(vmem,) * 5,
            scratch_shapes=[
                pltpu.VMEM((W_CHUNKS, n_seq, d_model // W_CHUNKS), bf16),
                pltpu.VMEM((W_SLOTS, d_model // W_CHUNKS, w_qkv.shape[1]), bf16),
                pltpu.VMEM((n_seq, w_qkv.shape[1]), f32),
                pltpu.VMEM((n_seq, head), f32),
                pltpu.VMEM((n_seq, head), f32),
                pltpu.VMEM(w_out.shape, bf16),
                pltpu.VMEM((n_seq - HELD * GROUP, rows, head), bf16),
                pltpu.VMEM((n_seq - HELD * GROUP, rows, head), bf16),
                pltpu.VMEM((n_seq * n_heads, head), f32),
                pltpu.VMEM((n_seq * n_heads, head), f32),
                pltpu.VMEM((n_seq * n_heads, head), f32),
                pltpu.VMEM((pair_rows, rows), jnp.int32),
                pltpu.VMEM((N_SP, pair_rows, rows), f32),
                pltpu.VMEM((n_groups, N_SP, pair_rows + 8, head), f32),
                pltpu.VMEM((n_groups, N_SP - 1, pair_rows + 8, head), f32),
                pltpu.VMEM((own * n_heads, head), f32),
                pltpu.VMEM((COLS, own, d_model // COLS), f32),
                pltpu.VMEM((COLS, own, d_model // COLS), f32),
                pltpu.VMEM((COLS, N_SP, own, d_model // COLS), f32),
                dma((W_CHUNKS,)), dma, dma((n_groups,)), dma((n_groups,)),
                dma((n_groups, N_SP - 1)), dma((n_groups, N_SP - 1)),
            ] + [dma((COLS,))] * 8,
            compiler_params=pltpu.CompilerParams(
                collective_id=0, has_side_effects=True, vmem_limit_bytes=33 * MIB),
            name='attend',
        )(positions, hidden, norm_scale.reshape(d_model // 128, 128), inv_freq, w_qkv, w_out, k_flat, v_flat)
        h_out, k_out, v_out, _, _ = pl.pallas_call(
            lambda *refs: write_kernel(dims, *refs),
            out_shape=(jax.ShapeDtypeStruct(hidden.shape, bf16),
                       jax.ShapeDtypeStruct(cache, bf16), jax.ShapeDtypeStruct(cache, bf16),
                       pltpu.VMEM(k_vm.shape, bf16), pltpu.VMEM(v_vm.shape, bf16)),
            in_specs=[smem] + [vmem] * 5 + [hbm] * 2,
            out_specs=(hbm,) * 3 + (vmem,) * 2,
            input_output_aliases={2: 3, 3: 4},
            scratch_shapes=[
                pltpu.VMEM((SLOTS, JOB, rows, head), bf16),
                dma, dma((n_jobs,)), dma((n_jobs,)), dma((2 * HELD,)),
            ],
            compiler_params=pltpu.CompilerParams(vmem_limit_bytes=W_VMEM * MIB),
            name='write',
        )(positions, *[keep(x, pltpu.VMEM) for x in (h_vm, k_vm, v_vm, new_k, new_v)], k_flat, v_flat)
        return h_out, k_out.reshape(k_cache.shape), v_out.reshape(v_cache.shape)

    return jax.shard_map(
        local_step,
        mesh=mesh,
        in_specs=(P('dp', None), P(None), P(None, 'tp'), P('tp', None), cache_spec, cache_spec, P('dp')),
        out_specs=(P('dp', None), cache_spec, cache_spec),
        check_vma=False,
    )
```

```python
import math
import jax
import jax.numpy as jnp
import numpy as np
from jax import lax
from jax.experimental import pallas as pl
from jax.experimental.pallas import tpu as pltpu
from jax.sharding import PartitionSpec as P

MESH = pl.DeviceIdType.MESH
NEG = -1e30
MIB = 1024 * 1024
N_SP = 4
COLS = 6
WO_AT = 6
GROUP = 8
W_CHUNKS = 6
AHEAD = 4
HELD = 7
JOB = 2
SLOTS = 4
WINDOW = 4
W_VMEM = 3


def attend_kernel(dims, pos_in, hidden_in, scale_in, freq_in, w_qkv, w_out, k_in, v_in,
                  h_out, k_vm, v_vm, new_k, new_v,
                  pos, hidden, norm_scale, inv_freq, u, wq, acc, rope_c, rope_s, wo, k_rest, v_rest, q_rows, kn_rows, vn_rows, tok, score, part, recv, merged, proj, proj_in, sums,
                  in_sem, w_sem, wo_sem, k_sem, v_sem, acc_send, acc_recv, part_send, part_recv, tp_send, tp_recv, x_send, x_recv,
                  core_send, core_recv, fwd_send, fwd_recv):
    n_seq, rows, kv, head, per_kv, d_model = dims
    n_heads = kv * per_kv
    n_groups = n_seq // GROUP
    pair_rows = 2 * n_heads
    own = n_seq // N_SP
    w_rows = d_model // W_CHUNKS
    sp = lax.axis_index('sp')
    tp = lax.axis_index('tp')
    seq_local = rows // kv
    scale2 = head ** -0.5 * math.log2(math.e)

    core = lax.rem(sp, 2)
    partner = sp + 1 - 2 * core
    across = lax.rem(sp + 2, N_SP)
    half_cols = w_qkv.shape[1] // 2

    def w_copy(c):
        cols = pl.ds(pl.multiple_of(core * half_cols, head), half_cols)
        return pltpu.make_async_copy(w_qkv.at[pl.ds(c * w_rows, w_rows), cols], wq.at[c], w_sem.at[c])

    def held(ref, rest, n_held, g):
        return (ref, g) if g < n_held else (rest, g - n_held)

    def cache_copy(src, ref, rest, n_held, sem, g):
        dst, i = held(ref, rest, n_held, g)
        return pltpu.make_async_copy(src.at[pl.ds(g * GROUP, GROUP)], dst.at[pl.ds(i * GROUP, GROUP)], sem.at[g])

    def k_copy(g):
        return cache_copy(k_in, k_vm, k_rest, HELD, k_sem, g)

    def v_copy(g):
        return cache_copy(v_in, v_vm, v_rest, HELD, v_sem, g)

    wo_copy = pltpu.make_async_copy(w_out, wo, wo_sem)
    small = [pltpu.make_async_copy(a, b, in_sem.at[i]) for i, (a, b) in enumerate(
        ((hidden_in, hidden), (scale_in, norm_scale), (freq_in, inv_freq), (pos_in, pos)))]
    for c in small:
        c.start()
    for c in range(W_CHUNKS):
        w_copy(c).start()

    barrier = pltpu.get_barrier_semaphore()
    for s in range(1, N_SP):
        pl.semaphore_signal(barrier, inc=1, device_id={'sp': lax.rem(sp + s, N_SP)}, device_id_type=MESH)
    pl.semaphore_signal(barrier, inc=1, device_id={'tp': 1 - tp}, device_id_type=MESH)

    for c in small:
        c.wait()
    hid = hidden[...].astype(jnp.float32)
    mean = jnp.mean(hid, axis=-1, keepdims=True)
    cen = hid - mean
    var = jnp.mean(cen * cen, axis=-1, keepdims=True)
    scale_rows = norm_scale[...].astype(jnp.float32)
    scale_row = jnp.concatenate([scale_rows[i:i + 1] for i in range(scale_rows.shape[0])], axis=1)
    normed = (cen * lax.rsqrt(var + 1e-5) * scale_row).astype(jnp.bfloat16)
    for c in range(W_CHUNKS):
        u[c] = normed[:, c * w_rows:(c + 1) * w_rows]

    col = lax.broadcasted_iota(jnp.int32, (pair_rows, rows), 1)
    row = lax.broadcasted_iota(jnp.int32, (pair_rows, rows), 0)
    row_kv = lax.rem(row, n_heads) // per_kv
    tok[...] = jnp.where(lax.rem(col, kv) == row_kv, sp * seq_local + col // kv, 1 << 30)

    acc[core] = jnp.zeros(acc.shape[1:], jnp.float32)

    brow = lax.broadcasted_iota(jnp.int32, (n_seq, 1), 0)
    pos_col = jnp.zeros((n_seq, 1), jnp.int32)
    for b in range(n_seq):
        pos_col = jnp.where(brow == b, pos[b], pos_col)
    angles = pos_col.astype(jnp.float32) * inv_freq[...]
    c2 = jnp.cos(angles)
    s2 = jnp.sin(angles)
    s2 = jnp.where(lax.broadcasted_iota(jnp.int32, s2.shape, 1) < head // 2, -s2, s2)
    rope_c[...] = c2
    rope_s[...] = s2

    cache_order = [f(g) for g in range(AHEAD) for f in (k_copy, v_copy)]
    for c in range(W_CHUNKS):
        w_copy(c).wait()
        for copy in cache_order[c * len(cache_order) // W_CHUNKS:(c + 1) * len(cache_order) // W_CHUNKS]:
            copy.start()
        acc[core] += jnp.dot(u[c], wq[c], preferred_element_type=jnp.float32)

    pl.semaphore_wait(barrier, N_SP)
    acc_copy = pltpu.make_async_remote_copy(acc.at[core], acc.at[core], acc_send, acc_recv,
                                            device_id={'sp': partner}, device_id_type=MESH)
    acc_copy.start()
    acc_copy.wait()

    c2 = rope_c[...]
    s2 = rope_s[...]
    for g in range(kv):
        for j in range(per_kv + 2):
            lo = (g % (kv // 2) * (per_kv + 2) + j) * head
            x = jnp.clip(acc[g // (kv // 2), :, lo:lo + head].astype(jnp.bfloat16).astype(jnp.float32), -8.0, 8.0)
            if j <= per_kv:
                x = (x * c2 + pltpu.roll(x, head // 2, 1) * s2).astype(jnp.bfloat16).astype(jnp.float32)
            if j < per_kv:
                q_rows[pl.ds(g * per_kv + j, n_seq, stride=n_heads), :] = x
            else:
                wide, rep = (kn_rows, new_k) if j == per_kv else (vn_rows, new_v)
                for i in range(per_kv):
                    wide[pl.ds(g * per_kv + i, n_seq, stride=n_heads), :] = x
                for i in range(16 // kv):
                    rep[pl.ds(i * kv + g, n_seq, stride=16), :] = x

    prow = lax.broadcasted_iota(jnp.int32, (pair_rows, 1), 0)
    first = prow < n_heads

    def part_copy(g, s):
        dst = lax.rem(sp + s, N_SP)
        return pltpu.make_async_remote_copy(
            src_ref=part.at[g, dst], dst_ref=recv.at[g, s - 1],
            send_sem=part_send.at[g, s - 1], recv_sem=part_recv.at[g, s - 1],
            device_id={'sp': dst}, device_id_type=MESH)

    lane = lax.broadcasted_iota(jnp.int32, (8, head), 1)
    n_stat = pair_rows // 8

    def scores(g, k_ref, k_off):
        for d in range(N_SP):
            kb = g * GROUP + 2 * d - k_off
            q = q_rows[pl.ds(pl.multiple_of((g * N_SP + d) * pair_rows, 8), pair_rows), :]
            zero = jnp.zeros_like(q)
            q_blk = jnp.concatenate([jnp.where(first, q, zero), jnp.where(first, zero, q)], axis=1).astype(jnp.bfloat16)
            k_cat = jnp.concatenate([k_ref[kb], k_ref[kb + 1]], axis=1)
            score[d] = lax.dot_general(q_blk, k_cat, (((1,), (1,)), ((), ())), preferred_element_type=jnp.float32)

    def values(g, v_ref, v_off):
        for d in range(N_SP):
            b = g * GROUP + 2 * d
            vb = b - v_off
            limit = jnp.where(first, pos[b], pos[b + 1])
            s = jnp.where(tok[...] < limit, score[d], NEG)
            m = jnp.max(s, axis=-1, keepdims=True)
            w = jnp.exp2((s - m) * scale2)
            l = jnp.sum(w, axis=-1, keepdims=True)
            v_cat = jnp.concatenate([v_ref[vb], v_ref[vb + 1]], axis=1)
            o = jnp.dot(w.astype(jnp.bfloat16), v_cat, preferred_element_type=jnp.float32)
            part[g, d, :pair_rows] = jnp.where(first, o[:, :head], o[:, head:])
            stat = jnp.zeros((8, head), jnp.float32)
            for i in range(n_stat):
                stat = jnp.where(lane == i, m[8 * i:8 * i + 8], stat)
                stat = jnp.where(lane == n_stat + i, l[8 * i:8 * i + 8], stat)
            part[g, d, pair_rows:] = stat
        for s in range(1, N_SP):
            part_copy(g, s).start()

    def held_step(g, carry):
        now, later = pl.ds(g * GROUP, GROUP), pl.ds((g + AHEAD) * GROUP, GROUP)
        pltpu.make_async_copy(k_in.at[now], k_vm.at[now], k_sem.at[g]).wait()
        pltpu.make_async_copy(k_in.at[later], k_vm.at[later], k_sem.at[g + AHEAD]).start()
        scores(g, k_vm, 0)
        pltpu.make_async_copy(v_in.at[now], v_vm.at[now], v_sem.at[g]).wait()
        pltpu.make_async_copy(v_in.at[later], v_vm.at[later], v_sem.at[g + AHEAD]).start()
        values(g, v_vm, 0)
        return carry

    lax.fori_loop(0, HELD - AHEAD, held_step, 0)
    for g in range(HELD - AHEAD, n_groups):
        k_ref, ki = held(k_vm, k_rest, HELD, g)
        v_ref, vi = held(v_vm, v_rest, HELD, g)
        k_copy(g).wait()
        if g + AHEAD < n_groups:
            k_copy(g + AHEAD).start()
        scores(g, k_ref, (g - ki) * GROUP)
        v_copy(g).wait()
        if g + AHEAD < n_groups:
            v_copy(g + AHEAD).start()
        if g == WO_AT:
            wo_copy.start()
        values(g, v_ref, (g - vi) * GROUP)

    def merge_step(g, carry):
        for s in range(1, N_SP):
            part_copy(g, s).wait()
        r = pl.ds(pl.multiple_of((g * N_SP + sp) * pair_rows, 8), pair_rows)
        s_new = jnp.sum(q_rows[r, :] * kn_rows[r, :], axis=-1, keepdims=True)
        outs = [part[g, sp]] + [recv[g, s] for s in range(N_SP - 1)]

        def column(x, first_lane):
            return jnp.concatenate(
                [x[pair_rows:, first_lane + i:first_lane + i + 1] for i in range(n_stat)], axis=0)

        ms = [column(x, 0) for x in outs]
        ls = [column(x, n_stat) for x in outs]
        top = s_new
        for m in ms:
            top = jnp.maximum(top, m)
        f = jnp.exp2((s_new - top) * scale2)
        o = f * vn_rows[r, :]
        l = f
        for x, m, ll in zip(outs, ms, ls):
            f = jnp.exp2((m - top) * scale2)
            o = o + f * x[:pair_rows]
            l = l + f * ll
        merged[pl.ds(pl.multiple_of(g * pair_rows, 8), pair_rows), :] = o / l
        return carry

    lax.fori_loop(0, n_groups, merge_step, 0)
    attn = jnp.concatenate(
        [merged[pl.ds(n, own, stride=n_heads), :].astype(jnp.bfloat16) for n in range(n_heads)], axis=1)
    wo_copy.wait()
    width = d_model // COLS

    def tp_copy(c):
        return pltpu.make_async_remote_copy(proj.at[c], proj_in.at[c], tp_send.at[c], tp_recv.at[c],
                                            device_id={'tp': 1 - tp}, device_id_type=MESH)

    def x_copy(c):
        return pltpu.make_async_remote_copy(sums.at[c, sp], sums.at[c, sp], x_send.at[c], x_recv.at[c],
                                            device_id={'sp': across}, device_id_type=MESH)

    def core_copy(c):
        return pltpu.make_async_remote_copy(sums.at[c, sp], sums.at[c, sp], core_send.at[c], core_recv.at[c],
                                            device_id={'sp': partner}, device_id_type=MESH)

    def fwd_copy(c):
        return pltpu.make_async_remote_copy(sums.at[c, across], sums.at[c, across], fwd_send.at[c], fwd_recv.at[c],
                                            device_id={'sp': partner}, device_id_type=MESH)

    for c in range(COLS):
        proj[c] = jnp.dot(attn, wo[:, c * width:(c + 1) * width], preferred_element_type=jnp.float32)
        tp_copy(c).start()
    for c in range(COLS):
        tp_copy(c).wait()
        sums[c, sp] = proj[c] + proj_in[c]
        x_copy(c).start()
        core_copy(c).start()
    for c in range(COLS):
        x_copy(c).wait()
        fwd_copy(c).start()

    srow = lax.broadcasted_iota(jnp.int32, (GROUP, 1), 0)
    for c in range(COLS):
        core_copy(c).wait()
        fwd_copy(c).wait()
        lanes = slice(c * width, (c + 1) * width)
        for g in range(n_groups):
            t = (2 * g) // GROUP * GROUP
            gathered = None
            for d in range(N_SP):
                x = sums[c, d, t:t + GROUP, :]
                shift = (2 * d - 2 * g) % GROUP
                if shift:
                    x = pltpu.roll(x, shift, 0)
                gathered = x if gathered is None else jnp.where(srow // 2 == d, x, gathered)
            r = slice(g * GROUP, (g + 1) * GROUP)
            h_out[r, lanes] = (hidden[r, lanes].astype(jnp.float32) + gathered).astype(jnp.bfloat16)


def write_kernel(dims, pos_in, h_in, k_vm, v_vm, new_k, new_v, k_in, v_in, h_out, k_out, v_out, k_same, v_same,
                 pos, slots, pos_sem, h_sem, rd_sem, wr_sem, blk_sem):
    n_seq, rows, kv, _, _, _ = dims
    sp = lax.axis_index('sp')
    seq_local = rows // kv
    n_held = HELD * GROUP
    per = 16 // kv
    sub = lax.broadcasted_iota(jnp.int32, (16, 1), 0) // kv
    jobs = [(src, out, new, b) for src, out, new in ((k_in, k_out, new_k), (v_in, v_out, new_v))
            for b in range(n_held, n_seq, JOB)]

    def patch(ref, i, b, new):
        p = pos[b] - sp * seq_local
        blk = jnp.clip(p, 0, seq_local - 1) // per
        r = pl.ds(pl.multiple_of(blk * 16, 16), 16)
        fresh = new[pl.ds(pl.multiple_of(b * 16, 16), 16), :]
        ref[i, r, :] = jnp.where(sub + blk * per == p, fresh, ref[i, r, :].astype(jnp.float32)).astype(jnp.bfloat16)

    def read(j):
        src, _, _, b = jobs[j]
        return pltpu.make_async_copy(src.at[pl.ds(b, JOB)], slots.at[j % SLOTS], rd_sem.at[j])

    def write(j):
        _, out, _, b = jobs[j]
        return pltpu.make_async_copy(slots.at[j % SLOTS], out.at[pl.ds(b, JOB)], wr_sem.at[j])

    def run(j):
        _, _, new, b = jobs[j]
        read(j).wait()
        for i in range(JOB):
            patch(slots.at[j % SLOTS], i, b + i, new)
        write(j).start()

    def again(j):
        write(j - SLOTS).wait()
        read(j).start()

    def block(n):
        vm, out = ((k_vm, k_out), (v_vm, v_out))[n % 2]
        s = pl.ds(n // 2 * GROUP, GROUP)
        return pltpu.make_async_copy(vm.at[s], out.at[s], blk_sem.at[n])

    def send(n):
        vm, new = ((k_vm, new_k), (v_vm, new_v))[n % 2]
        for i in range(GROUP):
            b = n // 2 * GROUP + i
            patch(vm, b, b, new)
        block(n).start()

    n_blocks = 2 * HELD
    pos_copy = pltpu.make_async_copy(pos_in, pos, pos_sem)
    pos_copy.start()
    h_copy = pltpu.make_async_copy(h_in, h_out, h_sem)
    h_copy.start()
    for j in range(SLOTS):
        read(j).start()
    pos_copy.wait()
    for n in range(n_blocks):
        if n >= WINDOW:
            block(n - WINDOW).wait()
        send(n)
        for j in range(len(jobs)):
            if j < SLOTS and n == WINDOW + j // 2 - 1:
                run(j)
            if j >= SLOTS and n == WINDOW + 2 + j // 2:
                again(j)
            if j >= SLOTS and n == WINDOW + 4 + j // 2:
                run(j)
    for n in range(n_blocks - WINDOW, n_blocks):
        block(n).wait()
    for j in range(len(jobs) - SLOTS, len(jobs)):
        write(j).wait()
    h_copy.wait()


def solution(mesh):
    cache_spec = P('dp', 'sp', 'tp', None)

    def local_step(hidden, norm_scale, w_qkv, w_out, k_cache, v_cache, positions):
        n_seq, seq_local, kv, head = k_cache.shape
        d_model = hidden.shape[1]
        per_kv = w_qkv.shape[1] // (kv * head) - 2
        rows = seq_local * kv
        n_heads = kv * per_kv
        n_groups = n_seq // GROUP
        pair_rows = 2 * n_heads
        own = n_seq // N_SP
        n_jobs = 2 * (n_seq - HELD * GROUP) // JOB
        dims = (n_seq, rows, kv, head, per_kv, d_model)
        half = np.arange(head) % (head // 2)
        inv_freq = np.exp(half * (-2.0 * math.log(500000.0) / head)).astype(np.float32)[None]
        f32, bf16 = jnp.float32, jnp.bfloat16
        vmem = pl.BlockSpec(memory_space=pltpu.VMEM)
        hbm = pl.BlockSpec(memory_space=pltpu.HBM)
        cache = (n_seq, rows, head)
        dma = pltpu.SemaphoreType.DMA
        keep = pltpu.with_memory_space_constraint
        w_qkv, w_out = keep(w_qkv, pltpu.HBM), keep(w_out, pltpu.HBM)
        k_flat = keep(k_cache.reshape(cache), pltpu.HBM)
        v_flat = keep(v_cache.reshape(cache), pltpu.HBM)
        h_vm, k_vm, v_vm, new_k, new_v = pl.pallas_call(
            lambda *refs: attend_kernel(dims, *refs),
            out_shape=(pltpu.VMEM(hidden.shape, bf16),
                       pltpu.VMEM((HELD * GROUP, rows, head), bf16),
                       pltpu.VMEM((HELD * GROUP, rows, head), bf16),
                       pltpu.VMEM((n_seq * 16, head), f32),
                       pltpu.VMEM((n_seq * 16, head), f32)),
            in_specs=[hbm] * 8,
            out_specs=(vmem,) * 5,
            scratch_shapes=[
                pltpu.SMEM((n_seq,), jnp.int32),
                pltpu.VMEM(hidden.shape, bf16),
                pltpu.VMEM((d_model // head, head), bf16),
                pltpu.VMEM((1, head), f32),
                pltpu.VMEM((W_CHUNKS, n_seq, d_model // W_CHUNKS), bf16),
                pltpu.VMEM((W_CHUNKS, d_model // W_CHUNKS, w_qkv.shape[1] // 2), bf16),
                pltpu.VMEM((2, n_seq, w_qkv.shape[1] // 2), f32),
                pltpu.VMEM((n_seq, head), f32),
                pltpu.VMEM((n_seq, head), f32),
                pltpu.VMEM(w_out.shape, bf16),
                pltpu.VMEM((n_seq - HELD * GROUP, rows, head), bf16),
                pltpu.VMEM((n_seq - HELD * GROUP, rows, head), bf16),
                pltpu.VMEM((n_seq * n_heads, head), f32),
                pltpu.VMEM((n_seq * n_heads, head), f32),
                pltpu.VMEM((n_seq * n_heads, head), f32),
                pltpu.VMEM((pair_rows, rows), jnp.int32),
                pltpu.VMEM((N_SP, pair_rows, rows), f32),
                pltpu.VMEM((n_groups, N_SP, pair_rows + 8, head), f32),
                pltpu.VMEM((n_groups, N_SP - 1, pair_rows + 8, head), f32),
                pltpu.VMEM((own * n_heads, head), f32),
                pltpu.VMEM((COLS, own, d_model // COLS), f32),
                pltpu.VMEM((COLS, own, d_model // COLS), f32),
                pltpu.VMEM((COLS, N_SP, own, d_model // COLS), f32),
                dma((4,)), dma((W_CHUNKS,)), dma, dma((n_groups,)), dma((n_groups,)), dma, dma,
                dma((n_groups, N_SP - 1)), dma((n_groups, N_SP - 1)),
            ] + [dma((COLS,))] * 8,
            compiler_params=pltpu.CompilerParams(
                collective_id=0, has_side_effects=True, vmem_limit_bytes=33 * MIB),
            name='attend',
        )(keep(positions, pltpu.HBM), keep(hidden, pltpu.HBM),
          keep(norm_scale.reshape(d_model // head, head), pltpu.HBM), inv_freq, w_qkv, w_out, k_flat, v_flat)
        h_out, k_out, v_out, _, _ = pl.pallas_call(
            lambda *refs: write_kernel(dims, *refs),
            out_shape=(jax.ShapeDtypeStruct(hidden.shape, bf16),
                       jax.ShapeDtypeStruct(cache, bf16), jax.ShapeDtypeStruct(cache, bf16),
                       pltpu.VMEM(k_vm.shape, bf16), pltpu.VMEM(v_vm.shape, bf16)),
            in_specs=[hbm] + [vmem] * 5 + [hbm] * 2,
            out_specs=(hbm,) * 3 + (vmem,) * 2,
            input_output_aliases={2: 3, 3: 4},
            scratch_shapes=[
                pltpu.SMEM((n_seq,), jnp.int32),
                pltpu.VMEM((SLOTS, JOB, rows, head), bf16),
                dma, dma, dma((n_jobs,)), dma((n_jobs,)), dma((2 * HELD,)),
            ],
            compiler_params=pltpu.CompilerParams(vmem_limit_bytes=W_VMEM * MIB),
            name='write',
        )(keep(positions, pltpu.HBM), *[keep(x, pltpu.VMEM) for x in (h_vm, k_vm, v_vm, new_k, new_v)], k_flat, v_flat)
        return h_out, k_out.reshape(k_cache.shape), v_out.reshape(v_cache.shape)

    return jax.shard_map(
        local_step,
        mesh=mesh,
        in_specs=(P('dp', None), P(None), P(None, 'tp'), P('tp', None), cache_spec, cache_spec, P('dp')),
        out_specs=(P('dp', None), cache_spec, cache_spec),
        check_vma=False,
    )
```

```python
import math
import jax
import jax.numpy as jnp
import numpy as np
from jax import lax
from jax.experimental import pallas as pl
from jax.experimental.pallas import tpu as pltpu
from jax.sharding import PartitionSpec as P

MESH = pl.DeviceIdType.MESH
NEG = -1e30
MIB = 1024 * 1024
N_SP = 4
COLS = 6
WO_AT = 4
PHASE = 2
GROUP = 8
AHEAD = 4
HELD = 7
JOB = 2
SLOTS = 4
WINDOW = 4
W_VMEM = 3


def attend_kernel(dims, pos_in, hidden_in, scale_in, freq_in, w_qkv, w_out, k_in, v_in,
                  h_out, k_vm, v_vm, new_k, new_v,
                  pos, hidden, norm_scale, inv_freq, u, wq, heads, rope_c, rope_s, wo, k_rest, v_rest, q_rows, kn_rows, vn_rows, tok, score, part, recv, merged, proj, proj_in, sums,
                  in_sem, w_sem, wo_sem, k_sem, v_sem, acc_send, acc_recv, part_send, part_recv, tp_send, tp_recv, x_send, x_recv,
                  core_send, core_recv, fwd_send, fwd_recv):
    n_seq, rows, kv, head, per_kv, d_model = dims
    n_heads = kv * per_kv
    n_groups = n_seq // GROUP
    pair_rows = 2 * n_heads
    own = n_seq // N_SP
    sp = lax.axis_index('sp')
    tp = lax.axis_index('tp')
    seq_local = rows // kv
    scale2 = head ** -0.5 * math.log2(math.e)

    core = lax.rem(sp, 2)
    partner = sp + 1 - 2 * core
    across = lax.rem(sp + 2, N_SP)
    half_cols = w_qkv.shape[1] // 2
    w_cols = 2 * head
    w_chunks = half_cols // w_cols

    def w_copy(c):
        cols = pl.ds(pl.multiple_of(core * half_cols + c * w_cols, head), w_cols)
        return pltpu.make_async_copy(w_qkv.at[:, cols], wq.at[c], w_sem.at[c])

    def held(ref, rest, n_held, g):
        return (ref, g) if g < n_held else (rest, g - n_held)

    def cache_copy(src, ref, rest, n_held, sem, g):
        dst, i = held(ref, rest, n_held, g)
        return pltpu.make_async_copy(src.at[pl.ds(g * GROUP, GROUP)], dst.at[pl.ds(i * GROUP, GROUP)], sem.at[g])

    def k_copy(g):
        return cache_copy(k_in, k_vm, k_rest, HELD, k_sem, g)

    def v_copy(g):
        return cache_copy(v_in, v_vm, v_rest, HELD, v_sem, g)

    wo_copy = pltpu.make_async_copy(w_out, wo, wo_sem)
    small = [pltpu.make_async_copy(a, b, in_sem.at[i]) for i, (a, b) in enumerate(
        ((hidden_in, hidden), (scale_in, norm_scale), (freq_in, inv_freq), (pos_in, pos)))]
    for c in small:
        c.start()
    for c in range(w_chunks):
        w_copy(c).start()

    barrier = pltpu.get_barrier_semaphore()
    for s in range(1, N_SP):
        pl.semaphore_signal(barrier, inc=1, device_id={'sp': lax.rem(sp + s, N_SP)}, device_id_type=MESH)
    pl.semaphore_signal(barrier, inc=1, device_id={'tp': 1 - tp}, device_id_type=MESH)

    for c in small:
        c.wait()
    hid = hidden[...].astype(jnp.float32)
    mean = jnp.mean(hid, axis=-1, keepdims=True)
    cen = hid - mean
    var = jnp.mean(cen * cen, axis=-1, keepdims=True)
    scale_rows = norm_scale[...].astype(jnp.float32)
    scale_row = jnp.concatenate([scale_rows[i:i + 1] for i in range(scale_rows.shape[0])], axis=1)
    normed = (cen * lax.rsqrt(var + 1e-5) * scale_row).astype(jnp.bfloat16)
    u[...] = normed

    col = lax.broadcasted_iota(jnp.int32, (pair_rows, rows), 1)
    row = lax.broadcasted_iota(jnp.int32, (pair_rows, rows), 0)
    row_kv = lax.rem(row, n_heads) // per_kv
    tok[...] = jnp.where(lax.rem(col, kv) == row_kv, sp * seq_local + col // kv, 1 << 30)

    brow = lax.broadcasted_iota(jnp.int32, (n_seq, 1), 0)
    pos_col = jnp.zeros((n_seq, 1), jnp.int32)
    for b in range(n_seq):
        pos_col = jnp.where(brow == b, pos[b], pos_col)
    angles = pos_col.astype(jnp.float32) * inv_freq[...]
    c2 = jnp.cos(angles)
    s2 = jnp.sin(angles)
    s2 = jnp.where(lax.broadcasted_iota(jnp.int32, s2.shape, 1) < head // 2, -s2, s2)
    rope_c[...] = c2
    rope_s[...] = s2

    cache_order = [f(g) for g in range(AHEAD) for f in (k_copy, v_copy)]
    group_heads = per_kv + 2

    def heads_copy(c):
        mine = heads.at[core, pl.ds(2 * c, 2)]
        return pltpu.make_async_remote_copy(mine, mine, acc_send.at[c], acc_recv.at[c],
                                            device_id={'sp': partner}, device_id_type=MESH)

    for c in range(w_chunks):
        w_copy(c).wait()
        for copy in cache_order[c * len(cache_order) // w_chunks:(c + 1) * len(cache_order) // w_chunks]:
            copy.start()
        qkv = jnp.dot(u[...], wq[c], preferred_element_type=jnp.float32)
        for i in range(2):
            x = jnp.clip(qkv[:, i * head:(i + 1) * head].astype(jnp.bfloat16).astype(jnp.float32), -8.0, 8.0)
            if (2 * c + i) % group_heads <= per_kv:
                x = x * rope_c[...] + pltpu.roll(x, head // 2, 1) * rope_s[...]
                x = x.astype(jnp.bfloat16).astype(jnp.float32)
            heads[core, 2 * c + i] = x
        if c == 0:
            pl.semaphore_wait(barrier, N_SP)
        heads_copy(c).start()

    def spread(half):
        for h in range(half_cols // head):
            g, j = half * (kv // 2) + h // group_heads, h % group_heads
            x = heads[half, h]
            if j < per_kv:
                q_rows[pl.ds(g * per_kv + j, n_seq, stride=n_heads), :] = x
            else:
                wide, rep = (kn_rows, new_k) if j == per_kv else (vn_rows, new_v)
                for i in range(per_kv):
                    wide[pl.ds(g * per_kv + i, n_seq, stride=n_heads), :] = x
                for i in range(16 // kv):
                    rep[pl.ds(i * kv + g, n_seq, stride=16), :] = x

    for half in range(2):
        @pl.when(core == half)
        def _():
            spread(half)

    for c in range(w_chunks):
        heads_copy(c).wait()
    for half in range(2):
        @pl.when(core != half)
        def _():
            spread(half)

    prow = lax.broadcasted_iota(jnp.int32, (pair_rows, 1), 0)
    first = prow < n_heads

    def part_copy(g, s):
        dst = lax.rem(sp + s, N_SP)
        return pltpu.make_async_remote_copy(
            src_ref=part.at[g, dst], dst_ref=recv.at[g, s - 1],
            send_sem=part_send.at[g, s - 1], recv_sem=part_recv.at[g, s - 1],
            device_id={'sp': dst}, device_id_type=MESH)

    lane = lax.broadcasted_iota(jnp.int32, (8, head), 1)
    n_stat = pair_rows // 8

    def scores(g, k_ref, k_off):
        for d in range(N_SP):
            kb = g * GROUP + 2 * d - k_off
            q = q_rows[pl.ds(pl.multiple_of((g * N_SP + d) * pair_rows, 8), pair_rows), :]
            zero = jnp.zeros_like(q)
            q_blk = jnp.concatenate([jnp.where(first, q, zero), jnp.where(first, zero, q)], axis=1).astype(jnp.bfloat16)
            k_cat = jnp.concatenate([k_ref[kb], k_ref[kb + 1]], axis=1)
            score[lax.rem(g, PHASE), d] = lax.dot_general(q_blk, k_cat, (((1,), (1,)), ((), ())), preferred_element_type=jnp.float32)

    def values(g, v_ref, v_off):
        for d in range(N_SP):
            b = g * GROUP + 2 * d
            vb = b - v_off
            limit = jnp.where(first, pos[b], pos[b + 1])
            s = jnp.where(tok[...] < limit, score[lax.rem(g, PHASE), d], NEG)
            m = jnp.max(s, axis=-1, keepdims=True)
            w = jnp.exp2((s - m) * scale2)
            l = jnp.sum(w, axis=-1, keepdims=True)
            v_cat = jnp.concatenate([v_ref[vb], v_ref[vb + 1]], axis=1)
            o = jnp.dot(w.astype(jnp.bfloat16), v_cat, preferred_element_type=jnp.float32)
            part[g, d, :pair_rows] = jnp.where(first, o[:, :head], o[:, head:])
            stat = jnp.zeros((8, head), jnp.float32)
            for i in range(n_stat):
                stat = jnp.where(lane == i, m[8 * i:8 * i + 8], stat)
                stat = jnp.where(lane == n_stat + i, l[8 * i:8 * i + 8], stat)
            part[g, d, pair_rows:] = stat
        for s in range(1, N_SP):
            part_copy(g, s).start()

    def phase_step(n, carry):
        for g in range(PHASE):
            g = n * PHASE + g
            now, later = pl.ds(g * GROUP, GROUP), pl.ds((g + AHEAD) * GROUP, GROUP)
            pltpu.make_async_copy(k_in.at[now], k_vm.at[now], k_sem.at[g]).wait()
            pltpu.make_async_copy(k_in.at[later], k_vm.at[later], k_sem.at[g + AHEAD]).start()
        for g in range(PHASE):
            scores(n * PHASE + g, k_vm, 0)
        for g in range(PHASE):
            g = n * PHASE + g
            now, later = pl.ds(g * GROUP, GROUP), pl.ds((g + AHEAD) * GROUP, GROUP)
            pltpu.make_async_copy(v_in.at[now], v_vm.at[now], v_sem.at[g]).wait()
            pltpu.make_async_copy(v_in.at[later], v_vm.at[later], v_sem.at[g + AHEAD]).start()
        for g in range(PHASE):
            values(n * PHASE + g, v_vm, 0)
        return carry

    looped = (HELD - AHEAD) // PHASE
    lax.fori_loop(0, looped, phase_step, 0)
    for n in range(looped, n_groups // PHASE):
        gs = range(n * PHASE, (n + 1) * PHASE)
        for g in gs:
            k_copy(g).wait()
            if g + AHEAD < n_groups:
                k_copy(g + AHEAD).start()
        for g in gs:
            k_ref, ki = held(k_vm, k_rest, HELD, g)
            scores(g, k_ref, (g - ki) * GROUP)
        for g in gs:
            v_copy(g).wait()
            if g + AHEAD < n_groups:
                v_copy(g + AHEAD).start()
        if WO_AT in gs:
            wo_copy.start()
        for g in gs:
            v_ref, vi = held(v_vm, v_rest, HELD, g)
            values(g, v_ref, (g - vi) * GROUP)

    def merge_step(g, carry):
        for s in range(1, N_SP):
            part_copy(g, s).wait()
        r = pl.ds(pl.multiple_of((g * N_SP + sp) * pair_rows, 8), pair_rows)
        s_new = jnp.sum(q_rows[r, :] * kn_rows[r, :], axis=-1, keepdims=True)
        outs = [part[g, sp]] + [recv[g, s] for s in range(N_SP - 1)]

        def column(x, first_lane):
            return jnp.concatenate(
                [x[pair_rows:, first_lane + i:first_lane + i + 1] for i in range(n_stat)], axis=0)

        ms = [column(x, 0) for x in outs]
        ls = [column(x, n_stat) for x in outs]
        top = s_new
        for m in ms:
            top = jnp.maximum(top, m)
        f = jnp.exp2((s_new - top) * scale2)
        o = f * vn_rows[r, :]
        l = f
        for x, m, ll in zip(outs, ms, ls):
            f = jnp.exp2((m - top) * scale2)
            o = o + f * x[:pair_rows]
            l = l + f * ll
        merged[pl.ds(pl.multiple_of(g * pair_rows, 8), pair_rows), :] = o / l
        return carry

    lax.fori_loop(0, n_groups, merge_step, 0)
    attn = jnp.concatenate(
        [merged[pl.ds(n, own, stride=n_heads), :].astype(jnp.bfloat16) for n in range(n_heads)], axis=1)
    wo_copy.wait()
    width = d_model // COLS

    def tp_copy(c):
        return pltpu.make_async_remote_copy(proj.at[c], proj_in.at[c], tp_send.at[c], tp_recv.at[c],
                                            device_id={'tp': 1 - tp}, device_id_type=MESH)

    def x_copy(c):
        return pltpu.make_async_remote_copy(sums.at[c, sp], sums.at[c, sp], x_send.at[c], x_recv.at[c],
                                            device_id={'sp': across}, device_id_type=MESH)

    def core_copy(c):
        return pltpu.make_async_remote_copy(sums.at[c, sp], sums.at[c, sp], core_send.at[c], core_recv.at[c],
                                            device_id={'sp': partner}, device_id_type=MESH)

    def fwd_copy(c):
        return pltpu.make_async_remote_copy(sums.at[c, across], sums.at[c, across], fwd_send.at[c], fwd_recv.at[c],
                                            device_id={'sp': partner}, device_id_type=MESH)

    for c in range(COLS):
        proj[c] = jnp.dot(attn, wo[:, c * width:(c + 1) * width], preferred_element_type=jnp.float32)
        tp_copy(c).start()
    for c in range(COLS):
        tp_copy(c).wait()
        sums[c, sp] = proj[c] + proj_in[c]
        x_copy(c).start()
        core_copy(c).start()
    for c in range(COLS):
        x_copy(c).wait()
        fwd_copy(c).start()

    srow = lax.broadcasted_iota(jnp.int32, (GROUP, 1), 0)
    for c in range(COLS):
        core_copy(c).wait()
        fwd_copy(c).wait()
        lanes = slice(c * width, (c + 1) * width)
        for g in range(n_groups):
            t = (2 * g) // GROUP * GROUP
            gathered = None
            for d in range(N_SP):
                x = sums[c, d, t:t + GROUP, :]
                shift = (2 * d - 2 * g) % GROUP
                if shift:
                    x = pltpu.roll(x, shift, 0)
                gathered = x if gathered is None else jnp.where(srow // 2 == d, x, gathered)
            r = slice(g * GROUP, (g + 1) * GROUP)
            h_out[r, lanes] = (hidden[r, lanes].astype(jnp.float32) + gathered).astype(jnp.bfloat16)


def write_kernel(dims, pos_in, h_in, k_vm, v_vm, new_k, new_v, k_in, v_in, h_out, k_out, v_out, k_same, v_same,
                 pos, slots, pos_sem, h_sem, rd_sem, wr_sem, blk_sem):
    n_seq, rows, kv, _, _, _ = dims
    sp = lax.axis_index('sp')
    seq_local = rows // kv
    n_held = HELD * GROUP
    per = 16 // kv
    sub = lax.broadcasted_iota(jnp.int32, (16, 1), 0) // kv
    jobs = [(src, out, new, b) for src, out, new in ((k_in, k_out, new_k), (v_in, v_out, new_v))
            for b in range(n_held, n_seq, JOB)]

    def patch(ref, i, b, new):
        p = pos[b] - sp * seq_local
        blk = jnp.clip(p, 0, seq_local - 1) // per
        r = pl.ds(pl.multiple_of(blk * 16, 16), 16)
        fresh = new[pl.ds(pl.multiple_of(b * 16, 16), 16), :]
        ref[i, r, :] = jnp.where(sub + blk * per == p, fresh, ref[i, r, :].astype(jnp.float32)).astype(jnp.bfloat16)

    def read(j):
        src, _, _, b = jobs[j]
        return pltpu.make_async_copy(src.at[pl.ds(b, JOB)], slots.at[j % SLOTS], rd_sem.at[j])

    def write(j):
        _, out, _, b = jobs[j]
        return pltpu.make_async_copy(slots.at[j % SLOTS], out.at[pl.ds(b, JOB)], wr_sem.at[j])

    def run(j):
        _, _, new, b = jobs[j]
        read(j).wait()
        for i in range(JOB):
            patch(slots.at[j % SLOTS], i, b + i, new)
        write(j).start()

    def again(j):
        write(j - SLOTS).wait()
        read(j).start()

    def block(n):
        vm, out = ((k_vm, k_out), (v_vm, v_out))[n % 2]
        s = pl.ds(n // 2 * GROUP, GROUP)
        return pltpu.make_async_copy(vm.at[s], out.at[s], blk_sem.at[n])

    def send(n):
        vm, new = ((k_vm, new_k), (v_vm, new_v))[n % 2]
        for i in range(GROUP):
            b = n // 2 * GROUP + i
            patch(vm, b, b, new)
        block(n).start()

    n_blocks = 2 * HELD
    pos_copy = pltpu.make_async_copy(pos_in, pos, pos_sem)
    pos_copy.start()
    h_copy = pltpu.make_async_copy(h_in, h_out, h_sem)
    h_copy.start()
    for j in range(SLOTS):
        read(j).start()
    pos_copy.wait()
    for n in range(n_blocks):
        if n >= WINDOW:
            block(n - WINDOW).wait()
        send(n)
        for j in range(len(jobs)):
            if j < SLOTS and n == WINDOW + j // 2 - 1:
                run(j)
            if j >= SLOTS and n == WINDOW + 2 + j // 2:
                again(j)
            if j >= SLOTS and n == WINDOW + 4 + j // 2:
                run(j)
    for n in range(n_blocks - WINDOW, n_blocks):
        block(n).wait()
    for j in range(len(jobs) - SLOTS, len(jobs)):
        write(j).wait()
    h_copy.wait()


def solution(mesh):
    cache_spec = P('dp', 'sp', 'tp', None)

    def local_step(hidden, norm_scale, w_qkv, w_out, k_cache, v_cache, positions):
        n_seq, seq_local, kv, head = k_cache.shape
        d_model = hidden.shape[1]
        per_kv = w_qkv.shape[1] // (kv * head) - 2
        rows = seq_local * kv
        n_heads = kv * per_kv
        n_groups = n_seq // GROUP
        pair_rows = 2 * n_heads
        own = n_seq // N_SP
        w_chunks = w_qkv.shape[1] // (4 * head)
        n_jobs = 2 * (n_seq - HELD * GROUP) // JOB
        dims = (n_seq, rows, kv, head, per_kv, d_model)
        half = np.arange(head) % (head // 2)
        inv_freq = np.exp(half * (-2.0 * math.log(500000.0) / head)).astype(np.float32)[None]
        f32, bf16 = jnp.float32, jnp.bfloat16
        vmem = pl.BlockSpec(memory_space=pltpu.VMEM)
        hbm = pl.BlockSpec(memory_space=pltpu.HBM)
        cache = (n_seq, rows, head)
        dma = pltpu.SemaphoreType.DMA
        keep = pltpu.with_memory_space_constraint
        w_qkv, w_out = keep(w_qkv, pltpu.HBM), keep(w_out, pltpu.HBM)
        k_flat = keep(k_cache.reshape(cache), pltpu.HBM)
        v_flat = keep(v_cache.reshape(cache), pltpu.HBM)
        h_vm, k_vm, v_vm, new_k, new_v = pl.pallas_call(
            lambda *refs: attend_kernel(dims, *refs),
            out_shape=(pltpu.VMEM(hidden.shape, bf16),
                       pltpu.VMEM((HELD * GROUP, rows, head), bf16),
                       pltpu.VMEM((HELD * GROUP, rows, head), bf16),
                       pltpu.VMEM((n_seq * 16, head), f32),
                       pltpu.VMEM((n_seq * 16, head), f32)),
            in_specs=[hbm] * 8,
            out_specs=(vmem,) * 5,
            scratch_shapes=[
                pltpu.SMEM((n_seq,), jnp.int32),
                pltpu.VMEM(hidden.shape, bf16),
                pltpu.VMEM((d_model // head, head), bf16),
                pltpu.VMEM((1, head), f32),
                pltpu.VMEM(hidden.shape, bf16),
                pltpu.VMEM((w_chunks, d_model, 2 * head), bf16),
                pltpu.VMEM((2, 2 * w_chunks, n_seq, head), f32),
                pltpu.VMEM((n_seq, head), f32),
                pltpu.VMEM((n_seq, head), f32),
                pltpu.VMEM(w_out.shape, bf16),
                pltpu.VMEM((n_seq - HELD * GROUP, rows, head), bf16),
                pltpu.VMEM((n_seq - HELD * GROUP, rows, head), bf16),
                pltpu.VMEM((n_seq * n_heads, head), f32),
                pltpu.VMEM((n_seq * n_heads, head), f32),
                pltpu.VMEM((n_seq * n_heads, head), f32),
                pltpu.VMEM((pair_rows, rows), jnp.int32),
                pltpu.VMEM((PHASE, N_SP, pair_rows, rows), f32),
                pltpu.VMEM((n_groups, N_SP, pair_rows + 8, head), f32),
                pltpu.VMEM((n_groups, N_SP - 1, pair_rows + 8, head), f32),
                pltpu.VMEM((own * n_heads, head), f32),
                pltpu.VMEM((COLS, own, d_model // COLS), f32),
                pltpu.VMEM((COLS, own, d_model // COLS), f32),
                pltpu.VMEM((COLS, N_SP, own, d_model // COLS), f32),
                dma((4,)), dma((w_chunks,)), dma, dma((n_groups,)), dma((n_groups,)),
                dma((w_chunks,)), dma((w_chunks,)),
                dma((n_groups, N_SP - 1)), dma((n_groups, N_SP - 1)),
            ] + [dma((COLS,))] * 8,
            compiler_params=pltpu.CompilerParams(
                collective_id=0, has_side_effects=True, vmem_limit_bytes=33 * MIB),
            name='attend',
        )(keep(positions, pltpu.HBM), keep(hidden, pltpu.HBM),
          keep(norm_scale.reshape(d_model // head, head), pltpu.HBM), inv_freq, w_qkv, w_out, k_flat, v_flat)
        h_out, k_out, v_out, _, _ = pl.pallas_call(
            lambda *refs: write_kernel(dims, *refs),
            out_shape=(jax.ShapeDtypeStruct(hidden.shape, bf16),
                       jax.ShapeDtypeStruct(cache, bf16), jax.ShapeDtypeStruct(cache, bf16),
                       pltpu.VMEM(k_vm.shape, bf16), pltpu.VMEM(v_vm.shape, bf16)),
            in_specs=[hbm] + [vmem] * 5 + [hbm] * 2,
            out_specs=(hbm,) * 3 + (vmem,) * 2,
            input_output_aliases={2: 3, 3: 4},
            scratch_shapes=[
                pltpu.SMEM((n_seq,), jnp.int32),
                pltpu.VMEM((SLOTS, JOB, rows, head), bf16),
                dma, dma, dma((n_jobs,)), dma((n_jobs,)), dma((2 * HELD,)),
            ],
            compiler_params=pltpu.CompilerParams(vmem_limit_bytes=W_VMEM * MIB),
            name='write',
        )(keep(positions, pltpu.HBM), *[keep(x, pltpu.VMEM) for x in (h_vm, k_vm, v_vm, new_k, new_v)], k_flat, v_flat)
        return h_out, k_out.reshape(k_cache.shape), v_out.reshape(v_cache.shape)

    return jax.shard_map(
        local_step,
        mesh=mesh,
        in_specs=(P('dp', None), P(None), P(None, 'tp'), P('tp', None), cache_spec, cache_spec, P('dp')),
        out_specs=(P('dp', None), cache_spec, cache_spec),
        check_vma=False,
    )
```

```python
import math
import jax
import jax.numpy as jnp
import numpy as np
from jax import lax
from jax.experimental import pallas as pl
from jax.experimental.pallas import tpu as pltpu
from jax.sharding import PartitionSpec as P

MESH = pl.DeviceIdType.MESH
NEG = -1e30
MIB = 1024 * 1024
N_SP = 4
COLS = 3
PARTS = 2
PHASES = (3, 3, 2)
GROUP = 8
WINDOW_IN = 8
HELD = 7
JOB = 2
SLOTS = 4
WINDOW = 4
W_VMEM = 3


def attend_kernel(dims, pos_in, hidden_in, scale_in, freq_in, w_qkv, w_out, k_in, v_in,
                  h_out, k_vm, v_vm, new_k, new_v,
                  pos, hidden, norm_scale, inv_freq, u, wq, heads, rope_c, rope_s, wo, k_rest, v_rest, q_rows, kn_rows, vn_rows, tok, score, part, recv, merged, proj, proj_in, sums,
                  in_sem, w_sem, wo_sem, k_sem, v_sem, acc_send, acc_recv, part_send, part_recv, tp_send, tp_recv, x_send, x_recv,
                  core_send, core_recv, fwd_send, fwd_recv):
    n_seq, rows, kv, head, per_kv, d_model = dims
    n_heads = kv * per_kv
    n_groups = n_seq // GROUP
    pair_rows = 2 * n_heads
    own = n_seq // N_SP
    sp = lax.axis_index('sp')
    tp = lax.axis_index('tp')
    seq_local = rows // kv
    scale2 = head ** -0.5 * math.log2(math.e)

    core = lax.rem(sp, 2)
    partner = sp + 1 - 2 * core
    across = lax.rem(sp + 2, N_SP)
    half_cols = w_qkv.shape[1] // 2
    w_cols = 2 * head
    w_chunks = half_cols // w_cols

    def w_copy(c):
        cols = pl.ds(pl.multiple_of(core * half_cols + c * w_cols, head), w_cols)
        return pltpu.make_async_copy(w_qkv.at[:, cols], wq.at[c], w_sem.at[c])

    def held(ref, rest, n_held, g):
        return (ref, g) if g < n_held else (rest, g - n_held)

    def cache_copy(src, ref, rest, n_held, sem, g):
        dst, i = held(ref, rest, n_held, g)
        return pltpu.make_async_copy(src.at[pl.ds(g * GROUP, GROUP)], dst.at[pl.ds(i * GROUP, GROUP)], sem.at[g])

    def k_copy(g):
        return cache_copy(k_in, k_vm, k_rest, HELD, k_sem, g)

    def v_copy(g):
        return cache_copy(v_in, v_vm, v_rest, HELD, v_sem, g)

    width = d_model // COLS

    def wo_copy(c):
        return pltpu.make_async_copy(w_out.at[:, pl.ds(c * width, width)], wo.at[c], wo_sem.at[c])

    queue = [w_copy(c) for c in range(w_chunks)]
    g = 0
    for n in PHASES:
        queue += [k_copy(i) for i in range(g, g + n)] + [v_copy(i) for i in range(g, g + n)]
        g += n
    queue += [wo_copy(c) for c in range(COLS)]
    started = 0

    def start(n):
        nonlocal started
        for copy in queue[started:started + n]:
            copy.start()
        started += n

    small = [pltpu.make_async_copy(a, b, in_sem.at[i]) for i, (a, b) in enumerate(
        ((hidden_in, hidden), (scale_in, norm_scale), (freq_in, inv_freq), (pos_in, pos)))]
    for c in small:
        c.start()
    start(3)

    barrier = pltpu.get_barrier_semaphore()
    for s in range(1, N_SP):
        pl.semaphore_signal(barrier, inc=1, device_id={'sp': lax.rem(sp + s, N_SP)}, device_id_type=MESH)
    pl.semaphore_signal(barrier, inc=1, device_id={'tp': 1 - tp}, device_id_type=MESH)

    for c in small:
        c.wait()
    hid = hidden[...].astype(jnp.float32)
    mean = jnp.mean(hid, axis=-1, keepdims=True)
    cen = hid - mean
    var = jnp.mean(cen * cen, axis=-1, keepdims=True)
    scale_rows = norm_scale[...].astype(jnp.float32)
    scale_row = jnp.concatenate([scale_rows[i:i + 1] for i in range(scale_rows.shape[0])], axis=1)
    normed = (cen * lax.rsqrt(var + 1e-5) * scale_row).astype(jnp.bfloat16)
    u[...] = normed

    brow = lax.broadcasted_iota(jnp.int32, (n_seq, 1), 0)
    pos_col = jnp.zeros((n_seq, 1), jnp.int32)
    for b in range(n_seq):
        pos_col = jnp.where(brow == b, pos[b], pos_col)
    angles = pos_col.astype(jnp.float32) * inv_freq[...]
    c2 = jnp.cos(angles)
    s2 = jnp.sin(angles)
    s2 = jnp.where(lax.broadcasted_iota(jnp.int32, s2.shape, 1) < head // 2, -s2, s2)
    rope_c[...] = c2
    rope_s[...] = s2

    group_heads = per_kv + 2

    def heads_copy(c):
        mine = heads.at[core, pl.ds(2 * c, 2)]
        return pltpu.make_async_remote_copy(mine, mine, acc_send.at[c], acc_recv.at[c],
                                            device_id={'sp': partner}, device_id_type=MESH)

    for c in range(w_chunks):
        w_copy(c).wait()
        start((1, 1, 1, 1, 4)[c])
        k_half = d_model // 2
        qkv = (jnp.dot(u[:, :k_half], wq[c, :k_half], preferred_element_type=jnp.float32)
               + jnp.dot(u[:, k_half:], wq[c, k_half:], preferred_element_type=jnp.float32))
        for i in range(2):
            x = jnp.clip(qkv[:, i * head:(i + 1) * head].astype(jnp.bfloat16).astype(jnp.float32), -8.0, 8.0)
            if (2 * c + i) % group_heads <= per_kv:
                x = x * rope_c[...] + pltpu.roll(x, head // 2, 1) * rope_s[...]
                x = x.astype(jnp.bfloat16).astype(jnp.float32)
            heads[core, 2 * c + i] = x
        if c == 0:
            pl.semaphore_wait(barrier, N_SP)
        heads_copy(c).start()

    def spread(half, queries):
        for h in range(half_cols // head):
            g, j = half * (kv // 2) + h // group_heads, h % group_heads
            if queries != (j < per_kv):
                continue
            x = heads[half, h]
            if queries:
                q_rows[pl.ds(g * per_kv + j, n_seq, stride=n_heads), :] = x
                continue
            wide, rep = (kn_rows, new_k) if j == per_kv else (vn_rows, new_v)
            for i in range(per_kv):
                wide[pl.ds(g * per_kv + i, n_seq, stride=n_heads), :] = x
            for i in range(16 // kv):
                rep[pl.ds(i * kv + g, n_seq, stride=16), :] = x

    col = lax.broadcasted_iota(jnp.int32, (pair_rows, rows), 1)
    row = lax.broadcasted_iota(jnp.int32, (pair_rows, rows), 0)
    row_kv = lax.rem(row, n_heads) // per_kv
    tok[...] = jnp.where(lax.rem(col, kv) == row_kv, sp * seq_local + col // kv, 1 << 30)

    for half in range(2):
        @pl.when(core == half)
        def _():
            spread(half, True)

    for c in range(w_chunks):
        heads_copy(c).wait()
    for half in range(2):
        @pl.when(core != half)
        def _():
            spread(half, True)

    prow = lax.broadcasted_iota(jnp.int32, (pair_rows, 1), 0)
    first = prow < n_heads

    def part_copy(g, s):
        dst = lax.rem(sp + s, N_SP)
        return pltpu.make_async_remote_copy(
            src_ref=part.at[g, dst], dst_ref=recv.at[g, s - 1],
            send_sem=part_send.at[g, s - 1], recv_sem=part_recv.at[g, s - 1],
            device_id={'sp': dst}, device_id_type=MESH)

    lane = lax.broadcasted_iota(jnp.int32, (8, head), 1)
    n_stat = pair_rows // 8

    def scores(g, buf, k_ref, k_off):
        for d in range(N_SP):
            kb = g * GROUP + 2 * d - k_off
            q = q_rows[pl.ds(pl.multiple_of((g * N_SP + d) * pair_rows, 8), pair_rows), :]
            zero = jnp.zeros_like(q)
            q_blk = jnp.concatenate([jnp.where(first, q, zero), jnp.where(first, zero, q)], axis=1).astype(jnp.bfloat16)
            k_cat = jnp.concatenate([k_ref[kb], k_ref[kb + 1]], axis=1)
            score[buf, d] = lax.dot_general(q_blk, k_cat, (((1,), (1,)), ((), ())), preferred_element_type=jnp.float32)

    def values(g, buf, v_ref, v_off):
        for d in range(N_SP):
            b = g * GROUP + 2 * d
            vb = b - v_off
            limit = jnp.where(first, pos[b], pos[b + 1])
            s = jnp.where(tok[...] < limit, score[buf, d], NEG)
            m = jnp.max(s, axis=-1, keepdims=True)
            w = jnp.exp2((s - m) * scale2)
            l = jnp.sum(w, axis=-1, keepdims=True)
            v_cat = jnp.concatenate([v_ref[vb], v_ref[vb + 1]], axis=1)
            o = jnp.dot(w.astype(jnp.bfloat16), v_cat, preferred_element_type=jnp.float32)
            part[g, d, :pair_rows] = jnp.where(first, o[:, :head], o[:, head:])
            stat = jnp.zeros((8, head), jnp.float32)
            for i in range(n_stat):
                stat = jnp.where(lane == i, m[8 * i:8 * i + 8], stat)
                stat = jnp.where(lane == n_stat + i, l[8 * i:8 * i + 8], stat)
            part[g, d, pair_rows:] = stat
        for s in range(1, N_SP):
            part_copy(g, s).start()

    g = 0
    for n in PHASES:
        gs = range(g, g + n)
        g += n
        if g == n_groups:
            for half in range(2):
                spread(half, False)
        for i in gs:
            k_copy(i).wait()
            start(1)
        for i in gs:
            k_ref, ki = held(k_vm, k_rest, HELD, i)
            scores(i, i - gs[0], k_ref, (i - ki) * GROUP)
        for i in gs:
            v_copy(i).wait()
            start(1)
        for i in gs:
            v_ref, vi = held(v_vm, v_rest, HELD, i)
            values(i, i - gs[0], v_ref, (i - vi) * GROUP)
    start(len(queue))
    def merge_step(g, carry):
        for s in range(1, N_SP):
            part_copy(g, s).wait()
        r = pl.ds(pl.multiple_of((g * N_SP + sp) * pair_rows, 8), pair_rows)
        s_new = jnp.sum(q_rows[r, :] * kn_rows[r, :], axis=-1, keepdims=True)
        outs = [part[g, sp]] + [recv[g, s] for s in range(N_SP - 1)]

        def column(x, first_lane):
            return jnp.concatenate(
                [x[pair_rows:, first_lane + i:first_lane + i + 1] for i in range(n_stat)], axis=0)

        ms = [column(x, 0) for x in outs]
        ls = [column(x, n_stat) for x in outs]
        top = s_new
        for m in ms:
            top = jnp.maximum(top, m)
        f = jnp.exp2((s_new - top) * scale2)
        o = f * vn_rows[r, :]
        l = f
        for x, m, ll in zip(outs, ms, ls):
            f = jnp.exp2((m - top) * scale2)
            o = o + f * x[:pair_rows]
            l = l + f * ll
        merged[pl.ds(pl.multiple_of(g * pair_rows, 8), pair_rows), :] = o / l
        return carry

    def tp_copy(p, c):
        return pltpu.make_async_remote_copy(proj.at[p, c], proj_in.at[p, c], tp_send.at[p, c], tp_recv.at[p, c],
                                            device_id={'tp': 1 - tp}, device_id_type=MESH)

    def x_copy(p, c):
        return pltpu.make_async_remote_copy(sums.at[p, c, sp], sums.at[p, c, sp], x_send.at[p, c], x_recv.at[p, c],
                                            device_id={'sp': across}, device_id_type=MESH)

    def core_copy(p, c):
        return pltpu.make_async_remote_copy(sums.at[p, c, sp], sums.at[p, c, sp], core_send.at[p, c], core_recv.at[p, c],
                                            device_id={'sp': partner}, device_id_type=MESH)

    def fwd_copy(p, c):
        return pltpu.make_async_remote_copy(sums.at[p, c, across], sums.at[p, c, across], fwd_send.at[p, c], fwd_recv.at[p, c],
                                            device_id={'sp': partner}, device_id_type=MESH)

    part_groups = n_groups // PARTS
    part_rows = own // PARTS

    def gather_heads(p):
        lax.fori_loop(p * part_groups, (p + 1) * part_groups, merge_step, 0)
        first_row = p * part_groups * pair_rows
        return jnp.concatenate([merged[pl.ds(first_row + n, part_rows, stride=n_heads), :].astype(jnp.bfloat16)
                                for n in range(n_heads)], axis=1)

    def project(p, c, attn):
        proj[p, c] = jnp.dot(attn, wo[c], preferred_element_type=jnp.float32)
        tp_copy(p, c).start()

    def add_tp(p, c):
        tp_copy(p, c).wait()
        sums[p, c, sp] = proj[p, c] + proj_in[p, c]
        x_copy(p, c).start()
        core_copy(p, c).start()

    def forward(p, c):
        x_copy(p, c).wait()
        fwd_copy(p, c).start()

    attn = gather_heads(0)
    for c in range(COLS):
        wo_copy(c).wait()
        project(0, c, attn)
    attn = gather_heads(1)
    for c in range(COLS):
        project(1, c, attn)
        add_tp(0, c)
    for c in range(COLS):
        add_tp(1, c)
        forward(0, c)
    for c in range(COLS):
        forward(1, c)

    srow = lax.broadcasted_iota(jnp.int32, (GROUP, 1), 0)
    for p in range(PARTS):
        for c in range(COLS):
            core_copy(p, c).wait()
            fwd_copy(p, c).wait()
            lanes = slice(c * width, (c + 1) * width)
            for i in range(part_groups):
                gathered = None
                for d in range(N_SP):
                    x = sums[p, c, d]
                    shift = (2 * d - 2 * i) % GROUP
                    if shift:
                        x = pltpu.roll(x, shift, 0)
                    gathered = x if gathered is None else jnp.where(srow // 2 == d, x, gathered)
                r = slice((p * part_groups + i) * GROUP, (p * part_groups + i + 1) * GROUP)
                h_out[r, lanes] = (hidden[r, lanes].astype(jnp.float32) + gathered).astype(jnp.bfloat16)


def write_kernel(dims, pos_in, h_in, k_vm, v_vm, new_k, new_v, k_in, v_in, h_out, k_out, v_out, k_same, v_same,
                 pos, slots, pos_sem, h_sem, rd_sem, wr_sem, blk_sem):
    n_seq, rows, kv, _, _, _ = dims
    sp = lax.axis_index('sp')
    seq_local = rows // kv
    n_held = HELD * GROUP
    per = 16 // kv
    sub = lax.broadcasted_iota(jnp.int32, (16, 1), 0) // kv
    jobs = [(src, out, new, b) for src, out, new in ((k_in, k_out, new_k), (v_in, v_out, new_v))
            for b in range(n_held, n_seq, JOB)]

    def patch(ref, i, b, new):
        p = pos[b] - sp * seq_local
        blk = jnp.clip(p, 0, seq_local - 1) // per
        r = pl.ds(pl.multiple_of(blk * 16, 16), 16)
        fresh = new[pl.ds(pl.multiple_of(b * 16, 16), 16), :]
        ref[i, r, :] = jnp.where(sub + blk * per == p, fresh, ref[i, r, :].astype(jnp.float32)).astype(jnp.bfloat16)

    def read(j):
        src, _, _, b = jobs[j]
        return pltpu.make_async_copy(src.at[pl.ds(b, JOB)], slots.at[j % SLOTS], rd_sem.at[j])

    def write(j):
        _, out, _, b = jobs[j]
        return pltpu.make_async_copy(slots.at[j % SLOTS], out.at[pl.ds(b, JOB)], wr_sem.at[j])

    def run(j):
        _, _, new, b = jobs[j]
        read(j).wait()
        for i in range(JOB):
            patch(slots.at[j % SLOTS], i, b + i, new)
        write(j).start()

    def again(j):
        write(j - SLOTS).wait()
        read(j).start()

    def block(n):
        vm, out = ((k_vm, k_out), (v_vm, v_out))[n % 2]
        s = pl.ds(n // 2 * GROUP, GROUP)
        return pltpu.make_async_copy(vm.at[s], out.at[s], blk_sem.at[n])

    def send(n):
        vm, new = ((k_vm, new_k), (v_vm, new_v))[n % 2]
        for i in range(GROUP):
            b = n // 2 * GROUP + i
            patch(vm, b, b, new)
        block(n).start()

    n_blocks = 2 * HELD
    pos_copy = pltpu.make_async_copy(pos_in, pos, pos_sem)
    pos_copy.start()
    h_copy = pltpu.make_async_copy(h_in, h_out, h_sem)
    h_copy.start()
    for j in range(SLOTS):
        read(j).start()
    pos_copy.wait()
    for n in range(n_blocks):
        if n >= WINDOW:
            block(n - WINDOW).wait()
        send(n)
        for j in range(len(jobs)):
            if j < SLOTS and n == WINDOW + j // 2 - 1:
                run(j)
            if j >= SLOTS and n == WINDOW + 2 + j // 2:
                again(j)
            if j >= SLOTS and n == WINDOW + 4 + j // 2:
                run(j)
    for n in range(n_blocks - WINDOW, n_blocks):
        block(n).wait()
    for j in range(len(jobs) - SLOTS, len(jobs)):
        write(j).wait()
    h_copy.wait()


def solution(mesh):
    cache_spec = P('dp', 'sp', 'tp', None)

    def local_step(hidden, norm_scale, w_qkv, w_out, k_cache, v_cache, positions):
        n_seq, seq_local, kv, head = k_cache.shape
        d_model = hidden.shape[1]
        per_kv = w_qkv.shape[1] // (kv * head) - 2
        rows = seq_local * kv
        n_heads = kv * per_kv
        n_groups = n_seq // GROUP
        pair_rows = 2 * n_heads
        own = n_seq // N_SP
        w_chunks = w_qkv.shape[1] // (4 * head)
        n_jobs = 2 * (n_seq - HELD * GROUP) // JOB
        dims = (n_seq, rows, kv, head, per_kv, d_model)
        half = np.arange(head) % (head // 2)
        inv_freq = np.exp(half * (-2.0 * math.log(500000.0) / head)).astype(np.float32)[None]
        f32, bf16 = jnp.float32, jnp.bfloat16
        vmem = pl.BlockSpec(memory_space=pltpu.VMEM)
        hbm = pl.BlockSpec(memory_space=pltpu.HBM)
        cache = (n_seq, rows, head)
        dma = pltpu.SemaphoreType.DMA
        keep = pltpu.with_memory_space_constraint
        w_qkv, w_out = keep(w_qkv, pltpu.HBM), keep(w_out, pltpu.HBM)
        k_flat = keep(k_cache.reshape(cache), pltpu.HBM)
        v_flat = keep(v_cache.reshape(cache), pltpu.HBM)
        h_vm, k_vm, v_vm, new_k, new_v = pl.pallas_call(
            lambda *refs: attend_kernel(dims, *refs),
            out_shape=(pltpu.VMEM(hidden.shape, bf16),
                       pltpu.VMEM((HELD * GROUP, rows, head), bf16),
                       pltpu.VMEM((HELD * GROUP, rows, head), bf16),
                       pltpu.VMEM((n_seq * 16, head), f32),
                       pltpu.VMEM((n_seq * 16, head), f32)),
            in_specs=[hbm] * 8,
            out_specs=(vmem,) * 5,
            scratch_shapes=[
                pltpu.SMEM((n_seq,), jnp.int32),
                pltpu.VMEM(hidden.shape, bf16),
                pltpu.VMEM((d_model // head, head), bf16),
                pltpu.VMEM((1, head), f32),
                pltpu.VMEM(hidden.shape, bf16),
                pltpu.VMEM((w_chunks, d_model, 2 * head), bf16),
                pltpu.VMEM((2, 2 * w_chunks, n_seq, head), f32),
                pltpu.VMEM((n_seq, head), f32),
                pltpu.VMEM((n_seq, head), f32),
                pltpu.VMEM((COLS, w_out.shape[0], d_model // COLS), bf16),
                pltpu.VMEM((n_seq - HELD * GROUP, rows, head), bf16),
                pltpu.VMEM((n_seq - HELD * GROUP, rows, head), bf16),
                pltpu.VMEM((n_seq * n_heads, head), f32),
                pltpu.VMEM((n_seq * n_heads, head), f32),
                pltpu.VMEM((n_seq * n_heads, head), f32),
                pltpu.VMEM((pair_rows, rows), jnp.int32),
                pltpu.VMEM((max(PHASES), N_SP, pair_rows, rows), f32),
                pltpu.VMEM((n_groups, N_SP, pair_rows + 8, head), f32),
                pltpu.VMEM((n_groups, N_SP - 1, pair_rows + 8, head), f32),
                pltpu.VMEM((own * n_heads, head), f32),
                pltpu.VMEM((PARTS, COLS, own // PARTS, d_model // COLS), f32),
                pltpu.VMEM((PARTS, COLS, own // PARTS, d_model // COLS), f32),
                pltpu.VMEM((PARTS, COLS, N_SP, own // PARTS, d_model // COLS), f32),
                dma((4,)), dma((w_chunks,)), dma((COLS,)), dma((n_groups,)), dma((n_groups,)),
                dma((w_chunks,)), dma((w_chunks,)),
                dma((n_groups, N_SP - 1)), dma((n_groups, N_SP - 1)),
            ] + [dma((PARTS, COLS))] * 8,
            compiler_params=pltpu.CompilerParams(
                collective_id=0, has_side_effects=True, vmem_limit_bytes=33 * MIB),
            name='attend',
        )(keep(positions, pltpu.HBM), keep(hidden, pltpu.HBM),
          keep(norm_scale.reshape(d_model // head, head), pltpu.HBM), inv_freq, w_qkv, w_out, k_flat, v_flat)
        h_out, k_out, v_out, _, _ = pl.pallas_call(
            lambda *refs: write_kernel(dims, *refs),
            out_shape=(jax.ShapeDtypeStruct(hidden.shape, bf16),
                       jax.ShapeDtypeStruct(cache, bf16), jax.ShapeDtypeStruct(cache, bf16),
                       pltpu.VMEM(k_vm.shape, bf16), pltpu.VMEM(v_vm.shape, bf16)),
            in_specs=[hbm] + [vmem] * 5 + [hbm] * 2,
            out_specs=(hbm,) * 3 + (vmem,) * 2,
            input_output_aliases={2: 3, 3: 4},
            scratch_shapes=[
                pltpu.SMEM((n_seq,), jnp.int32),
                pltpu.VMEM((SLOTS, JOB, rows, head), bf16),
                dma, dma, dma((n_jobs,)), dma((n_jobs,)), dma((2 * HELD,)),
            ],
            compiler_params=pltpu.CompilerParams(vmem_limit_bytes=W_VMEM * MIB),
            name='write',
        )(keep(positions, pltpu.HBM), *[keep(x, pltpu.VMEM) for x in (h_vm, k_vm, v_vm, new_k, new_v)], k_flat, v_flat)
        return h_out, k_out.reshape(k_cache.shape), v_out.reshape(v_cache.shape)

    return jax.shard_map(
        local_step,
        mesh=mesh,
        in_specs=(P('dp', None), P(None), P(None, 'tp'), P('tp', None), cache_spec, cache_spec, P('dp')),
        out_specs=(P('dp', None), cache_spec, cache_spec),
        check_vma=False,
    )
```

```python
import math
import jax
import jax.numpy as jnp
import numpy as np
from jax import lax
from jax.experimental import pallas as pl
from jax.experimental.pallas import tpu as pltpu
from jax.sharding import PartitionSpec as P

MESH = pl.DeviceIdType.MESH
NEG = -1e30
MIB = 1024 * 1024
N_SP = 4
COLS = 3
PARTS = 2
PHASES = (2, 2, 2, 2)
GROUP = 8
FIRST = 3
STARTS = (1, 1, 1, 2, 4)
HELD = 7
JOB = 2
SLOTS = 4
WINDOW = 4
W_VMEM = 3


def attend_kernel(dims, pos_in, hidden_in, scale_in, freq_in, w_qkv, w_out, k_in, v_in,
                  h_out, k_vm, v_vm, new_k, new_v,
                  pos, hidden, norm_scale, inv_freq, u, wq, heads, rope_c, rope_s, wo, k_rest, v_rest, q_rows, kn_rows, vn_rows, tok, score, part, recv, merged, proj, proj_in, sums,
                  in_sem, w_sem, wo_sem, k_sem, v_sem, acc_send, acc_recv, part_send, part_recv, tp_send, tp_recv, x_send, x_recv,
                  core_send, core_recv, fwd_send, fwd_recv):
    n_seq, rows, kv, head, per_kv, d_model = dims
    n_heads = kv * per_kv
    n_groups = n_seq // GROUP
    pair_rows = 2 * n_heads
    own = n_seq // N_SP
    sp = lax.axis_index('sp')
    tp = lax.axis_index('tp')
    seq_local = rows // kv
    scale2 = head ** -0.5 * math.log2(math.e)

    core = lax.rem(sp, 2)
    partner = sp + 1 - 2 * core
    across = lax.rem(sp + 2, N_SP)
    half_cols = w_qkv.shape[1] // 2
    w_cols = 2 * head
    w_chunks = half_cols // w_cols

    def w_copy(c):
        cols = pl.ds(pl.multiple_of(core * half_cols + c * w_cols, head), w_cols)
        return pltpu.make_async_copy(w_qkv.at[:, cols], wq.at[c], w_sem.at[c])

    def held(ref, rest, n_held, g):
        return (ref, g) if g < n_held else (rest, g - n_held)

    def cache_copy(src, ref, rest, n_held, sem, g):
        dst, i = held(ref, rest, n_held, g)
        return pltpu.make_async_copy(src.at[pl.ds(g * GROUP, GROUP)], dst.at[pl.ds(i * GROUP, GROUP)], sem.at[g])

    def k_copy(g):
        return cache_copy(k_in, k_vm, k_rest, HELD, k_sem, g)

    def v_copy(g):
        return cache_copy(v_in, v_vm, v_rest, HELD, v_sem, g)

    width = d_model // COLS

    def wo_copy(c):
        return pltpu.make_async_copy(w_out.at[:, pl.ds(c * width, width)], wo.at[c], wo_sem.at[c])

    queue = [w_copy(c) for c in range(w_chunks)]
    g = 0
    for n in PHASES:
        queue += [k_copy(i) for i in range(g, g + n)] + [v_copy(i) for i in range(g, g + n)]
        g += n
    queue += [wo_copy(c) for c in range(COLS)]
    started = 0

    def start(n):
        nonlocal started
        for copy in queue[started:started + n]:
            copy.start()
        started += n

    small = [pltpu.make_async_copy(a, b, in_sem.at[i]) for i, (a, b) in enumerate(
        ((hidden_in, hidden), (scale_in, norm_scale), (freq_in, inv_freq), (pos_in, pos)))]
    for c in small:
        c.start()
    start(FIRST)

    barrier = pltpu.get_barrier_semaphore()
    for s in range(1, N_SP):
        pl.semaphore_signal(barrier, inc=1, device_id={'sp': lax.rem(sp + s, N_SP)}, device_id_type=MESH)
    pl.semaphore_signal(barrier, inc=1, device_id={'tp': 1 - tp}, device_id_type=MESH)

    for c in small:
        c.wait()
    hid = hidden[...].astype(jnp.float32)
    mean = jnp.mean(hid, axis=-1, keepdims=True)
    cen = hid - mean
    var = jnp.mean(cen * cen, axis=-1, keepdims=True)
    scale_rows = norm_scale[...].astype(jnp.float32)
    scale_row = jnp.concatenate([scale_rows[i:i + 1] for i in range(scale_rows.shape[0])], axis=1)
    normed = (cen * lax.rsqrt(var + 1e-5) * scale_row).astype(jnp.bfloat16)
    u[...] = normed

    brow = lax.broadcasted_iota(jnp.int32, (n_seq, 1), 0)
    pos_col = jnp.zeros((n_seq, 1), jnp.int32)
    for b in range(n_seq):
        pos_col = jnp.where(brow == b, pos[b], pos_col)
    angles = pos_col.astype(jnp.float32) * inv_freq[...]
    c2 = jnp.cos(angles)
    s2 = jnp.sin(angles)
    s2 = jnp.where(lax.broadcasted_iota(jnp.int32, s2.shape, 1) < head // 2, -s2, s2)
    rope_c[...] = c2
    rope_s[...] = s2

    group_heads = per_kv + 2

    def heads_copy(c):
        mine = heads.at[core, pl.ds(2 * c, 2)]
        return pltpu.make_async_remote_copy(mine, mine, acc_send.at[c], acc_recv.at[c],
                                            device_id={'sp': partner}, device_id_type=MESH)

    for c in range(w_chunks):
        w_copy(c).wait()
        start(STARTS[c])
        k_half = d_model // 2
        qkv = (jnp.dot(u[:, :k_half], wq[c, :k_half], preferred_element_type=jnp.float32)
               + jnp.dot(u[:, k_half:], wq[c, k_half:], preferred_element_type=jnp.float32))
        for i in range(2):
            x = jnp.clip(qkv[:, i * head:(i + 1) * head].astype(jnp.bfloat16).astype(jnp.float32), -8.0, 8.0)
            if (2 * c + i) % group_heads <= per_kv:
                x = x * rope_c[...] + pltpu.roll(x, head // 2, 1) * rope_s[...]
                x = x.astype(jnp.bfloat16).astype(jnp.float32)
            heads[core, 2 * c + i] = x
        if c == 0:
            pl.semaphore_wait(barrier, N_SP)
        heads_copy(c).start()

    def spread(half, queries):
        for h in range(half_cols // head):
            g, j = half * (kv // 2) + h // group_heads, h % group_heads
            if queries != (j < per_kv):
                continue
            x = heads[half, h]
            if queries:
                q_rows[pl.ds(g * per_kv + j, n_seq, stride=n_heads), :] = x
                continue
            wide, rep = (kn_rows, new_k) if j == per_kv else (vn_rows, new_v)
            for i in range(per_kv):
                wide[pl.ds(g * per_kv + i, n_seq, stride=n_heads), :] = x
            for i in range(16 // kv):
                rep[pl.ds(i * kv + g, n_seq, stride=16), :] = x

    col = lax.broadcasted_iota(jnp.int32, (pair_rows, rows), 1)
    row = lax.broadcasted_iota(jnp.int32, (pair_rows, rows), 0)
    row_kv = lax.rem(row, n_heads) // per_kv
    tok[...] = jnp.where(lax.rem(col, kv) == row_kv, sp * seq_local + col // kv, 1 << 30)

    for half in range(2):
        @pl.when(core == half)
        def _():
            spread(half, True)

    for c in range(w_chunks - 1):
        heads_copy(c).wait()
    for half in range(2):
        @pl.when(core != half)
        def _():
            spread(half, True)

    prow = lax.broadcasted_iota(jnp.int32, (pair_rows, 1), 0)
    first = prow < n_heads

    def part_copy(g, s):
        dst = lax.rem(sp + s, N_SP)
        return pltpu.make_async_remote_copy(
            src_ref=part.at[g, dst], dst_ref=recv.at[g, s - 1],
            send_sem=part_send.at[g, s - 1], recv_sem=part_recv.at[g, s - 1],
            device_id={'sp': dst}, device_id_type=MESH)

    lane = lax.broadcasted_iota(jnp.int32, (8, head), 1)
    n_stat = pair_rows // 8

    def scores(g, buf, k_ref, k_off):
        for d in range(N_SP):
            kb = g * GROUP + 2 * d - k_off
            q = q_rows[pl.ds(pl.multiple_of((g * N_SP + d) * pair_rows, 8), pair_rows), :]
            zero = jnp.zeros_like(q)
            q_blk = jnp.concatenate([jnp.where(first, q, zero), jnp.where(first, zero, q)], axis=1).astype(jnp.bfloat16)
            k_cat = jnp.concatenate([k_ref[kb], k_ref[kb + 1]], axis=1)
            score[buf, d] = lax.dot_general(q_blk, k_cat, (((1,), (1,)), ((), ())), preferred_element_type=jnp.float32)

    def values(g, buf, v_ref, v_off):
        for d in range(N_SP):
            b = g * GROUP + 2 * d
            vb = b - v_off
            limit = jnp.where(first, pos[b], pos[b + 1])
            s = jnp.where(tok[...] < limit, score[buf, d], NEG)
            m = jnp.max(s, axis=-1, keepdims=True)
            w = jnp.exp2((s - m) * scale2)
            l = jnp.sum(w, axis=-1, keepdims=True)
            v_cat = jnp.concatenate([v_ref[vb], v_ref[vb + 1]], axis=1)
            o = jnp.dot(w.astype(jnp.bfloat16), v_cat, preferred_element_type=jnp.float32)
            part[g, d, :pair_rows] = jnp.where(first, o[:, :head], o[:, head:])
            stat = jnp.zeros((8, head), jnp.float32)
            for i in range(n_stat):
                stat = jnp.where(lane == i, m[8 * i:8 * i + 8], stat)
                stat = jnp.where(lane == n_stat + i, l[8 * i:8 * i + 8], stat)
            part[g, d, pair_rows:] = stat
        for s in range(1, N_SP):
            part_copy(g, s).start()

    g = 0
    for n in PHASES:
        gs = range(g, g + n)
        g += n
        if g == n_groups:
            heads_copy(w_chunks - 1).wait()
            for half in range(2):
                spread(half, False)
        for i in gs:
            k_copy(i).wait()
            start(1)
        for i in gs:
            k_ref, ki = held(k_vm, k_rest, HELD, i)
            scores(i, i - gs[0], k_ref, (i - ki) * GROUP)
        for i in gs:
            v_copy(i).wait()
            start(1)
        for i in gs:
            v_ref, vi = held(v_vm, v_rest, HELD, i)
            values(i, i - gs[0], v_ref, (i - vi) * GROUP)
    start(len(queue))
    def merge_step(g, carry):
        for s in range(1, N_SP):
            part_copy(g, s).wait()
        r = pl.ds(pl.multiple_of((g * N_SP + sp) * pair_rows, 8), pair_rows)
        s_new = jnp.sum(q_rows[r, :] * kn_rows[r, :], axis=-1, keepdims=True)
        outs = [part[g, sp]] + [recv[g, s] for s in range(N_SP - 1)]

        def column(x, first_lane):
            return jnp.concatenate(
                [x[pair_rows:, first_lane + i:first_lane + i + 1] for i in range(n_stat)], axis=0)

        ms = [column(x, 0) for x in outs]
        ls = [column(x, n_stat) for x in outs]
        top = s_new
        for m in ms:
            top = jnp.maximum(top, m)
        f = jnp.exp2((s_new - top) * scale2)
        o = f * vn_rows[r, :]
        l = f
        for x, m, ll in zip(outs, ms, ls):
            f = jnp.exp2((m - top) * scale2)
            o = o + f * x[:pair_rows]
            l = l + f * ll
        merged[pl.ds(pl.multiple_of(g * pair_rows, 8), pair_rows), :] = o / l
        return carry

    def tp_copy(p, c):
        return pltpu.make_async_remote_copy(proj.at[p, c], proj_in.at[p, c], tp_send.at[p, c], tp_recv.at[p, c],
                                            device_id={'tp': 1 - tp}, device_id_type=MESH)

    def x_copy(p, c):
        return pltpu.make_async_remote_copy(sums.at[p, c, sp], sums.at[p, c, sp], x_send.at[p, c], x_recv.at[p, c],
                                            device_id={'sp': across}, device_id_type=MESH)

    def core_copy(p, c):
        return pltpu.make_async_remote_copy(sums.at[p, c, sp], sums.at[p, c, sp], core_send.at[p, c], core_recv.at[p, c],
                                            device_id={'sp': partner}, device_id_type=MESH)

    def fwd_copy(p, c):
        return pltpu.make_async_remote_copy(sums.at[p, c, across], sums.at[p, c, across], fwd_send.at[p, c], fwd_recv.at[p, c],
                                            device_id={'sp': partner}, device_id_type=MESH)

    part_groups = n_groups // PARTS
    part_rows = own // PARTS

    def gather_heads(p):
        lax.fori_loop(p * part_groups, (p + 1) * part_groups, merge_step, 0)
        first_row = p * part_groups * pair_rows
        return jnp.concatenate([merged[pl.ds(first_row + n, part_rows, stride=n_heads), :].astype(jnp.bfloat16)
                                for n in range(n_heads)], axis=1)

    def project(p, c, attn):
        proj[p, c] = jnp.dot(attn, wo[c], preferred_element_type=jnp.float32)
        tp_copy(p, c).start()

    def add_tp(p, c):
        tp_copy(p, c).wait()
        sums[p, c, sp] = proj[p, c] + proj_in[p, c]
        x_copy(p, c).start()
        core_copy(p, c).start()

    def forward(p, c):
        x_copy(p, c).wait()
        fwd_copy(p, c).start()

    attn = gather_heads(0)
    for c in range(COLS):
        wo_copy(c).wait()
        project(0, c, attn)
    attn = gather_heads(1)
    for c in range(COLS):
        project(1, c, attn)
        add_tp(0, c)
    for c in range(COLS):
        add_tp(1, c)
        forward(0, c)
    for c in range(COLS):
        forward(1, c)

    srow = lax.broadcasted_iota(jnp.int32, (GROUP, 1), 0)
    for p in range(PARTS):
        for c in range(COLS):
            core_copy(p, c).wait()
            fwd_copy(p, c).wait()
            lanes = slice(c * width, (c + 1) * width)
            for i in range(part_groups):
                gathered = None
                for d in range(N_SP):
                    x = sums[p, c, d]
                    shift = (2 * d - 2 * i) % GROUP
                    if shift:
                        x = pltpu.roll(x, shift, 0)
                    gathered = x if gathered is None else jnp.where(srow // 2 == d, x, gathered)
                r = slice((p * part_groups + i) * GROUP, (p * part_groups + i + 1) * GROUP)
                h_out[r, lanes] = (hidden[r, lanes].astype(jnp.float32) + gathered).astype(jnp.bfloat16)


def write_kernel(dims, pos_in, h_in, k_vm, v_vm, new_k, new_v, k_in, v_in, h_out, k_out, v_out, k_same, v_same,
                 pos, slots, pos_sem, h_sem, rd_sem, wr_sem, blk_sem):
    n_seq, rows, kv, _, _, _ = dims
    sp = lax.axis_index('sp')
    seq_local = rows // kv
    n_held = HELD * GROUP
    per = 16 // kv
    sub = lax.broadcasted_iota(jnp.int32, (16, 1), 0) // kv
    jobs = [(src, out, new, b) for src, out, new in ((k_in, k_out, new_k), (v_in, v_out, new_v))
            for b in range(n_held, n_seq, JOB)]

    def patch(ref, i, b, new):
        p = pos[b] - sp * seq_local
        blk = jnp.clip(p, 0, seq_local - 1) // per
        r = pl.ds(pl.multiple_of(blk * 16, 16), 16)
        fresh = new[pl.ds(pl.multiple_of(b * 16, 16), 16), :]
        ref[i, r, :] = jnp.where(sub + blk * per == p, fresh, ref[i, r, :].astype(jnp.float32)).astype(jnp.bfloat16)

    def read(j):
        src, _, _, b = jobs[j]
        return pltpu.make_async_copy(src.at[pl.ds(b, JOB)], slots.at[j % SLOTS], rd_sem.at[j])

    def write(j):
        _, out, _, b = jobs[j]
        return pltpu.make_async_copy(slots.at[j % SLOTS], out.at[pl.ds(b, JOB)], wr_sem.at[j])

    def run(j):
        _, _, new, b = jobs[j]
        read(j).wait()
        for i in range(JOB):
            patch(slots.at[j % SLOTS], i, b + i, new)
        write(j).start()

    def again(j):
        write(j - SLOTS).wait()
        read(j).start()

    def block(n):
        vm, out = ((k_vm, k_out), (v_vm, v_out))[n % 2]
        s = pl.ds(n // 2 * GROUP, GROUP)
        return pltpu.make_async_copy(vm.at[s], out.at[s], blk_sem.at[n])

    def send(n):
        vm, new = ((k_vm, new_k), (v_vm, new_v))[n % 2]
        for i in range(GROUP):
            b = n // 2 * GROUP + i
            patch(vm, b, b, new)
        block(n).start()

    n_blocks = 2 * HELD
    pos_copy = pltpu.make_async_copy(pos_in, pos, pos_sem)
    pos_copy.start()
    h_copy = pltpu.make_async_copy(h_in, h_out, h_sem)
    h_copy.start()
    for j in range(SLOTS):
        read(j).start()
    pos_copy.wait()
    for n in range(n_blocks):
        if n >= WINDOW:
            block(n - WINDOW).wait()
        send(n)
        for j in range(len(jobs)):
            if j < SLOTS and n == WINDOW + j // 2 - 1:
                run(j)
            if j >= SLOTS and n == WINDOW + 2 + j // 2:
                again(j)
            if j >= SLOTS and n == WINDOW + 4 + j // 2:
                run(j)
    for n in range(n_blocks - WINDOW, n_blocks):
        block(n).wait()
    for j in range(len(jobs) - SLOTS, len(jobs)):
        write(j).wait()
    h_copy.wait()


def solution(mesh):
    cache_spec = P('dp', 'sp', 'tp', None)

    def local_step(hidden, norm_scale, w_qkv, w_out, k_cache, v_cache, positions):
        n_seq, seq_local, kv, head = k_cache.shape
        d_model = hidden.shape[1]
        per_kv = w_qkv.shape[1] // (kv * head) - 2
        rows = seq_local * kv
        n_heads = kv * per_kv
        n_groups = n_seq // GROUP
        pair_rows = 2 * n_heads
        own = n_seq // N_SP
        w_chunks = w_qkv.shape[1] // (4 * head)
        n_jobs = 2 * (n_seq - HELD * GROUP) // JOB
        dims = (n_seq, rows, kv, head, per_kv, d_model)
        half = np.arange(head) % (head // 2)
        inv_freq = np.exp(half * (-2.0 * math.log(500000.0) / head)).astype(np.float32)[None]
        f32, bf16 = jnp.float32, jnp.bfloat16
        vmem = pl.BlockSpec(memory_space=pltpu.VMEM)
        hbm = pl.BlockSpec(memory_space=pltpu.HBM)
        cache = (n_seq, rows, head)
        dma = pltpu.SemaphoreType.DMA
        keep = pltpu.with_memory_space_constraint
        w_qkv, w_out = keep(w_qkv, pltpu.HBM), keep(w_out, pltpu.HBM)
        k_flat = keep(k_cache.reshape(cache), pltpu.HBM)
        v_flat = keep(v_cache.reshape(cache), pltpu.HBM)
        h_vm, k_vm, v_vm, new_k, new_v = pl.pallas_call(
            lambda *refs: attend_kernel(dims, *refs),
            out_shape=(pltpu.VMEM(hidden.shape, bf16),
                       pltpu.VMEM((HELD * GROUP, rows, head), bf16),
                       pltpu.VMEM((HELD * GROUP, rows, head), bf16),
                       pltpu.VMEM((n_seq * 16, head), f32),
                       pltpu.VMEM((n_seq * 16, head), f32)),
            in_specs=[hbm] * 8,
            out_specs=(vmem,) * 5,
            scratch_shapes=[
                pltpu.SMEM((n_seq,), jnp.int32),
                pltpu.VMEM(hidden.shape, bf16),
                pltpu.VMEM((d_model // head, head), bf16),
                pltpu.VMEM((1, head), f32),
                pltpu.VMEM(hidden.shape, bf16),
                pltpu.VMEM((w_chunks, d_model, 2 * head), bf16),
                pltpu.VMEM((2, 2 * w_chunks, n_seq, head), f32),
                pltpu.VMEM((n_seq, head), f32),
                pltpu.VMEM((n_seq, head), f32),
                pltpu.VMEM((COLS, w_out.shape[0], d_model // COLS), bf16),
                pltpu.VMEM((n_seq - HELD * GROUP, rows, head), bf16),
                pltpu.VMEM((n_seq - HELD * GROUP, rows, head), bf16),
                pltpu.VMEM((n_seq * n_heads, head), f32),
                pltpu.VMEM((n_seq * n_heads, head), f32),
                pltpu.VMEM((n_seq * n_heads, head), f32),
                pltpu.VMEM((pair_rows, rows), jnp.int32),
                pltpu.VMEM((max(PHASES), N_SP, pair_rows, rows), f32),
                pltpu.VMEM((n_groups, N_SP, pair_rows + 8, head), f32),
                pltpu.VMEM((n_groups, N_SP - 1, pair_rows + 8, head), f32),
                pltpu.VMEM((own * n_heads, head), f32),
                pltpu.VMEM((PARTS, COLS, own // PARTS, d_model // COLS), f32),
                pltpu.VMEM((PARTS, COLS, own // PARTS, d_model // COLS), f32),
                pltpu.VMEM((PARTS, COLS, N_SP, own // PARTS, d_model // COLS), f32),
                dma((4,)), dma((w_chunks,)), dma((COLS,)), dma((n_groups,)), dma((n_groups,)),
                dma((w_chunks,)), dma((w_chunks,)),
                dma((n_groups, N_SP - 1)), dma((n_groups, N_SP - 1)),
            ] + [dma((PARTS, COLS))] * 8,
            compiler_params=pltpu.CompilerParams(
                collective_id=0, has_side_effects=True, vmem_limit_bytes=33 * MIB),
            name='attend',
        )(keep(positions, pltpu.HBM), keep(hidden, pltpu.HBM),
          keep(norm_scale.reshape(d_model // head, head), pltpu.HBM), inv_freq, w_qkv, w_out, k_flat, v_flat)
        h_out, k_out, v_out, _, _ = pl.pallas_call(
            lambda *refs: write_kernel(dims, *refs),
            out_shape=(jax.ShapeDtypeStruct(hidden.shape, bf16),
                       jax.ShapeDtypeStruct(cache, bf16), jax.ShapeDtypeStruct(cache, bf16),
                       pltpu.VMEM(k_vm.shape, bf16), pltpu.VMEM(v_vm.shape, bf16)),
            in_specs=[hbm] + [vmem] * 5 + [hbm] * 2,
            out_specs=(hbm,) * 3 + (vmem,) * 2,
            input_output_aliases={2: 3, 3: 4},
            scratch_shapes=[
                pltpu.SMEM((n_seq,), jnp.int32),
                pltpu.VMEM((SLOTS, JOB, rows, head), bf16),
                dma, dma, dma((n_jobs,)), dma((n_jobs,)), dma((2 * HELD,)),
            ],
            compiler_params=pltpu.CompilerParams(vmem_limit_bytes=W_VMEM * MIB),
            name='write',
        )(keep(positions, pltpu.HBM), *[keep(x, pltpu.VMEM) for x in (h_vm, k_vm, v_vm, new_k, new_v)], k_flat, v_flat)
        return h_out, k_out.reshape(k_cache.shape), v_out.reshape(v_cache.shape)

    return jax.shard_map(
        local_step,
        mesh=mesh,
        in_specs=(P('dp', None), P(None), P(None, 'tp'), P('tp', None), cache_spec, cache_spec, P('dp')),
        out_specs=(P('dp', None), cache_spec, cache_spec),
        check_vma=False,
    )
```

```python
import math
import jax
import jax.numpy as jnp
import numpy as np
from jax import lax
from jax.experimental import pallas as pl
from jax.experimental.pallas import tpu as pltpu
from jax.sharding import PartitionSpec as P

MESH = pl.DeviceIdType.MESH
NEG = -1e30
MIB = 1024 * 1024
N_SP = 4
COLS = 3
PARTS = 2
MERGES = (((0, 1, 2, 3),), ((4, 5), (6, 7)))
PHASES = (2, 2, 2, 2)
GROUP = 8
FIRST = 3
STARTS = (1, 1, 1, 2, 4)
HELD = 7
JOB = 2
SLOTS = 4
WINDOW = 4
W_VMEM = 3


def attend_kernel(dims, pos_in, hidden_in, scale_in, freq_in, w_qkv, w_out, k_in, v_in,
                  h_out, k_vm, v_vm, new_k, new_v,
                  pos, hidden, norm_scale, inv_freq, u, wq, heads, rope_c, rope_s, wo, k_rest, v_rest, q_rows, kn_rows, vn_rows, tok, score, part, recv, merged, proj, proj_in, sums,
                  in_sem, w_sem, wo_sem, k_sem, v_sem, acc_send, acc_recv, part_send, part_recv, tp_send, tp_recv, x_send, x_recv,
                  core_send, core_recv, fwd_send, fwd_recv):
    n_seq, rows, kv, head, per_kv, d_model = dims
    n_heads = kv * per_kv
    n_groups = n_seq // GROUP
    pair_rows = 2 * n_heads
    own = n_seq // N_SP
    sp = lax.axis_index('sp')
    tp = lax.axis_index('tp')
    seq_local = rows // kv
    scale2 = head ** -0.5 * math.log2(math.e)

    core = lax.rem(sp, 2)
    partner = sp + 1 - 2 * core
    across = lax.rem(sp + 2, N_SP)
    half_cols = w_qkv.shape[1] // 2
    w_cols = 2 * head
    w_chunks = half_cols // w_cols

    def w_copy(c):
        cols = pl.ds(pl.multiple_of(core * half_cols + c * w_cols, head), w_cols)
        return pltpu.make_async_copy(w_qkv.at[:, cols], wq.at[c], w_sem.at[c])

    def held(ref, rest, n_held, g):
        return (ref, g) if g < n_held else (rest, g - n_held)

    def cache_copy(src, ref, rest, n_held, sem, g):
        dst, i = held(ref, rest, n_held, g)
        return pltpu.make_async_copy(src.at[pl.ds(g * GROUP, GROUP)], dst.at[pl.ds(i * GROUP, GROUP)], sem.at[g])

    def k_copy(g):
        return cache_copy(k_in, k_vm, k_rest, HELD, k_sem, g)

    def v_copy(g):
        return cache_copy(v_in, v_vm, v_rest, HELD, v_sem, g)

    width = d_model // COLS

    def wo_copy(c):
        return pltpu.make_async_copy(w_out.at[:, pl.ds(c * width, width)], wo.at[c], wo_sem.at[c])

    queue = [w_copy(c) for c in range(w_chunks)]
    g = 0
    for n in PHASES:
        queue += [k_copy(i) for i in range(g, g + n)] + [v_copy(i) for i in range(g, g + n)]
        g += n
    queue += [wo_copy(c) for c in range(COLS)]
    started = 0

    def start(n):
        nonlocal started
        for copy in queue[started:started + n]:
            copy.start()
        started += n

    small = [pltpu.make_async_copy(a, b, in_sem.at[i]) for i, (a, b) in enumerate(
        ((hidden_in, hidden), (scale_in, norm_scale), (freq_in, inv_freq), (pos_in, pos)))]
    for c in small:
        c.start()
    start(FIRST)

    barrier = pltpu.get_barrier_semaphore()
    for s in range(1, N_SP):
        pl.semaphore_signal(barrier, inc=1, device_id={'sp': lax.rem(sp + s, N_SP)}, device_id_type=MESH)
    pl.semaphore_signal(barrier, inc=1, device_id={'tp': 1 - tp}, device_id_type=MESH)

    for c in small:
        c.wait()
    hid = hidden[...].astype(jnp.float32)
    mean = jnp.mean(hid, axis=-1, keepdims=True)
    cen = hid - mean
    var = jnp.mean(cen * cen, axis=-1, keepdims=True)
    scale_rows = norm_scale[...].astype(jnp.float32)
    scale_row = jnp.concatenate([scale_rows[i:i + 1] for i in range(scale_rows.shape[0])], axis=1)
    normed = (cen * lax.rsqrt(var + 1e-5) * scale_row).astype(jnp.bfloat16)
    u[...] = normed

    brow = lax.broadcasted_iota(jnp.int32, (n_seq, 1), 0)
    pos_col = jnp.zeros((n_seq, 1), jnp.int32)
    for b in range(n_seq):
        pos_col = jnp.where(brow == b, pos[b], pos_col)
    angles = pos_col.astype(jnp.float32) * inv_freq[...]
    c2 = jnp.cos(angles)
    s2 = jnp.sin(angles)
    s2 = jnp.where(lax.broadcasted_iota(jnp.int32, s2.shape, 1) < head // 2, -s2, s2)
    rope_c[...] = c2
    rope_s[...] = s2

    group_heads = per_kv + 2

    def heads_copy(c):
        mine = heads.at[core, pl.ds(2 * c, 2)]
        return pltpu.make_async_remote_copy(mine, mine, acc_send.at[c], acc_recv.at[c],
                                            device_id={'sp': partner}, device_id_type=MESH)

    for c in range(w_chunks):
        w_copy(c).wait()
        start(STARTS[c])
        k_half = d_model // 2
        qkv = (jnp.dot(u[:, :k_half], wq[c, :k_half], preferred_element_type=jnp.float32)
               + jnp.dot(u[:, k_half:], wq[c, k_half:], preferred_element_type=jnp.float32))
        for i in range(2):
            x = jnp.clip(qkv[:, i * head:(i + 1) * head].astype(jnp.bfloat16).astype(jnp.float32), -8.0, 8.0)
            if (2 * c + i) % group_heads <= per_kv:
                x = x * rope_c[...] + pltpu.roll(x, head // 2, 1) * rope_s[...]
                x = x.astype(jnp.bfloat16).astype(jnp.float32)
            heads[core, 2 * c + i] = x
        if c == 0:
            pl.semaphore_wait(barrier, N_SP)
        heads_copy(c).start()

    def spread(half, queries):
        for h in range(half_cols // head):
            g, j = half * (kv // 2) + h // group_heads, h % group_heads
            if queries != (j < per_kv):
                continue
            x = heads[half, h]
            if queries:
                q_rows[pl.ds(g * per_kv + j, n_seq, stride=n_heads), :] = x
                continue
            wide, rep = (kn_rows, new_k) if j == per_kv else (vn_rows, new_v)
            for i in range(per_kv):
                wide[pl.ds(g * per_kv + i, n_seq, stride=n_heads), :] = x
            for i in range(16 // kv):
                rep[pl.ds(i * kv + g, n_seq, stride=16), :] = x

    col = lax.broadcasted_iota(jnp.int32, (pair_rows, rows), 1)
    row = lax.broadcasted_iota(jnp.int32, (pair_rows, rows), 0)
    row_kv = lax.rem(row, n_heads) // per_kv
    tok[...] = jnp.where(lax.rem(col, kv) == row_kv, sp * seq_local + col // kv, 1 << 30)

    for half in range(2):
        @pl.when(core == half)
        def _():
            spread(half, True)

    for c in range(w_chunks - 1):
        heads_copy(c).wait()
    for half in range(2):
        @pl.when(core != half)
        def _():
            spread(half, True)

    prow = lax.broadcasted_iota(jnp.int32, (pair_rows, 1), 0)
    first = prow < n_heads

    def part_copy(g, s):
        dst = lax.rem(sp + s, N_SP)
        return pltpu.make_async_remote_copy(
            src_ref=part.at[g, dst], dst_ref=recv.at[g, s - 1],
            send_sem=part_send.at[g, s - 1], recv_sem=part_recv.at[g, s - 1],
            device_id={'sp': dst}, device_id_type=MESH)

    lane = lax.broadcasted_iota(jnp.int32, (8, head), 1)
    n_stat = pair_rows // 8

    def scores(g, buf, k_ref, k_off):
        for d in range(N_SP):
            kb = g * GROUP + 2 * d - k_off
            q = q_rows[pl.ds(pl.multiple_of((g * N_SP + d) * pair_rows, 8), pair_rows), :]
            zero = jnp.zeros_like(q)
            q_blk = jnp.concatenate([jnp.where(first, q, zero), jnp.where(first, zero, q)], axis=1).astype(jnp.bfloat16)
            k_cat = jnp.concatenate([k_ref[kb], k_ref[kb + 1]], axis=1)
            score[buf, d] = lax.dot_general(q_blk, k_cat, (((1,), (1,)), ((), ())), preferred_element_type=jnp.float32)

    def values(g, buf, v_ref, v_off):
        for d in range(N_SP):
            b = g * GROUP + 2 * d
            vb = b - v_off
            limit = jnp.where(first, pos[b], pos[b + 1])
            s = jnp.where(tok[...] < limit, score[buf, d], NEG)
            m = jnp.maximum(jnp.max(s, axis=-1, keepdims=True), NEG / 2)
            w = jnp.exp2((s - m) * scale2)
            l = jnp.sum(w, axis=-1, keepdims=True)
            v_cat = jnp.concatenate([v_ref[vb], v_ref[vb + 1]], axis=1)
            o = jnp.dot(w.astype(jnp.bfloat16), v_cat, preferred_element_type=jnp.float32)
            part[g, d, :pair_rows] = jnp.where(first, o[:, :head], o[:, head:])
            stat = jnp.zeros((8, head), jnp.float32)
            for i in range(n_stat):
                stat = jnp.where(lane == i, m[8 * i:8 * i + 8], stat)
                stat = jnp.where(lane == n_stat + i, l[8 * i:8 * i + 8], stat)
            part[g, d, pair_rows:] = stat
        for s in range(1, N_SP):
            part_copy(g, s).start()

    g = 0
    for n in PHASES:
        gs = range(g, g + n)
        g += n
        if g == n_groups:
            heads_copy(w_chunks - 1).wait()
            for half in range(2):
                spread(half, False)
        for i in gs:
            k_copy(i).wait()
            start(1)
        for i in gs:
            k_ref, ki = held(k_vm, k_rest, HELD, i)
            scores(i, i - gs[0], k_ref, (i - ki) * GROUP)
        for i in gs:
            v_copy(i).wait()
            start(1)
        for i in gs:
            v_ref, vi = held(v_vm, v_rest, HELD, i)
            values(i, i - gs[0], v_ref, (i - vi) * GROUP)
    start(len(queue))
    def merge(g):
        r = pl.ds(pl.multiple_of((g * N_SP + sp) * pair_rows, 8), pair_rows)
        s_new = jnp.sum(q_rows[r, :] * kn_rows[r, :], axis=-1, keepdims=True)
        outs = [part[g, sp]] + [recv[g, s] for s in range(N_SP - 1)]

        def column(x, first_lane):
            return jnp.concatenate(
                [x[pair_rows:, first_lane + i:first_lane + i + 1] for i in range(n_stat)], axis=0)

        ms = [column(x, 0) for x in outs]
        ls = [column(x, n_stat) for x in outs]
        top = s_new
        for m in ms:
            top = jnp.maximum(top, m)
        f = jnp.exp2((s_new - top) * scale2)
        o = f * vn_rows[r, :]
        l = f
        for x, m, ll in zip(outs, ms, ls):
            f = jnp.exp2((m - top) * scale2)
            o = o + f * x[:pair_rows]
            l = l + f * ll
        merged[pl.ds(pl.multiple_of(g * pair_rows, 8), pair_rows), :] = o / l

    def tp_copy(p, c):
        return pltpu.make_async_remote_copy(proj.at[p, c], proj_in.at[p, c], tp_send.at[p, c], tp_recv.at[p, c],
                                            device_id={'tp': 1 - tp}, device_id_type=MESH)

    def x_copy(p, c):
        return pltpu.make_async_remote_copy(sums.at[p, c, sp], sums.at[p, c, sp], x_send.at[p, c], x_recv.at[p, c],
                                            device_id={'sp': across}, device_id_type=MESH)

    def core_copy(p, c):
        return pltpu.make_async_remote_copy(sums.at[p, c, sp], sums.at[p, c, sp], core_send.at[p, c], core_recv.at[p, c],
                                            device_id={'sp': partner}, device_id_type=MESH)

    def fwd_copy(p, c):
        return pltpu.make_async_remote_copy(sums.at[p, c, across], sums.at[p, c, across], fwd_send.at[p, c], fwd_recv.at[p, c],
                                            device_id={'sp': partner}, device_id_type=MESH)

    part_groups = n_groups // PARTS
    part_rows = own // PARTS

    def gather_heads(p):
        for gs in MERGES[p]:
            for g in gs:
                for s in range(1, N_SP):
                    part_copy(g, s).wait()
            for g in gs:
                merge(g)
        first_row = p * part_groups * pair_rows
        return jnp.concatenate([merged[pl.ds(first_row + n, part_rows, stride=n_heads), :].astype(jnp.bfloat16)
                                for n in range(n_heads)], axis=1)

    def project(p, c, attn):
        proj[p, c] = jnp.dot(attn, wo[c], preferred_element_type=jnp.float32)
        tp_copy(p, c).start()

    def add_tp(p, c):
        tp_copy(p, c).wait()
        sums[p, c, sp] = proj[p, c] + proj_in[p, c]
        x_copy(p, c).start()
        core_copy(p, c).start()

    def forward(p, c):
        x_copy(p, c).wait()
        fwd_copy(p, c).start()

    attn = gather_heads(0)
    for c in range(COLS):
        wo_copy(c).wait()
        project(0, c, attn)
    attn = gather_heads(1)
    for c in range(COLS):
        project(1, c, attn)
        add_tp(0, c)
    for c in range(COLS):
        add_tp(1, c)
        forward(0, c)
    for c in range(COLS):
        forward(1, c)

    srow = lax.broadcasted_iota(jnp.int32, (GROUP, 1), 0)
    for p in range(PARTS):
        for c in range(COLS):
            core_copy(p, c).wait()
            fwd_copy(p, c).wait()
            lanes = slice(c * width, (c + 1) * width)
            for i in range(part_groups):
                gathered = None
                for d in range(N_SP):
                    x = sums[p, c, d]
                    shift = (2 * d - 2 * i) % GROUP
                    if shift:
                        x = pltpu.roll(x, shift, 0)
                    gathered = x if gathered is None else jnp.where(srow // 2 == d, x, gathered)
                r = slice((p * part_groups + i) * GROUP, (p * part_groups + i + 1) * GROUP)
                h_out[r, lanes] = (hidden[r, lanes].astype(jnp.float32) + gathered).astype(jnp.bfloat16)


def write_kernel(dims, pos_in, h_in, k_vm, v_vm, new_k, new_v, k_in, v_in, h_out, k_out, v_out, k_same, v_same,
                 pos, slots, pos_sem, h_sem, rd_sem, wr_sem, blk_sem):
    n_seq, rows, kv, _, _, _ = dims
    sp = lax.axis_index('sp')
    seq_local = rows // kv
    n_held = HELD * GROUP
    per = 16 // kv
    sub = lax.broadcasted_iota(jnp.int32, (16, 1), 0) // kv
    jobs = [(src, out, new, b) for src, out, new in ((k_in, k_out, new_k), (v_in, v_out, new_v))
            for b in range(n_held, n_seq, JOB)]

    def patch(ref, i, b, new):
        p = pos[b] - sp * seq_local
        blk = jnp.clip(p, 0, seq_local - 1) // per
        r = pl.ds(pl.multiple_of(blk * 16, 16), 16)
        fresh = new[pl.ds(pl.multiple_of(b * 16, 16), 16), :]
        ref[i, r, :] = jnp.where(sub + blk * per == p, fresh, ref[i, r, :].astype(jnp.float32)).astype(jnp.bfloat16)

    def read(j):
        src, _, _, b = jobs[j]
        return pltpu.make_async_copy(src.at[pl.ds(b, JOB)], slots.at[j % SLOTS], rd_sem.at[j])

    def write(j):
        _, out, _, b = jobs[j]
        return pltpu.make_async_copy(slots.at[j % SLOTS], out.at[pl.ds(b, JOB)], wr_sem.at[j])

    def run(j):
        _, _, new, b = jobs[j]
        read(j).wait()
        for i in range(JOB):
            patch(slots.at[j % SLOTS], i, b + i, new)
        write(j).start()

    def again(j):
        write(j - SLOTS).wait()
        read(j).start()

    def block(n):
        vm, out = ((k_vm, k_out), (v_vm, v_out))[n % 2]
        s = pl.ds(n // 2 * GROUP, GROUP)
        return pltpu.make_async_copy(vm.at[s], out.at[s], blk_sem.at[n])

    def send(n):
        vm, new = ((k_vm, new_k), (v_vm, new_v))[n % 2]
        for i in range(GROUP):
            b = n // 2 * GROUP + i
            patch(vm, b, b, new)
        block(n).start()

    n_blocks = 2 * HELD
    pos_copy = pltpu.make_async_copy(pos_in, pos, pos_sem)
    pos_copy.start()
    h_copy = pltpu.make_async_copy(h_in, h_out, h_sem)
    h_copy.start()
    for j in range(SLOTS):
        read(j).start()
    pos_copy.wait()
    for n in range(n_blocks):
        if n >= WINDOW:
            block(n - WINDOW).wait()
        send(n)
        for j in range(len(jobs)):
            if j < SLOTS and n == WINDOW + j // 2 - 1:
                run(j)
            if j >= SLOTS and n == WINDOW + 2 + j // 2:
                again(j)
            if j >= SLOTS and n == WINDOW + 4 + j // 2:
                run(j)
    for n in range(n_blocks - WINDOW, n_blocks):
        block(n).wait()
    for j in range(len(jobs) - SLOTS, len(jobs)):
        write(j).wait()
    h_copy.wait()


def solution(mesh):
    cache_spec = P('dp', 'sp', 'tp', None)

    def local_step(hidden, norm_scale, w_qkv, w_out, k_cache, v_cache, positions):
        n_seq, seq_local, kv, head = k_cache.shape
        d_model = hidden.shape[1]
        per_kv = w_qkv.shape[1] // (kv * head) - 2
        rows = seq_local * kv
        n_heads = kv * per_kv
        n_groups = n_seq // GROUP
        pair_rows = 2 * n_heads
        own = n_seq // N_SP
        w_chunks = w_qkv.shape[1] // (4 * head)
        n_jobs = 2 * (n_seq - HELD * GROUP) // JOB
        dims = (n_seq, rows, kv, head, per_kv, d_model)
        half = np.arange(head) % (head // 2)
        inv_freq = np.exp(half * (-2.0 * math.log(500000.0) / head)).astype(np.float32)[None]
        f32, bf16 = jnp.float32, jnp.bfloat16
        vmem = pl.BlockSpec(memory_space=pltpu.VMEM)
        hbm = pl.BlockSpec(memory_space=pltpu.HBM)
        cache = (n_seq, rows, head)
        dma = pltpu.SemaphoreType.DMA
        keep = pltpu.with_memory_space_constraint
        w_qkv, w_out = keep(w_qkv, pltpu.HBM), keep(w_out, pltpu.HBM)
        k_flat = keep(k_cache.reshape(cache), pltpu.HBM)
        v_flat = keep(v_cache.reshape(cache), pltpu.HBM)
        h_vm, k_vm, v_vm, new_k, new_v = pl.pallas_call(
            lambda *refs: attend_kernel(dims, *refs),
            out_shape=(pltpu.VMEM(hidden.shape, bf16),
                       pltpu.VMEM((HELD * GROUP, rows, head), bf16),
                       pltpu.VMEM((HELD * GROUP, rows, head), bf16),
                       pltpu.VMEM((n_seq * 16, head), f32),
                       pltpu.VMEM((n_seq * 16, head), f32)),
            in_specs=[hbm] * 8,
            out_specs=(vmem,) * 5,
            scratch_shapes=[
                pltpu.SMEM((n_seq,), jnp.int32),
                pltpu.VMEM(hidden.shape, bf16),
                pltpu.VMEM((d_model // head, head), bf16),
                pltpu.VMEM((1, head), f32),
                pltpu.VMEM(hidden.shape, bf16),
                pltpu.VMEM((w_chunks, d_model, 2 * head), bf16),
                pltpu.VMEM((2, 2 * w_chunks, n_seq, head), f32),
                pltpu.VMEM((n_seq, head), f32),
                pltpu.VMEM((n_seq, head), f32),
                pltpu.VMEM((COLS, w_out.shape[0], d_model // COLS), bf16),
                pltpu.VMEM((n_seq - HELD * GROUP, rows, head), bf16),
                pltpu.VMEM((n_seq - HELD * GROUP, rows, head), bf16),
                pltpu.VMEM((n_seq * n_heads, head), f32),
                pltpu.VMEM((n_seq * n_heads, head), f32),
                pltpu.VMEM((n_seq * n_heads, head), f32),
                pltpu.VMEM((pair_rows, rows), jnp.int32),
                pltpu.VMEM((max(PHASES), N_SP, pair_rows, rows), f32),
                pltpu.VMEM((n_groups, N_SP, pair_rows + 8, head), f32),
                pltpu.VMEM((n_groups, N_SP - 1, pair_rows + 8, head), f32),
                pltpu.VMEM((own * n_heads, head), f32),
                pltpu.VMEM((PARTS, COLS, own // PARTS, d_model // COLS), f32),
                pltpu.VMEM((PARTS, COLS, own // PARTS, d_model // COLS), f32),
                pltpu.VMEM((PARTS, COLS, N_SP, own // PARTS, d_model // COLS), f32),
                dma((4,)), dma((w_chunks,)), dma((COLS,)), dma((n_groups,)), dma((n_groups,)),
                dma((w_chunks,)), dma((w_chunks,)),
                dma((n_groups, N_SP - 1)), dma((n_groups, N_SP - 1)),
            ] + [dma((PARTS, COLS))] * 8,
            compiler_params=pltpu.CompilerParams(
                collective_id=0, has_side_effects=True, vmem_limit_bytes=33 * MIB),
            name='attend',
        )(keep(positions, pltpu.HBM), keep(hidden, pltpu.HBM),
          keep(norm_scale.reshape(d_model // head, head), pltpu.HBM), inv_freq, w_qkv, w_out, k_flat, v_flat)
        h_out, k_out, v_out, _, _ = pl.pallas_call(
            lambda *refs: write_kernel(dims, *refs),
            out_shape=(jax.ShapeDtypeStruct(hidden.shape, bf16),
                       jax.ShapeDtypeStruct(cache, bf16), jax.ShapeDtypeStruct(cache, bf16),
                       pltpu.VMEM(k_vm.shape, bf16), pltpu.VMEM(v_vm.shape, bf16)),
            in_specs=[hbm] + [vmem] * 5 + [hbm] * 2,
            out_specs=(hbm,) * 3 + (vmem,) * 2,
            input_output_aliases={2: 3, 3: 4},
            scratch_shapes=[
                pltpu.SMEM((n_seq,), jnp.int32),
                pltpu.VMEM((SLOTS, JOB, rows, head), bf16),
                dma, dma, dma((n_jobs,)), dma((n_jobs,)), dma((2 * HELD,)),
            ],
            compiler_params=pltpu.CompilerParams(vmem_limit_bytes=W_VMEM * MIB),
            name='write',
        )(keep(positions, pltpu.HBM), *[keep(x, pltpu.VMEM) for x in (h_vm, k_vm, v_vm, new_k, new_v)], k_flat, v_flat)
        return h_out, k_out.reshape(k_cache.shape), v_out.reshape(v_cache.shape)

    return jax.shard_map(
        local_step,
        mesh=mesh,
        in_specs=(P('dp', None), P(None), P(None, 'tp'), P('tp', None), cache_spec, cache_spec, P('dp')),
        out_specs=(P('dp', None), cache_spec, cache_spec),
        check_vma=False,
    )
```

```python
import math
import jax
import jax.numpy as jnp
import numpy as np
from jax import lax
from jax.experimental import pallas as pl
from jax.experimental.pallas import tpu as pltpu
from jax.sharding import PartitionSpec as P

MESH = pl.DeviceIdType.MESH
NEG = -1e30
MIB = 1024 * 1024
N_SP = 4
COLS = 3
PARTS = 2
MERGES = (((0, 1, 2, 3),), ((4, 5), (6, 7)))
PHASES = (2, 2, 2, 2)
GROUP = 8
FIRST = 3
STARTS = (1, 1, 1, 2, 4)
HELD = 7
JOB = 2
SLOTS = 4
WINDOW = 4
W_VMEM = 3


def attend_kernel(dims, pos_in, hidden_in, scale_in, freq_in, w_qkv, w_out, k_in, v_in,
                  h_out, k_vm, v_vm, new_k, new_v,
                  pos, hidden, norm_scale, inv_freq, u, wq, heads, rope_c, rope_s, wo, k_rest, v_rest, q_rows, kn_rows, vn_rows, tok, score, part, recv, merged, proj, proj_in, sums,
                  in_sem, w_sem, wo_sem, k_sem, v_sem, acc_send, acc_recv, part_send, part_recv, tp_send, tp_recv, x_send, x_recv,
                  core_send, core_recv, fwd_send, fwd_recv):
    n_seq, rows, kv, head, per_kv, d_model = dims
    n_heads = kv * per_kv
    n_groups = n_seq // GROUP
    pair_rows = 2 * n_heads
    own = n_seq // N_SP
    sp = lax.axis_index('sp')
    tp = lax.axis_index('tp')
    seq_local = rows // kv
    scale2 = head ** -0.5 * math.log2(math.e)

    core = lax.rem(sp, 2)
    partner = sp + 1 - 2 * core
    across = lax.rem(sp + 2, N_SP)
    half_cols = w_qkv.shape[1] // 2
    w_cols = 2 * head
    w_chunks = half_cols // w_cols

    def w_copy(c):
        cols = pl.ds(pl.multiple_of(core * half_cols + c * w_cols, head), w_cols)
        return pltpu.make_async_copy(w_qkv.at[:, cols], wq.at[c], w_sem.at[c])

    def held(ref, rest, n_held, g):
        return (ref, g) if g < n_held else (rest, g - n_held)

    def cache_copy(src, ref, rest, n_held, sem, g):
        dst, i = held(ref, rest, n_held, g)
        return pltpu.make_async_copy(src.at[pl.ds(g * GROUP, GROUP)], dst.at[pl.ds(i * GROUP, GROUP)], sem.at[g])

    def k_copy(g):
        return cache_copy(k_in, k_vm, k_rest, HELD, k_sem, g)

    def v_copy(g):
        return cache_copy(v_in, v_vm, v_rest, HELD, v_sem, g)

    width = d_model // COLS

    def wo_copy(c):
        return pltpu.make_async_copy(w_out.at[:, pl.ds(c * width, width)], wo.at[c], wo_sem.at[c])

    queue = [w_copy(c) for c in range(w_chunks)]
    g = 0
    for n in PHASES:
        queue += [k_copy(i) for i in range(g, g + n)] + [v_copy(i) for i in range(g, g + n)]
        g += n
    queue += [wo_copy(c) for c in range(COLS)]
    started = 0

    def start(n):
        nonlocal started
        for copy in queue[started:started + n]:
            copy.start()
        started += n

    small = [pltpu.make_async_copy(a, b, in_sem.at[i]) for i, (a, b) in enumerate(
        ((hidden_in, hidden), (scale_in, norm_scale), (freq_in, inv_freq), (pos_in, pos)))]
    for c in small:
        c.start()
    start(FIRST)

    barrier = pltpu.get_barrier_semaphore()
    for s in range(1, N_SP):
        pl.semaphore_signal(barrier, inc=1, device_id={'sp': lax.rem(sp + s, N_SP)}, device_id_type=MESH)
    pl.semaphore_signal(barrier, inc=1, device_id={'tp': 1 - tp}, device_id_type=MESH)

    for c in small:
        c.wait()
    hid = hidden[...].astype(jnp.float32)
    mean = jnp.mean(hid, axis=-1, keepdims=True)
    cen = hid - mean
    var = jnp.mean(cen * cen, axis=-1, keepdims=True)
    scale_rows = norm_scale[...].astype(jnp.float32)
    scale_row = jnp.concatenate([scale_rows[i:i + 1] for i in range(scale_rows.shape[0])], axis=1)
    normed = (cen * lax.rsqrt(var + 1e-5) * scale_row).astype(jnp.bfloat16)
    u[...] = normed

    brow = lax.broadcasted_iota(jnp.int32, (n_seq, 1), 0)
    pos_col = jnp.zeros((n_seq, 1), jnp.int32)
    for b in range(n_seq):
        pos_col = jnp.where(brow == b, pos[b], pos_col)
    angles = pos_col.astype(jnp.float32) * inv_freq[...]
    c2 = jnp.cos(angles)
    s2 = jnp.sin(angles)
    s2 = jnp.where(lax.broadcasted_iota(jnp.int32, s2.shape, 1) < head // 2, -s2, s2)
    rope_c[...] = c2
    rope_s[...] = s2

    group_heads = per_kv + 2

    def heads_copy(c):
        mine = heads.at[core, pl.ds(2 * c, 2)]
        return pltpu.make_async_remote_copy(mine, mine, acc_send.at[c], acc_recv.at[c],
                                            device_id={'sp': partner}, device_id_type=MESH)

    for c in range(w_chunks):
        w_copy(c).wait()
        start(STARTS[c])
        k_half = d_model // 2
        qkv = (jnp.dot(u[:, :k_half], wq[c, :k_half], preferred_element_type=jnp.float32)
               + jnp.dot(u[:, k_half:], wq[c, k_half:], preferred_element_type=jnp.float32))
        for i in range(2):
            x = jnp.clip(qkv[:, i * head:(i + 1) * head].astype(jnp.bfloat16).astype(jnp.float32), -8.0, 8.0)
            if (2 * c + i) % group_heads <= per_kv:
                x = x * rope_c[...] + pltpu.roll(x, head // 2, 1) * rope_s[...]
                x = x.astype(jnp.bfloat16).astype(jnp.float32)
            heads[core, 2 * c + i] = x
        if c == 0:
            pl.semaphore_wait(barrier, N_SP)
        heads_copy(c).start()

    def spread(half, queries):
        for h in range(half_cols // head):
            g, j = half * (kv // 2) + h // group_heads, h % group_heads
            if queries != (j < per_kv):
                continue
            x = heads[half, h]
            if queries:
                q_rows[pl.ds(g * per_kv + j, n_seq, stride=n_heads), :] = x
                continue
            wide = kn_rows if j == per_kv else vn_rows
            for i in range(per_kv):
                wide[pl.ds(g * per_kv + i, n_seq, stride=n_heads), :] = x

    def repeat_rows():
        for g in range(kv):
            for j, rep in ((per_kv, new_k), (per_kv + 1, new_v)):
                x = heads[g // (kv // 2), g % (kv // 2) * group_heads + j]
                for i in range(16 // kv):
                    rep[pl.ds(i * kv + g, n_seq, stride=16), :] = x

    col = lax.broadcasted_iota(jnp.int32, (pair_rows, rows), 1)
    row = lax.broadcasted_iota(jnp.int32, (pair_rows, rows), 0)
    row_kv = lax.rem(row, n_heads) // per_kv
    tok[...] = jnp.where(lax.rem(col, kv) == row_kv, sp * seq_local + col // kv, 1 << 30)

    for half in range(2):
        @pl.when(core == half)
        def _():
            spread(half, True)

    for c in range(w_chunks - 1):
        heads_copy(c).wait()
    for half in range(2):
        @pl.when(core != half)
        def _():
            spread(half, True)

    prow = lax.broadcasted_iota(jnp.int32, (pair_rows, 1), 0)
    first = prow < n_heads

    def part_copy(g, s):
        dst = lax.rem(sp + s, N_SP)
        return pltpu.make_async_remote_copy(
            src_ref=part.at[g, dst], dst_ref=recv.at[g, s - 1],
            send_sem=part_send.at[g, s - 1], recv_sem=part_recv.at[g, s - 1],
            device_id={'sp': dst}, device_id_type=MESH)

    lane = lax.broadcasted_iota(jnp.int32, (8, head), 1)
    n_stat = pair_rows // 8

    def scores(g, buf, k_ref, k_off):
        for d in range(N_SP):
            kb = g * GROUP + 2 * d - k_off
            q = q_rows[pl.ds(pl.multiple_of((g * N_SP + d) * pair_rows, 8), pair_rows), :]
            zero = jnp.zeros_like(q)
            q_blk = jnp.concatenate([jnp.where(first, q, zero), jnp.where(first, zero, q)], axis=1).astype(jnp.bfloat16)
            k_cat = jnp.concatenate([k_ref[kb], k_ref[kb + 1]], axis=1)
            score[buf, d] = lax.dot_general(q_blk, k_cat, (((1,), (1,)), ((), ())), preferred_element_type=jnp.float32)

    def values(g, buf, v_ref, v_off):
        for d in range(N_SP):
            b = g * GROUP + 2 * d
            vb = b - v_off
            limit = jnp.where(first, pos[b], pos[b + 1])
            s = jnp.where(tok[...] < limit, score[buf, d], NEG)
            m = jnp.maximum(jnp.max(s, axis=-1, keepdims=True), NEG / 2)
            w = jnp.exp2((s - m) * scale2)
            l = jnp.sum(w, axis=-1, keepdims=True)
            v_cat = jnp.concatenate([v_ref[vb], v_ref[vb + 1]], axis=1)
            o = jnp.dot(w.astype(jnp.bfloat16), v_cat, preferred_element_type=jnp.float32)
            part[g, d, :pair_rows] = jnp.where(first, o[:, :head], o[:, head:])
            stat = jnp.zeros((8, head), jnp.float32)
            for i in range(n_stat):
                stat = jnp.where(lane == i, m[8 * i:8 * i + 8], stat)
                stat = jnp.where(lane == n_stat + i, l[8 * i:8 * i + 8], stat)
            part[g, d, pair_rows:] = stat
        for s in range(1, N_SP):
            part_copy(g, s).start()

    g = 0
    for n in PHASES:
        gs = range(g, g + n)
        g += n
        if g == n_groups:
            heads_copy(w_chunks - 1).wait()
            for half in range(2):
                spread(half, False)
        for i in gs:
            k_copy(i).wait()
            start(1)
        for i in gs:
            k_ref, ki = held(k_vm, k_rest, HELD, i)
            scores(i, i - gs[0], k_ref, (i - ki) * GROUP)
        for i in gs:
            v_copy(i).wait()
            start(1)
        for i in gs:
            v_ref, vi = held(v_vm, v_rest, HELD, i)
            values(i, i - gs[0], v_ref, (i - vi) * GROUP)
    start(len(queue))
    def merge(g):
        r = pl.ds(pl.multiple_of((g * N_SP + sp) * pair_rows, 8), pair_rows)
        s_new = jnp.sum(q_rows[r, :] * kn_rows[r, :], axis=-1, keepdims=True)
        outs = [part[g, sp]] + [recv[g, s] for s in range(N_SP - 1)]

        def column(x, first_lane):
            return jnp.concatenate(
                [x[pair_rows:, first_lane + i:first_lane + i + 1] for i in range(n_stat)], axis=0)

        ms = [column(x, 0) for x in outs]
        ls = [column(x, n_stat) for x in outs]
        top = s_new
        for m in ms:
            top = jnp.maximum(top, m)
        f = jnp.exp2((s_new - top) * scale2)
        o = f * vn_rows[r, :]
        l = f
        for x, m, ll in zip(outs, ms, ls):
            f = jnp.exp2((m - top) * scale2)
            o = o + f * x[:pair_rows]
            l = l + f * ll
        merged[pl.ds(pl.multiple_of(g * pair_rows, 8), pair_rows), :] = o / l

    def tp_copy(p, c):
        return pltpu.make_async_remote_copy(proj.at[p, c], proj_in.at[p, c], tp_send.at[p, c], tp_recv.at[p, c],
                                            device_id={'tp': 1 - tp}, device_id_type=MESH)

    def x_copy(p, c):
        return pltpu.make_async_remote_copy(sums.at[p, c, sp], sums.at[p, c, sp], x_send.at[p, c], x_recv.at[p, c],
                                            device_id={'sp': across}, device_id_type=MESH)

    def core_copy(p, c):
        return pltpu.make_async_remote_copy(sums.at[p, c, sp], sums.at[p, c, sp], core_send.at[p, c], core_recv.at[p, c],
                                            device_id={'sp': partner}, device_id_type=MESH)

    def fwd_copy(p, c):
        return pltpu.make_async_remote_copy(sums.at[p, c, across], sums.at[p, c, across], fwd_send.at[p, c], fwd_recv.at[p, c],
                                            device_id={'sp': partner}, device_id_type=MESH)

    part_groups = n_groups // PARTS
    part_rows = own // PARTS

    def gather_heads(p):
        for gs in MERGES[p]:
            for g in gs:
                for s in range(1, N_SP):
                    part_copy(g, s).wait()
            for g in gs:
                merge(g)
        first_row = p * part_groups * pair_rows
        return jnp.concatenate([merged[pl.ds(first_row + n, part_rows, stride=n_heads), :].astype(jnp.bfloat16)
                                for n in range(n_heads)], axis=1)

    def project(p, c, attn):
        proj[p, c] = jnp.dot(attn, wo[c], preferred_element_type=jnp.float32)
        tp_copy(p, c).start()

    def add_tp(p, c):
        tp_copy(p, c).wait()
        sums[p, c, sp] = proj[p, c] + proj_in[p, c]
        x_copy(p, c).start()
        core_copy(p, c).start()

    def forward(p, c):
        x_copy(p, c).wait()
        fwd_copy(p, c).start()

    attn = gather_heads(0)
    for c in range(COLS):
        wo_copy(c).wait()
        project(0, c, attn)
    attn = gather_heads(1)
    for c in range(COLS):
        project(1, c, attn)
        add_tp(0, c)
    repeat_rows()
    for c in range(COLS):
        add_tp(1, c)
        forward(0, c)
    for c in range(COLS):
        forward(1, c)

    srow = lax.broadcasted_iota(jnp.int32, (GROUP, 1), 0)
    for p in range(PARTS):
        for c in range(COLS):
            core_copy(p, c).wait()
            fwd_copy(p, c).wait()
            lanes = slice(c * width, (c + 1) * width)
            for i in range(part_groups):
                gathered = None
                for d in range(N_SP):
                    x = sums[p, c, d]
                    shift = (2 * d - 2 * i) % GROUP
                    if shift:
                        x = pltpu.roll(x, shift, 0)
                    gathered = x if gathered is None else jnp.where(srow // 2 == d, x, gathered)
                r = slice((p * part_groups + i) * GROUP, (p * part_groups + i + 1) * GROUP)
                h_out[r, lanes] = (hidden[r, lanes].astype(jnp.float32) + gathered).astype(jnp.bfloat16)


def write_kernel(dims, pos_in, h_in, k_vm, v_vm, new_k, new_v, k_in, v_in, h_out, k_out, v_out, k_same, v_same,
                 pos, slots, pos_sem, h_sem, rd_sem, wr_sem, blk_sem):
    n_seq, rows, kv, _, _, _ = dims
    sp = lax.axis_index('sp')
    seq_local = rows // kv
    n_held = HELD * GROUP
    per = 16 // kv
    sub = lax.broadcasted_iota(jnp.int32, (16, 1), 0) // kv
    jobs = [(src, out, new, b) for src, out, new in ((k_in, k_out, new_k), (v_in, v_out, new_v))
            for b in range(n_held, n_seq, JOB)]

    def patch(ref, i, b, new):
        p = pos[b] - sp * seq_local
        blk = jnp.clip(p, 0, seq_local - 1) // per
        r = pl.ds(pl.multiple_of(blk * 16, 16), 16)
        fresh = new[pl.ds(pl.multiple_of(b * 16, 16), 16), :]
        ref[i, r, :] = jnp.where(sub + blk * per == p, fresh, ref[i, r, :].astype(jnp.float32)).astype(jnp.bfloat16)

    def read(j):
        src, _, _, b = jobs[j]
        return pltpu.make_async_copy(src.at[pl.ds(b, JOB)], slots.at[j % SLOTS], rd_sem.at[j])

    def write(j):
        _, out, _, b = jobs[j]
        return pltpu.make_async_copy(slots.at[j % SLOTS], out.at[pl.ds(b, JOB)], wr_sem.at[j])

    def run(j):
        _, _, new, b = jobs[j]
        read(j).wait()
        for i in range(JOB):
            patch(slots.at[j % SLOTS], i, b + i, new)
        write(j).start()

    def again(j):
        write(j - SLOTS).wait()
        read(j).start()

    def block(n):
        vm, out = ((k_vm, k_out), (v_vm, v_out))[n % 2]
        s = pl.ds(n // 2 * GROUP, GROUP)
        return pltpu.make_async_copy(vm.at[s], out.at[s], blk_sem.at[n])

    def send(n):
        vm, new = ((k_vm, new_k), (v_vm, new_v))[n % 2]
        for i in range(GROUP):
            b = n // 2 * GROUP + i
            patch(vm, b, b, new)
        block(n).start()

    n_blocks = 2 * HELD
    pos_copy = pltpu.make_async_copy(pos_in, pos, pos_sem)
    pos_copy.start()
    h_copy = pltpu.make_async_copy(h_in, h_out, h_sem)
    h_copy.start()
    for j in range(SLOTS):
        read(j).start()
    pos_copy.wait()
    for n in range(n_blocks):
        if n >= WINDOW:
            block(n - WINDOW).wait()
        send(n)
        for j in range(len(jobs)):
            if j < SLOTS and n == WINDOW + j // 2 - 1:
                run(j)
            if j >= SLOTS and n == WINDOW + 2 + j // 2:
                again(j)
            if j >= SLOTS and n == WINDOW + 4 + j // 2:
                run(j)
    for n in range(n_blocks - WINDOW, n_blocks):
        block(n).wait()
    for j in range(len(jobs) - SLOTS, len(jobs)):
        write(j).wait()
    h_copy.wait()


def solution(mesh):
    cache_spec = P('dp', 'sp', 'tp', None)

    def local_step(hidden, norm_scale, w_qkv, w_out, k_cache, v_cache, positions):
        n_seq, seq_local, kv, head = k_cache.shape
        d_model = hidden.shape[1]
        per_kv = w_qkv.shape[1] // (kv * head) - 2
        rows = seq_local * kv
        n_heads = kv * per_kv
        n_groups = n_seq // GROUP
        pair_rows = 2 * n_heads
        own = n_seq // N_SP
        w_chunks = w_qkv.shape[1] // (4 * head)
        n_jobs = 2 * (n_seq - HELD * GROUP) // JOB
        dims = (n_seq, rows, kv, head, per_kv, d_model)
        half = np.arange(head) % (head // 2)
        inv_freq = np.exp(half * (-2.0 * math.log(500000.0) / head)).astype(np.float32)[None]
        f32, bf16 = jnp.float32, jnp.bfloat16
        vmem = pl.BlockSpec(memory_space=pltpu.VMEM)
        hbm = pl.BlockSpec(memory_space=pltpu.HBM)
        cache = (n_seq, rows, head)
        dma = pltpu.SemaphoreType.DMA
        keep = pltpu.with_memory_space_constraint
        w_qkv, w_out = keep(w_qkv, pltpu.HBM), keep(w_out, pltpu.HBM)
        k_flat = keep(k_cache.reshape(cache), pltpu.HBM)
        v_flat = keep(v_cache.reshape(cache), pltpu.HBM)
        h_vm, k_vm, v_vm, new_k, new_v = pl.pallas_call(
            lambda *refs: attend_kernel(dims, *refs),
            out_shape=(pltpu.VMEM(hidden.shape, bf16),
                       pltpu.VMEM((HELD * GROUP, rows, head), bf16),
                       pltpu.VMEM((HELD * GROUP, rows, head), bf16),
                       pltpu.VMEM((n_seq * 16, head), f32),
                       pltpu.VMEM((n_seq * 16, head), f32)),
            in_specs=[hbm] * 8,
            out_specs=(vmem,) * 5,
            scratch_shapes=[
                pltpu.SMEM((n_seq,), jnp.int32),
                pltpu.VMEM(hidden.shape, bf16),
                pltpu.VMEM((d_model // head, head), bf16),
                pltpu.VMEM((1, head), f32),
                pltpu.VMEM(hidden.shape, bf16),
                pltpu.VMEM((w_chunks, d_model, 2 * head), bf16),
                pltpu.VMEM((2, 2 * w_chunks, n_seq, head), f32),
                pltpu.VMEM((n_seq, head), f32),
                pltpu.VMEM((n_seq, head), f32),
                pltpu.VMEM((COLS, w_out.shape[0], d_model // COLS), bf16),
                pltpu.VMEM((n_seq - HELD * GROUP, rows, head), bf16),
                pltpu.VMEM((n_seq - HELD * GROUP, rows, head), bf16),
                pltpu.VMEM((n_seq * n_heads, head), f32),
                pltpu.VMEM((n_seq * n_heads, head), f32),
                pltpu.VMEM((n_seq * n_heads, head), f32),
                pltpu.VMEM((pair_rows, rows), jnp.int32),
                pltpu.VMEM((max(PHASES), N_SP, pair_rows, rows), f32),
                pltpu.VMEM((n_groups, N_SP, pair_rows + 8, head), f32),
                pltpu.VMEM((n_groups, N_SP - 1, pair_rows + 8, head), f32),
                pltpu.VMEM((own * n_heads, head), f32),
                pltpu.VMEM((PARTS, COLS, own // PARTS, d_model // COLS), f32),
                pltpu.VMEM((PARTS, COLS, own // PARTS, d_model // COLS), f32),
                pltpu.VMEM((PARTS, COLS, N_SP, own // PARTS, d_model // COLS), f32),
                dma((4,)), dma((w_chunks,)), dma((COLS,)), dma((n_groups,)), dma((n_groups,)),
                dma((w_chunks,)), dma((w_chunks,)),
                dma((n_groups, N_SP - 1)), dma((n_groups, N_SP - 1)),
            ] + [dma((PARTS, COLS))] * 8,
            compiler_params=pltpu.CompilerParams(
                collective_id=0, has_side_effects=True, vmem_limit_bytes=33 * MIB),
            name='attend',
        )(keep(positions, pltpu.HBM), keep(hidden, pltpu.HBM),
          keep(norm_scale.reshape(d_model // head, head), pltpu.HBM), inv_freq, w_qkv, w_out, k_flat, v_flat)
        h_out, k_out, v_out, _, _ = pl.pallas_call(
            lambda *refs: write_kernel(dims, *refs),
            out_shape=(jax.ShapeDtypeStruct(hidden.shape, bf16),
                       jax.ShapeDtypeStruct(cache, bf16), jax.ShapeDtypeStruct(cache, bf16),
                       pltpu.VMEM(k_vm.shape, bf16), pltpu.VMEM(v_vm.shape, bf16)),
            in_specs=[hbm] + [vmem] * 5 + [hbm] * 2,
            out_specs=(hbm,) * 3 + (vmem,) * 2,
            input_output_aliases={2: 3, 3: 4},
            scratch_shapes=[
                pltpu.SMEM((n_seq,), jnp.int32),
                pltpu.VMEM((SLOTS, JOB, rows, head), bf16),
                dma, dma, dma((n_jobs,)), dma((n_jobs,)), dma((2 * HELD,)),
            ],
            compiler_params=pltpu.CompilerParams(vmem_limit_bytes=W_VMEM * MIB),
            name='write',
        )(keep(positions, pltpu.HBM), *[keep(x, pltpu.VMEM) for x in (h_vm, k_vm, v_vm, new_k, new_v)], k_flat, v_flat)
        return h_out, k_out.reshape(k_cache.shape), v_out.reshape(v_cache.shape)

    return jax.shard_map(
        local_step,
        mesh=mesh,
        in_specs=(P('dp', None), P(None), P(None, 'tp'), P('tp', None), cache_spec, cache_spec, P('dp')),
        out_specs=(P('dp', None), cache_spec, cache_spec),
        check_vma=False,
    )
```
